256 devices in a mesh: src: 128 (over z, y, x_lo, core), tgt: 2 (over x_hi).
Axes of the slice: x: 4 (x_hi: 2, x_lo: 2; x = x_hi * 2 + x_lo), y: 4, z: 8, core: 2. Of those that a mesh axis runs over, the one named last changes fastest.
Arguments:
- positions: float32 [3, 32768], P(None, ('src', 'tgt')), may hold values from -1.3 to 1.3, as said below
- areas: float32 [32768], P(('src', 'tgt')), may hold values from 0.25 to 4
- right_side: float32 [3, 32768], P(None, ('src', 'tgt')), may hold values from -6 to 6
Outputs:
- solution_field: float32 [3, 32768], P(None, ('src', 'tgt'))
- residual: float32 [3, 32768], P(None, ('src', 'tgt'))
- hessenberg: float32 [5, 4], replicated
The draws below stay inside these ranges and needn't reach their ends.
Inputs may be any that keep to these rules, and one draw needn't show every extreme that they name: positions lie on a sphere of radius 1 or an ellipsoid centred at the anchor with semi-axes between 0.7 and 1.3, with no locality in how panels are assigned to devices.
All inputs are finite; a program needn't handle non-finite values.
Results may differ from the reference program's by a relative error of at most 0.0003.
Values sent between devices are 32-bit elements.
A program may use at most 64 MiB of HBM per device.

```python
import math
import jax
import jax.numpy as jnp
from jax import lax

ITERS = 4
PANELS = 32768


def draw_positions(key, part):
    points = jax.random.normal(key, (3, PANELS), jnp.float32)
    sphere = points / jnp.linalg.norm(points, axis=0, keepdims=True)
    return sphere


def level_of(key, dims, shards, low, largest):
    level = 1.0
    for position, parts in shards:
        heights = jax.random.uniform(jax.random.fold_in(jax.random.fold_in(key, 6), position), (parts,), jnp.float32, low / len(shards), largest / len(shards))
        level = level * jnp.repeat(jnp.exp(heights), dims[position] // parts).reshape((-1,) + (1,) * (len(dims) - 1 - position))
    return level


def bell_draw(rng, shape, scale, bound, pieces=(), held_as=jnp.bfloat16):
    drawn = jax.random.normal(rng, shape, jnp.float32) * scale
    if len(pieces) > 0:
        drawn = level_of(rng, shape, pieces, -0.22, 0.18) * drawn
    return jnp.clip(drawn, min=-bound, max=bound).astype(held_as)


def setup_inputs(seed: int = 0) -> dict:
    streams_of = jax.random.split(jax.random.key(seed), 4)
    positions = draw_positions(jax.random.fold_in(streams_of[3], 71), 0)
    areas = jnp.clip(jnp.exp(math.log(4.0) - 2.7725887 * jax.random.uniform(streams_of[1], (PANELS,), jnp.float32) ** level_of(streams_of[1], (PANELS,), ((0, 256),), -0.2, 0.2)), 0.25, 4.0)
    right_side = bell_draw(streams_of[2], (3, PANELS), 1.0, 6.0, ((1, 256),), jnp.float32)
    return dict(positions=positions, areas=areas, right_side=right_side)


soften = 0.0025

def stokes_block(targets, sources, densities):
    offset = targets[:, :, None] - sources[:, None, :]
    square = lax.optimization_barrier(jnp.sum(offset * offset, axis=0)) + soften
    factor = square ** (-1.5)
    projected = lax.optimization_barrier(jnp.sum(offset * densities[:, None, :], axis=0))
    return lax.optimization_barrier(jnp.sum(factor[None] * ((square + soften)[None] * densities[:, None, :] + offset * projected[None]), axis=2))

def apply_operator(vector, positions, areas):
    weighted = vector * (areas * PANELS ** (-0.5))[None, :]
    row_block = math.gcd(PANELS, 256)
    blocks = PANELS // row_block
    target_blocks = positions.reshape(3, blocks, row_block).transpose(1, 0, 2)

    def one_block(targets):
        return stokes_block(targets, positions, weighted)
    induced = lax.map(one_block, target_blocks)
    return vector + induced.transpose(1, 0, 2).reshape(3, PANELS)

def least_squares(hessenberg, initial):
    columns = hessenberg.shape[1]
    triangle = hessenberg
    target = jnp.zeros((hessenberg.shape[0],), jnp.float32).at[0].set(initial)
    for column in range(columns):
        leading = triangle[column, column]
        second = triangle[column + 1, column]
        radius = jnp.sqrt(leading * leading + second * second)
        cosine = leading / radius
        sine_value = second / radius
        row_top = triangle[column]
        row_low = triangle[column + 1]
        triangle = triangle.at[column].set(cosine * row_top + sine_value * row_low)
        triangle = triangle.at[column + 1].set(cosine * row_low - sine_value * row_top)
        target_top = target[column]
        target_low = target[column + 1]
        target = target.at[column].set(cosine * target_top + sine_value * target_low)
        target = target.at[column + 1].set(cosine * target_low - sine_value * target_top)
    solution = jnp.zeros((columns,), jnp.float32)
    for row_index in reversed(range(columns)):
        partial_sum = jnp.sum(triangle[row_index, row_index + 1:columns] * solution[row_index + 1:columns])
        solution = solution.at[row_index].set((target[row_index] - partial_sum) / triangle[row_index, row_index])
    return solution

def reference(positions, areas, right_side):
    initial = jnp.sqrt(jnp.sum(right_side * right_side))
    krylov_basis = [right_side / initial]
    hessenberg = jnp.zeros((ITERS + 1, ITERS), jnp.float32)
    for iteration in range(ITERS):
        applied = apply_operator(krylov_basis[iteration], positions, areas)
        stacked = jnp.stack(krylov_basis)
        projections = lax.optimization_barrier(jnp.sum(stacked * applied[None], axis=(1, 2)))
        remainder = applied - lax.optimization_barrier(jnp.sum(projections[:, None, None] * stacked, axis=0))
        height = jnp.sqrt(jnp.sum(remainder * remainder))
        hessenberg = hessenberg.at[:iteration + 1, iteration].set(projections)
        hessenberg = hessenberg.at[iteration + 1, iteration].set(height)
        krylov_basis.append(remainder / height)
    coefficients = least_squares(hessenberg, initial)
    stacked = jnp.stack(krylov_basis)
    solution_field = lax.optimization_barrier(jnp.sum(coefficients[:, None, None] * stacked[:ITERS], axis=0))
    misfit = -lax.optimization_barrier(jnp.sum(hessenberg * coefficients[None, :], axis=1))
    misfit = misfit.at[0].add(initial)
    residual = lax.optimization_barrier(jnp.sum(misfit[:, None, None] * stacked, axis=0))
    return (solution_field, residual, hessenberg)
```

```python
import functools

import jax
import jax.numpy as jnp
from jax import lax
from jax.experimental import pallas as pl
from jax.experimental.pallas import tpu as pltpu
from jax.sharding import Mesh
from jax.sharding import PartitionSpec as P

ITERS = 4
soften = 0.0025
LANES = 128
DEPTH = 8
PLANE = 32
MESH = pl.DeviceIdType.MESH
F32 = jnp.float32
BF16 = jnp.bfloat16


def split3(value):
    first = value.astype(BF16).astype(F32)
    rest = value - first
    second = rest.astype(BF16).astype(F32)
    return first, second, rest - second


def row_iota(rows):
    return lax.broadcasted_iota(jnp.int32, (rows, LANES), 0)


def total_of(value):
    return jnp.sum(jnp.sum(value, axis=0, keepdims=True), axis=1, keepdims=True)


def least_squares(columns, heights, beta):
    zero = jnp.zeros_like(beta)
    size = len(columns)
    table = [[zero] * size for _ in range(size + 1)]
    for k in range(size):
        for i in range(k + 1):
            table[i][k] = columns[k][i]
        table[k + 1][k] = heights[k]
    target = [beta] + [zero] * size
    for c in range(size):
        lead, second = table[c][c], table[c + 1][c]
        radius = jnp.sqrt(lead * lead + second * second)
        cosine, sine = lead / radius, second / radius
        top, low = table[c], table[c + 1]
        new_top = [cosine * t + sine * l for t, l in zip(top, low)]
        new_low = [cosine * l - sine * t for t, l in zip(top, low)]
        table[c], table[c + 1] = new_top, new_low
        a, b = target[c], target[c + 1]
        target[c], target[c + 1] = cosine * a + sine * b, cosine * b - sine * a
    y = [zero] * size
    for r in reversed(range(size)):
        partial = zero
        for c in range(r + 1, size):
            partial = partial + table[r][c] * y[c]
        y[r] = (target[r] - partial) / table[r][r]
    return y


def kernel(
    pos_ref, area_ref, rhs_ref, sol_ref, res_ref, hes_ref,
    plane_in, column_in, matrix, sf, tf, coef, phi, psi,
    plane_w, column_p, plane_u, column_u, norm_in, hes, inverse,
    send_sem, plane_sem, column_sem, norm_sem,
):
    my_z = lax.axis_index("z")
    my_p = lax.axis_index("p")
    sources = PLANE * LANES

    def plane_peer(step):
        return (my_z, lax.rem(my_p + step, PLANE))

    def column_peer(step):
        return (lax.rem(my_z + step, DEPTH), my_p)

    barrier = pltpu.get_barrier_semaphore()

    def greet_plane(step, carry):
        pl.semaphore_signal(barrier, inc=1, device_id=plane_peer(step), device_id_type=MESH)
        return carry

    def greet_column(step, carry):
        pl.semaphore_signal(barrier, inc=1, device_id=column_peer(step), device_id_type=MESH)
        return carry

    lax.fori_loop(1, PLANE, greet_plane, 0)
    lax.fori_loop(1, DEPTH, greet_column, 0)
    own = jnp.concatenate(
        [pos_ref[...], area_ref[...], rhs_ref[...], jnp.zeros((1, LANES), F32)], axis=0
    )
    plane_in[my_p] = own
    column_in[my_z] = own
    hes[...] = jnp.zeros_like(hes)
    inverse[...] = jnp.zeros_like(inverse)
    plane_u[...] = jnp.zeros_like(plane_u)
    column_u[...] = jnp.zeros_like(column_u)
    pl.semaphore_wait(barrier, PLANE - 1 + DEPTH - 1)

    def to_plane(ref, recv_sem, slot):
        def send(step, carry):
            pltpu.make_async_remote_copy(
                src_ref=ref.at[my_p], dst_ref=ref.at[my_p],
                send_sem=send_sem.at[slot], recv_sem=recv_sem,
                device_id=plane_peer(step), device_id_type=MESH,
            ).start()
            return carry
        lax.fori_loop(1, PLANE, send, 0, unroll=True)

    def to_column(ref, recv_sem, slot):
        def send(step, carry):
            pltpu.make_async_remote_copy(
                src_ref=ref.at[my_z], dst_ref=ref.at[my_z],
                send_sem=send_sem.at[slot], recv_sem=recv_sem,
                device_id=column_peer(step), device_id_type=MESH,
            ).start()
            return carry
        lax.fori_loop(1, DEPTH, send, 0, unroll=True)

    def all_of(ref, count, recv_sem, slot):
        part = ref.at[pl.ds(0, count - 1)]
        return pltpu.make_async_remote_copy(
            src_ref=part, dst_ref=part, send_sem=send_sem.at[slot], recv_sem=recv_sem,
            device_id=(my_z, my_p), device_id_type=MESH,
        )

    to_column(column_in, column_sem.at[ITERS], 0)
    to_plane(plane_in, plane_sem.at[ITERS], 1)

    all_of(column_in, DEPTH, column_sem.at[ITERS], 0).wait()
    rows8, rows16 = row_iota(8), row_iota(16)
    for t in range(DEPTH):
        block = column_in[t]
        lanes = pl.ds(t * LANES, LANES)
        x = [block[b:b + 1] for b in range(3)]
        square = x[0] * x[0] + x[1] * x[1] + x[2] * x[2]
        feature = jnp.where(
            rows8 < 3, -2.0 * block,
            jnp.where(rows8 == 3, 1.0, jnp.where(rows8 == 4, square + soften, 0.0)),
        )
        t1, t2, t3 = split3(feature)
        tf[0:16, lanes] = jnp.concatenate([t1, t1], axis=0).astype(BF16)
        tf[16:32, lanes] = jnp.concatenate([t2, t1], axis=0).astype(BF16)
        tf[32:48, lanes] = jnp.concatenate([t3, t2], axis=0).astype(BF16)
        for a in range(3):
            value = jnp.zeros((16, LANES), F32)
            for b in range(3):
                value = jnp.where(rows16 == b, x[a] * x[b] + (square if a == b else 0.0), value)
                for c in range(3):
                    part = jnp.zeros((1, LANES), F32)
                    if c == a:
                        part = part - 2.0 * x[b]
                    if b == c:
                        part = part - x[a]
                    if b == a:
                        part = part - x[c]
                    value = jnp.where(rows16 == 3 + 3 * b + c, part, value)
            phi[a, :, lanes] = jnp.where(rows16 == 12 + a, 1.0, value)
            column_u[0, a * DEPTH + t:a * DEPTH + t + 1, :] = block[4 + a:5 + a]

    all_of(plane_in, PLANE, plane_sem.at[ITERS], 1).wait()
    scale = float(PLANE * DEPTH * LANES) ** (-0.5)

    def one_source_block(s, carry):
        block = plane_in[s]
        lanes = pl.ds(pl.multiple_of(s * LANES, LANES), LANES)
        y = [block[b:b + 1] for b in range(3)]
        weight = block[3:4] * scale
        square = y[0] * y[0] + y[1] * y[1] + y[2] * y[2]
        feature = jnp.where(
            rows8 < 3, block, jnp.where(rows8 == 3, square, jnp.where(rows8 == 4, 1.0, 0.0))
        )
        m1, m2, m3 = split3(feature)
        sf[0:16, lanes] = jnp.concatenate([m1, m2], axis=0).astype(BF16)
        sf[16:32, lanes] = jnp.concatenate([m1, m3], axis=0).astype(BF16)
        sf[32:48, lanes] = jnp.concatenate([m1, m2], axis=0).astype(BF16)
        chosen = jnp.zeros((16, LANES), F32)
        for b in range(3):
            mine = ((rows16 >= 3 + 3 * b) & (rows16 < 6 + 3 * b)) | (rows16 == 12 + b)
            chosen = jnp.where(mine, y[b], chosen)
        for b in range(3):
            linear = (rows16 == 3 + b) | (rows16 == 6 + b) | (rows16 == 9 + b)
            last = (rows16 >= 12) & (rows16 < 15)
            value = jnp.where(
                rows16 == b, 1.0, jnp.where(linear, chosen, jnp.where(last, chosen * y[b], 0.0))
            )
            value = value + jnp.where(rows16 == 12 + b, square + 2.0 * soften, 0.0)
            coef[b, :, lanes] = value * weight
        plane_u[0, s] = block[4:8]
        return carry

    lax.fori_loop(0, PLANE, one_source_block, 0)

    chunk = 512

    def factor_block(t, carry):
        targets = tf[:, pl.ds(pl.multiple_of(t * LANES, LANES), LANES)]
        for s in range(sources // chunk):
            lanes = slice(s * chunk, (s + 1) * chunk)
            square = lax.dot_general(
                targets, sf[:, lanes], (((0,), (0,)), ((), ())), preferred_element_type=F32
            )
            root = lax.rsqrt(square)
            factor = root * root * root
            high = factor.astype(BF16)
            matrix[t, 0:LANES, lanes] = high
            matrix[t, LANES:2 * LANES, lanes] = (factor - high.astype(F32)).astype(BF16)
        return carry

    lax.fori_loop(0, DEPTH, factor_block, 0)

    lane_row = lax.broadcasted_iota(jnp.int32, (1, LANES), 1)
    hes_rows, hes_lanes = row_iota(8), lax.broadcasted_iota(jnp.int32, (8, LANES), 1)

    def one_step(k, carry):
        for s in range(PLANE):
            lanes = slice(s * LANES, (s + 1) * LANES)
            block = plane_u[k, s]
            value = (
                coef[0, :, lanes] * block[0:1]
                + coef[1, :, lanes] * block[1:2]
                + coef[2, :, lanes] * block[2:3]
            )
            p1, p2, p3 = split3(value)
            psi[0:16, lanes] = p1.astype(BF16)
            psi[16:32, lanes] = p2.astype(BF16)
            psi[32:48, lanes] = p3.astype(BF16)

        def image_block(t, inner):
            product = lax.dot_general(
                matrix[t], psi[...], (((1,), (1,)), ((), ())), preferred_element_type=F32
            )
            both = product[0:LANES] + product[LANES:2 * LANES]
            turned = both.T
            summed = turned[0:16] + turned[16:32] + turned[32:48]
            lanes = pl.ds(pl.multiple_of(t * LANES, LANES), LANES)
            for a in range(3):
                column_p[k, my_z, pl.ds(a * DEPTH + t, 1), :] = jnp.sum(
                    phi[a, :, lanes] * summed, axis=0, keepdims=True
                )
            return inner

        lax.fori_loop(0, DEPTH, image_block, 0)

        to_column(column_p.at[k], column_sem.at[k], 0)
        latest = column_u[k]
        all_of(column_p.at[k], DEPTH, column_sem.at[k], 0).wait()
        applied = latest
        for z in range(DEPTH):
            applied = applied + column_p[k, z]
        column_u[k + 1] = applied
        message = jnp.where(lane_row == 4, total_of(latest * latest), 0.0)
        for i in range(ITERS):
            message = message + jnp.where(lane_row == i, total_of(column_u[i] * applied), 0.0) * (
                jnp.where(i <= k, 1.0, 0.0)
            )
        for a in range(3):
            plane_w[k, my_p, a:a + 1, :] = column_u[k + 1, pl.ds(a * DEPTH + my_z, 1), :]
        plane_w[k, my_p, 3:4, :] = message
        to_plane(plane_w.at[k], plane_sem.at[k], 1)
        all_of(plane_w.at[k], PLANE, plane_sem.at[k], 1).wait()
        sums = jnp.sum(plane_w[k, :, 3, :], axis=0, keepdims=True)
        norm = jnp.sqrt(sums[:, 4:5])
        scaled = 1.0 / norm
        inverse[pl.ds(k, 1), :] = jnp.broadcast_to(scaled, (1, LANES))
        table = jnp.where((hes_rows == k) & (hes_lanes == k - 1), norm, hes[0:8])
        factors = []
        for i in range(ITERS):
            present = inverse[i:i + 1, 0:1]
            value = sums[:, i:i + 1] * present * scaled
            table = jnp.where((hes_rows == i) & (hes_lanes == k), value, table)
            factors.append(value * present)
        hes[0:8] = table
        hes[8:9] = jnp.where(k == 0, jnp.broadcast_to(norm, (1, LANES)), hes[8:9])
        fresh = applied * scaled
        for i in range(ITERS):
            fresh = fresh - jnp.where(i <= k, factors[i] * column_u[i], 0.0)
        column_u[k + 1] = fresh
        for s in range(PLANE):
            fresh = plane_w[k, s] * scaled
            for i in range(ITERS):
                fresh = fresh - factors[i] * plane_u[i, s]
            plane_u[k + 1, s] = fresh
        return carry

    lax.fori_loop(0, ITERS, one_step, 0)

    last = column_u[ITERS]
    norm_in[my_p] = jnp.broadcast_to(total_of(last * last), (8, LANES))
    to_plane(norm_in, norm_sem, 1)
    all_of(norm_in, PLANE, norm_sem, 1).wait()
    sums = jnp.sum(norm_in[:, 0, :], axis=0, keepdims=True)
    norm = jnp.sqrt(sums[:, 0:1])
    inverse[ITERS:ITERS + 1, :] = jnp.broadcast_to(1.0 / norm, (1, LANES))
    table = jnp.where((hes_rows == ITERS) & (hes_lanes == ITERS - 1), norm, hes[0:8])
    hes_ref[...] = table[0:ITERS + 1, 0:ITERS]
    entry = [[table[i:i + 1, k:k + 1] for k in range(ITERS)] for i in range(ITERS + 1)]
    beta = hes[8:9, 0:1]
    y = least_squares(
        [[entry[i][k] for i in range(k + 1)] for k in range(ITERS)],
        [entry[k + 1][k] for k in range(ITERS)],
        beta,
    )
    for a in range(3):
        solved = jnp.zeros((1, LANES), F32)
        misfit = jnp.zeros((1, LANES), F32)
        for i in range(ITERS + 1):
            basis = column_u[i, pl.ds(a * DEPTH + my_z, 1), :] * inverse[i:i + 1, :]
            if i < ITERS:
                solved = solved + y[i] * basis
            g = beta if i == 0 else jnp.zeros_like(beta)
            for k in range(max(i - 1, 0), ITERS):
                g = g - entry[i][k] * y[k]
            misfit = misfit + g * basis
        sol_ref[a:a + 1, :] = solved
        res_ref[a:a + 1, :] = misfit


def shards(positions, areas, right_side):
    vmem = pl.BlockSpec(memory_space=pltpu.VMEM)
    sources, targets = PLANE * LANES, DEPTH * LANES
    return pl.pallas_call(
        kernel,
        out_shape=(
            jax.ShapeDtypeStruct((3, LANES), F32),
            jax.ShapeDtypeStruct((3, LANES), F32),
            jax.ShapeDtypeStruct((ITERS + 1, ITERS), F32),
        ),
        in_specs=[vmem] * 3,
        out_specs=(vmem,) * 3,
        scratch_shapes=[
            pltpu.VMEM((PLANE, 8, LANES), F32),
            pltpu.VMEM((DEPTH, 8, LANES), F32),
            pltpu.VMEM((DEPTH, 2 * LANES, sources), BF16),
            pltpu.VMEM((48, sources), BF16),
            pltpu.VMEM((48, targets), BF16),
            pltpu.VMEM((3, 16, sources), F32),
            pltpu.VMEM((3, 16, targets), F32),
            pltpu.VMEM((48, sources), BF16),
            pltpu.VMEM((ITERS, PLANE, 4, LANES), F32),
            pltpu.VMEM((ITERS, DEPTH, 3 * DEPTH, LANES), F32),
            pltpu.VMEM((ITERS + 1, PLANE, 4, LANES), F32),
            pltpu.VMEM((ITERS + 1, 3 * DEPTH, LANES), F32),
            pltpu.VMEM((PLANE, 8, LANES), F32),
            pltpu.VMEM((16, LANES), F32),
            pltpu.VMEM((8, LANES), F32),
            pltpu.SemaphoreType.DMA((2,)),
            pltpu.SemaphoreType.DMA((ITERS + 1,)),
            pltpu.SemaphoreType.DMA((ITERS + 1,)),
            pltpu.SemaphoreType.DMA,
        ],
        compiler_params=pltpu.CompilerParams(
            collective_id=0, has_side_effects=True, vmem_limit_bytes=56 * 1024 * 1024
        ),
        name="arnoldi",
    )(positions, areas.reshape(1, -1), right_side)


def solution(mesh):
    split = Mesh(mesh.devices.reshape(DEPTH, PLANE), ("z", "p"))
    return jax.shard_map(
        shards,
        mesh=split,
        in_specs=(P(None, ("z", "p")), P(("z", "p")), P(None, ("z", "p"))),
        out_specs=(P(None, ("z", "p")), P(None, ("z", "p")), P()),
        check_vma=False,
    )
```

```python
import functools

import jax
import jax.numpy as jnp
from jax import lax
from jax.experimental import pallas as pl
from jax.experimental.pallas import tpu as pltpu
from jax.sharding import Mesh
from jax.sharding import PartitionSpec as P

ITERS = 4
soften = 0.0025
LANES = 128
WIDE = 256
CHUNK = 256
DEPTH = 8
PLANE = 32
BLOCKS = DEPTH * LANES // WIDE
MESH = pl.DeviceIdType.MESH
F32 = jnp.float32
BF16 = jnp.bfloat16


def split3(value):
    first = value.astype(BF16).astype(F32)
    rest = value - first
    second = rest.astype(BF16).astype(F32)
    return first, second, rest - second


def row_iota(rows):
    return lax.broadcasted_iota(jnp.int32, (rows, LANES), 0)


def total_of(value):
    return jnp.sum(jnp.sum(value, axis=0, keepdims=True), axis=1, keepdims=True)


def least_squares(columns, heights, beta):
    zero = jnp.zeros_like(beta)
    size = len(columns)
    table = [[zero] * size for _ in range(size + 1)]
    for k in range(size):
        for i in range(k + 1):
            table[i][k] = columns[k][i]
        table[k + 1][k] = heights[k]
    target = [beta] + [zero] * size
    for c in range(size):
        lead, second = table[c][c], table[c + 1][c]
        radius = jnp.sqrt(lead * lead + second * second)
        cosine, sine = lead / radius, second / radius
        top, low = table[c], table[c + 1]
        new_top = [cosine * t + sine * l for t, l in zip(top, low)]
        new_low = [cosine * l - sine * t for t, l in zip(top, low)]
        table[c], table[c + 1] = new_top, new_low
        a, b = target[c], target[c + 1]
        target[c], target[c + 1] = cosine * a + sine * b, cosine * b - sine * a
    y = [zero] * size
    for r in reversed(range(size)):
        partial = zero
        for c in range(r + 1, size):
            partial = partial + table[r][c] * y[c]
        y[r] = (target[r] - partial) / table[r][r]
    return y


def kernel(
    pos_ref, area_ref, rhs_ref, packed_ref,
    plane_in, column_in, matrix, sf, tf, coef, phi, psi,
    plane_w, column_p, plane_u, column_u, gram, hes, inverse,
    send_sem, plane_sem, column_sem,
):
    my_z = lax.axis_index("z")
    my_p = lax.axis_index("p")
    sources = PLANE * LANES

    def plane_peer(step):
        return (my_z, lax.rem(my_p + step, PLANE))

    def column_peer(step):
        return (lax.rem(my_z + step, DEPTH), my_p)

    barrier = pltpu.get_barrier_semaphore()

    def greet_plane(step, carry):
        pl.semaphore_signal(barrier, inc=1, device_id=plane_peer(step), device_id_type=MESH)
        return carry

    def greet_column(step, carry):
        pl.semaphore_signal(barrier, inc=1, device_id=column_peer(step), device_id_type=MESH)
        return carry

    lax.fori_loop(1, PLANE, greet_plane, 0)
    lax.fori_loop(1, DEPTH, greet_column, 0)
    own = jnp.concatenate(
        [pos_ref[...], area_ref[...], rhs_ref[...], jnp.zeros((1, LANES), F32)], axis=0
    )
    plane_in[my_p] = own
    column_in[my_z] = own
    hes[...] = jnp.zeros_like(hes)
    inverse[...] = jnp.zeros_like(inverse)
    plane_u[...] = jnp.zeros_like(plane_u)
    column_u[...] = jnp.zeros_like(column_u)
    pl.semaphore_wait(barrier, PLANE - 1 + DEPTH - 1)

    def to_plane(ref, recv_sem, slot):
        def send(step, carry):
            pltpu.make_async_remote_copy(
                src_ref=ref.at[my_p], dst_ref=ref.at[my_p],
                send_sem=send_sem.at[slot], recv_sem=recv_sem,
                device_id=plane_peer(step), device_id_type=MESH,
            ).start()
            return carry
        lax.fori_loop(1, PLANE, send, 0, unroll=True)

    def to_column(ref, recv_sem, slot):
        def send(step, carry):
            pltpu.make_async_remote_copy(
                src_ref=ref.at[my_z], dst_ref=ref.at[my_z],
                send_sem=send_sem.at[slot], recv_sem=recv_sem,
                device_id=column_peer(step), device_id_type=MESH,
            ).start()
            return carry
        lax.fori_loop(1, DEPTH, send, 0, unroll=True)

    def all_of(ref, count, recv_sem, slot):
        part = ref.at[pl.ds(0, count - 1)]
        return pltpu.make_async_remote_copy(
            src_ref=part, dst_ref=part, send_sem=send_sem.at[slot], recv_sem=recv_sem,
            device_id=(my_z, my_p), device_id_type=MESH,
        )

    to_column(column_in, column_sem.at[ITERS], 0)
    to_plane(plane_in, plane_sem.at[ITERS], 1)

    all_of(column_in, DEPTH, column_sem.at[ITERS], 0).wait()
    rows8, rows16 = row_iota(8), row_iota(16)
    for t in range(DEPTH):
        block = column_in[t]
        lanes = pl.ds(t * LANES, LANES)
        x = [block[b:b + 1] for b in range(3)]
        square = x[0] * x[0] + x[1] * x[1] + x[2] * x[2]
        feature = jnp.where(
            rows8 < 3, -2.0 * block,
            jnp.where(rows8 == 3, 1.0, jnp.where(rows8 == 4, square + soften, 0.0)),
        )
        t1, t2, t3 = split3(feature)
        tf[0:16, lanes] = jnp.concatenate([t1, t1], axis=0).astype(BF16)
        tf[16:32, lanes] = jnp.concatenate([t2, t1], axis=0).astype(BF16)
        tf[32:48, lanes] = jnp.concatenate([t3, t2], axis=0).astype(BF16)
        for a in range(3):
            value = jnp.zeros((16, LANES), F32)
            for b in range(3):
                value = jnp.where(rows16 == b, x[a] * x[b] + (square if a == b else 0.0), value)
                for c in range(3):
                    part = jnp.zeros((1, LANES), F32)
                    if c == a:
                        part = part - 2.0 * x[b]
                    if b == c:
                        part = part - x[a]
                    if b == a:
                        part = part - x[c]
                    value = jnp.where(rows16 == 3 + 3 * b + c, part, value)
            phi[a, :, lanes] = jnp.where(rows16 == 12 + a, 1.0, value)
            column_u[0, a * DEPTH + t:a * DEPTH + t + 1, :] = block[4 + a:5 + a]

    all_of(plane_in, PLANE, plane_sem.at[ITERS], 1).wait()
    scale = float(PLANE * DEPTH * LANES) ** (-0.5)

    def one_source_block(s, carry):
        block = plane_in[s]
        lanes = pl.ds(pl.multiple_of(s * LANES, LANES), LANES)
        y = [block[b:b + 1] for b in range(3)]
        weight = block[3:4] * scale
        square = y[0] * y[0] + y[1] * y[1] + y[2] * y[2]
        feature = jnp.where(
            rows8 < 3, block, jnp.where(rows8 == 3, square, jnp.where(rows8 == 4, 1.0, 0.0))
        )
        m1, m2, m3 = split3(feature)
        sf[0:16, lanes] = jnp.concatenate([m1, m2], axis=0).astype(BF16)
        sf[16:32, lanes] = jnp.concatenate([m1, m3], axis=0).astype(BF16)
        sf[32:48, lanes] = jnp.concatenate([m1, m2], axis=0).astype(BF16)
        chosen = jnp.zeros((16, LANES), F32)
        for b in range(3):
            mine = ((rows16 >= 3 + 3 * b) & (rows16 < 6 + 3 * b)) | (rows16 == 12 + b)
            chosen = jnp.where(mine, y[b], chosen)
        for b in range(3):
            linear = (rows16 == 3 + b) | (rows16 == 6 + b) | (rows16 == 9 + b)
            last = (rows16 >= 12) & (rows16 < 15)
            value = jnp.where(
                rows16 == b, 1.0, jnp.where(linear, chosen, jnp.where(last, chosen * y[b], 0.0))
            )
            value = value + jnp.where(rows16 == 12 + b, square + 2.0 * soften, 0.0)
            coef[b, :, lanes] = value * weight
        plane_u[0, s] = block[4:8]
        return carry

    lax.fori_loop(0, PLANE, one_source_block, 0)

    def factor_block(s, carry):
        rows = pl.ds(pl.multiple_of(s * CHUNK, CHUNK), CHUNK)
        for b in range(BLOCKS):
            square = lax.dot_general(
                sf[:, rows], tf[:, b * WIDE:(b + 1) * WIDE], (((0,), (0,)), ((), ())),
                preferred_element_type=F32,
            )
            root = lax.rsqrt(square)
            factor = root * root * root
            high = factor.astype(BF16)
            matrix[b, rows, 0:WIDE] = high
            matrix[b, rows, WIDE:2 * WIDE] = (factor - high.astype(F32)).astype(BF16)
        return carry

    lax.fori_loop(0, sources // CHUNK, factor_block, 0)

    lane_row = lax.broadcasted_iota(jnp.int32, (1, LANES), 1)
    hes_rows, hes_lanes = row_iota(8), lax.broadcasted_iota(jnp.int32, (8, LANES), 1)

    def one_step(k, carry):
        for s in range(PLANE):
            lanes = slice(s * LANES, (s + 1) * LANES)
            block = plane_u[k, s]
            value = (
                coef[0, :, lanes] * block[0:1]
                + coef[1, :, lanes] * block[1:2]
                + coef[2, :, lanes] * block[2:3]
            )
            p1, p2, p3 = split3(value)
            psi[0:16, lanes] = p1.astype(BF16)
            psi[16:32, lanes] = p2.astype(BF16)
            psi[32:48, lanes] = p3.astype(BF16)

        for b in range(BLOCKS):
            product = lax.dot_general(
                psi[...], matrix[b], (((1,), (0,)), ((), ())), preferred_element_type=F32
            )
            both = product[:, 0:WIDE] + product[:, WIDE:2 * WIDE]
            summed = both[0:16] + both[16:32] + both[32:48]
            for a in range(3):
                row = jnp.sum(
                    phi[a, :, b * WIDE:(b + 1) * WIDE] * summed, axis=0, keepdims=True
                )
                for c in range(WIDE // LANES):
                    t = b * (WIDE // LANES) + c
                    column_p[k, my_z, a * DEPTH + t:a * DEPTH + t + 1, :] = (
                        row[:, c * LANES:(c + 1) * LANES]
                    )

        to_column(column_p.at[k], column_sem.at[k], 0)
        latest = column_u[k]
        message = jnp.where(lane_row == 6, total_of(latest * latest), 0.0)
        for i in range(ITERS):
            part = jnp.where(lane_row == 8 + i, total_of(column_u[i] * latest), 0.0)
            message = message + part
        all_of(column_p.at[k], DEPTH, column_sem.at[k], 0).wait()
        applied = latest
        for z in range(DEPTH):
            applied = applied + column_p[k, z]
        message = message + jnp.where(lane_row == 4, total_of(applied * applied), 0.0)
        for i in range(ITERS):
            message = message + jnp.where(lane_row == i, total_of(column_u[i] * applied), 0.0)
        column_u[k + 1] = applied
        for a in range(3):
            plane_w[k, my_p, a:a + 1, :] = column_u[k + 1, pl.ds(a * DEPTH + my_z, 1), :]
        plane_w[k, my_p, 3:4, :] = message
        to_plane(plane_w.at[k], plane_sem.at[k], 1)
        all_of(plane_w.at[k], PLANE, plane_sem.at[k], 1).wait()
        sums = jnp.sum(plane_w[k, :, 3, :], axis=0, keepdims=True)
        gram[pl.ds(k, 1), :] = sums
        norm = jnp.sqrt(sums[:, 6:7])
        scaled = 1.0 / norm
        inverse[pl.ds(k, 1), :] = jnp.broadcast_to(scaled, (1, LANES))
        table = jnp.where((hes_rows == k) & (hes_lanes == k - 1), norm, hes[0:8])
        factors = []
        for i in range(ITERS):
            present = inverse[i:i + 1, 0:1]
            value = sums[:, i:i + 1] * present * scaled
            table = jnp.where((hes_rows == i) & (hes_lanes == k), value, table)
            factors.append(value * present)
        hes[0:8] = table
        hes[8:9] = jnp.where(k == 0, jnp.broadcast_to(norm, (1, LANES)), hes[8:9])
        fresh = applied * scaled
        for i in range(ITERS):
            fresh = fresh - jnp.where(i <= k, factors[i] * column_u[i], 0.0)
        column_u[k + 1] = fresh
        for s in range(PLANE):
            fresh = plane_w[k, s] * scaled
            for i in range(ITERS):
                fresh = fresh - factors[i] * plane_u[i, s]
            plane_u[k + 1, s] = fresh
        return carry

    lax.fori_loop(0, ITERS, one_step, 0)

    present = [inverse[i:i + 1, 0:1] for i in range(ITERS)]
    tall = [hes[i:i + 1, ITERS - 1:ITERS] for i in range(ITERS)]
    whole = gram[ITERS - 1:ITERS, 4:5] * present[-1] * present[-1]
    square = whole
    for i in range(ITERS):
        square = square - tall[i] * tall[i]
        for j in range(i + 1, ITERS):
            square = square + 2.0 * (tall[i] * present[i]) * (tall[j] * present[j]) * (
                gram[j:j + 1, 8 + i:9 + i]
            )
    norm = jnp.sqrt(jnp.maximum(square, whole * 1e-14))
    inverse[ITERS:ITERS + 1, :] = jnp.broadcast_to(1.0 / norm, (1, LANES))
    table = jnp.where((hes_rows == ITERS) & (hes_lanes == ITERS - 1), norm, hes[0:8])
    packed_ref[8:16] = table
    entry = [[table[i:i + 1, k:k + 1] for k in range(ITERS)] for i in range(ITERS + 1)]
    beta = hes[8:9, 0:1]
    y = least_squares(
        [[entry[i][k] for i in range(k + 1)] for k in range(ITERS)],
        [entry[k + 1][k] for k in range(ITERS)],
        beta,
    )
    for a in range(3):
        solved = jnp.zeros((1, LANES), F32)
        misfit = jnp.zeros((1, LANES), F32)
        for i in range(ITERS + 1):
            basis = column_u[i, pl.ds(a * DEPTH + my_z, 1), :] * inverse[i:i + 1, :]
            if i < ITERS:
                solved = solved + y[i] * basis
            g = beta if i == 0 else jnp.zeros_like(beta)
            for k in range(max(i - 1, 0), ITERS):
                g = g - entry[i][k] * y[k]
            misfit = misfit + g * basis
        packed_ref[a:a + 1, :] = solved
        packed_ref[4 + a:5 + a, :] = misfit


def unpack(packed_ref, sol_ref, res_ref, hes_ref):
    sol_ref[...] = packed_ref[0:3]
    res_ref[...] = packed_ref[4:7]
    hes_ref[...] = packed_ref[8:16].T[0:ITERS, 0:ITERS + 1]


def shards(positions, areas, right_side):
    vmem = pl.BlockSpec(memory_space=pltpu.VMEM)
    sources, targets = PLANE * LANES, DEPTH * LANES
    packed = pl.pallas_call(
        kernel,
        out_shape=jax.ShapeDtypeStruct((16, LANES), F32),
        in_specs=[vmem] * 3,
        out_specs=vmem,
        scratch_shapes=[
            pltpu.VMEM((PLANE, 8, LANES), F32),
            pltpu.VMEM((DEPTH, 8, LANES), F32),
            pltpu.VMEM((BLOCKS, sources, 2 * WIDE), BF16),
            pltpu.VMEM((48, sources), BF16),
            pltpu.VMEM((48, targets), BF16),
            pltpu.VMEM((3, 16, sources), F32),
            pltpu.VMEM((3, 16, targets), F32),
            pltpu.VMEM((48, sources), BF16),
            pltpu.VMEM((ITERS, PLANE, 4, LANES), F32),
            pltpu.VMEM((ITERS, DEPTH, 3 * DEPTH, LANES), F32),
            pltpu.VMEM((ITERS + 1, PLANE, 4, LANES), F32),
            pltpu.VMEM((ITERS + 1, 3 * DEPTH, LANES), F32),
            pltpu.VMEM((8, LANES), F32),
            pltpu.VMEM((16, LANES), F32),
            pltpu.VMEM((8, LANES), F32),
            pltpu.SemaphoreType.DMA((2,)),
            pltpu.SemaphoreType.DMA((ITERS + 1,)),
            pltpu.SemaphoreType.DMA((ITERS + 1,)),
        ],
        compiler_params=pltpu.CompilerParams(
            collective_id=0, has_side_effects=True, vmem_limit_bytes=56 * 1024 * 1024
        ),
        name="arnoldi",
    )(positions, areas.reshape(1, -1), right_side)
    solved, misfit, turned = pl.pallas_call(
        unpack,
        out_shape=(
            jax.ShapeDtypeStruct((3, LANES), F32),
            jax.ShapeDtypeStruct((3, LANES), F32),
            jax.ShapeDtypeStruct((ITERS, ITERS + 1), F32),
        ),
        in_specs=[vmem],
        out_specs=(vmem,) * 3,
        name="unpack",
    )(packed)
    return solved, misfit, turned.T


def solution(mesh):
    split = Mesh(mesh.devices.reshape(DEPTH, PLANE), ("z", "p"))
    return jax.shard_map(
        shards,
        mesh=split,
        in_specs=(P(None, ("z", "p")), P(("z", "p")), P(None, ("z", "p"))),
        out_specs=(P(None, ("z", "p")), P(None, ("z", "p")), P()),
        check_vma=False,
    )
```

```python
import functools

import jax
import jax.numpy as jnp
from jax import lax
from jax.experimental import pallas as pl
from jax.experimental.pallas import tpu as pltpu
from jax.sharding import Mesh
from jax.sharding import PartitionSpec as P

ITERS = 4
soften = 0.0025
LANES = 128
WIDE = 256
CHUNK = 512
DEEP = 1024
DEPTH = 8
PLANE = 32
BLOCKS = DEPTH * LANES // WIDE
MESH = pl.DeviceIdType.MESH
F32 = jnp.float32
BF16 = jnp.bfloat16


def split3(value):
    first = value.astype(BF16).astype(F32)
    rest = value - first
    second = rest.astype(BF16).astype(F32)
    return first, second, rest - second


def row_iota(rows):
    return lax.broadcasted_iota(jnp.int32, (rows, LANES), 0)


def total_of(value):
    return jnp.sum(jnp.sum(value, axis=0, keepdims=True), axis=1, keepdims=True)


def least_squares(columns, heights, beta):
    zero = jnp.zeros_like(beta)
    size = len(columns)
    table = [[zero] * size for _ in range(size + 1)]
    for k in range(size):
        for i in range(k + 1):
            table[i][k] = columns[k][i]
        table[k + 1][k] = heights[k]
    target = [beta] + [zero] * size
    for c in range(size):
        lead, second = table[c][c], table[c + 1][c]
        radius = jnp.sqrt(lead * lead + second * second)
        cosine, sine = lead / radius, second / radius
        top, low = table[c], table[c + 1]
        new_top = [cosine * t + sine * l for t, l in zip(top, low)]
        new_low = [cosine * l - sine * t for t, l in zip(top, low)]
        table[c], table[c + 1] = new_top, new_low
        a, b = target[c], target[c + 1]
        target[c], target[c + 1] = cosine * a + sine * b, cosine * b - sine * a
    y = [zero] * size
    for r in reversed(range(size)):
        partial = zero
        for c in range(r + 1, size):
            partial = partial + table[r][c] * y[c]
        y[r] = (target[r] - partial) / table[r][r]
    return y


def kernel(
    pos_ref, area_ref, rhs_ref, packed_ref,
    plane_in, column_in, matrix, sf, tf, coef, phi, psi, image,
    plane_w, column_w, part_out, part_in, part_all, plane_u, column_u, gram, hes, inverse,
    load_sem, send_sem, plane_sem, column_sem, part_sem,
):
    my_z = lax.axis_index("z")
    my_p = lax.axis_index("p")
    my_y, my_x = my_p // 8, (my_p % 2) * 2 + (my_p // 4) % 2
    my_c = (my_p // 2) % 2
    sources = PLANE * LANES

    ys = [((my_y + d) % 4) * 8 for d in range(4)]
    xs = [((my_x + d) % 4) for d in range(4)]
    xs = [(x % 2) * 4 + x // 2 for x in xs]
    cs = [((my_c + d) % 2) * 2 for d in range(2)]
    hops = (0, 1, 2, 1)
    steps = [(a, b, c) for a in range(4) for b in range(4) for c in range(2)][1:]
    steps.sort(key=lambda s: -(4 * (hops[s[0]] + hops[s[1]]) + s[2]))
    plane_peers = [(s[0], (my_z, ys[s[0]] + xs[s[1]] + cs[s[2]])) for s in steps]
    column_peers = [((my_z + d) % DEPTH, my_p) for d in (4, 3, 5, 2, 6, 1, 7)]

    barrier = pltpu.get_barrier_semaphore()
    for device in column_peers + [peer for _, peer in plane_peers]:
        pl.semaphore_signal(barrier, inc=1, device_id=device, device_id_type=MESH)
    own = plane_in.at[my_p]
    loads = [
        pltpu.make_async_copy(pos_ref, own.at[0:3], load_sem.at[0]),
        pltpu.make_async_copy(area_ref, own.at[3:4], load_sem.at[1]),
        pltpu.make_async_copy(rhs_ref, own.at[4:7], load_sem.at[2]),
    ]
    for load in loads:
        load.start()
    plane_in[my_p, 7:8, :] = jnp.zeros((1, LANES), F32)
    hes[...] = jnp.zeros_like(hes)
    inverse[...] = jnp.zeros_like(inverse)
    plane_u[...] = jnp.zeros_like(plane_u)
    column_u[...] = jnp.zeros_like(column_u)
    part_out[...] = jnp.zeros_like(part_out)
    for load in loads:
        load.wait()
    pl.semaphore_wait(barrier, PLANE - 1 + DEPTH - 1)

    def send(src, dst, device, slot, recv_sem):
        pltpu.make_async_remote_copy(
            src_ref=src, dst_ref=dst, send_sem=send_sem.at[slot], recv_sem=recv_sem,
            device_id=device, device_id_type=MESH,
        ).start()

    def arrived(part, recv_sem):
        pltpu.make_async_remote_copy(
            src_ref=part, dst_ref=part, send_sem=send_sem.at[0], recv_sem=recv_sem,
            device_id=(my_z, my_p), device_id_type=MESH,
        ).wait_recv()

    def sent(part, slot):
        pltpu.make_async_remote_copy(
            src_ref=part, dst_ref=part, send_sem=send_sem.at[slot], recv_sem=load_sem.at[0],
            device_id=(my_z, my_p), device_id_type=MESH,
        ).wait_send()

    for device in column_peers:
        send(own, column_in.at[my_z], device, 0, column_sem.at[ITERS])
    for turn, device in plane_peers:
        send(own, own, device, 1, plane_sem.at[ITERS + (4 - turn) % 4])
    column_in[my_z] = plane_in[my_p]

    rows8, rows16 = row_iota(8), row_iota(16)
    scale = float(PLANE * DEPTH * LANES) ** (-0.5)

    def one_source_block(s):
        block = plane_in[s]
        lanes = pl.ds(pl.multiple_of(s * LANES, LANES), LANES)
        y = [block[b:b + 1] for b in range(3)]
        weight = block[3:4] * scale
        square = y[0] * y[0] + y[1] * y[1] + y[2] * y[2]
        feature = jnp.where(
            rows8 < 3, block, jnp.where(rows8 == 3, square, jnp.where(rows8 == 4, 1.0, 0.0))
        )
        m1, m2, m3 = split3(feature)
        sf[0:16, lanes] = jnp.concatenate([m1, m2], axis=0).astype(BF16)
        sf[16:32, lanes] = jnp.concatenate([m1, m3], axis=0).astype(BF16)
        sf[32:48, lanes] = jnp.concatenate([m1, m2], axis=0).astype(BF16)
        chosen = jnp.zeros((16, LANES), F32)
        for b in range(3):
            mine = ((rows16 >= 3 + 3 * b) & (rows16 < 6 + 3 * b)) | (rows16 == 12 + b)
            chosen = jnp.where(mine, y[b], chosen)
        total = jnp.zeros((16, LANES), F32)
        for b in range(3):
            linear = (rows16 == 3 + b) | (rows16 == 6 + b) | (rows16 == 9 + b)
            last = (rows16 >= 12) & (rows16 < 15)
            value = jnp.where(
                rows16 == b, 1.0, jnp.where(linear, chosen, jnp.where(last, chosen * y[b], 0.0))
            )
            value = value + jnp.where(rows16 == 12 + b, square + 2.0 * soften, 0.0)
            value = value * weight
            coef[b, :, lanes] = value
            total = total + value * block[4 + b:5 + b]
        for piece, part in enumerate(split3(total)):
            psi[16 * piece:16 * piece + 16, lanes] = part.astype(BF16)
        plane_u[0, s] = block[4:8]

    def source_rows(turn, count):
        arrived(plane_in.at[pl.ds(0, count)], plane_sem.at[ITERS + turn])
        first = ((my_y + turn) % 4) * 8

        def body(s, carry):
            one_source_block(first + s)
            return carry

        lax.fori_loop(0, 8, body, 0)

    source_rows(0, 7)
    source_rows(1, 8)
    source_rows(3, 8)

    arrived(column_in.at[pl.ds(0, DEPTH - 1)], column_sem.at[ITERS])
    for t in range(DEPTH):
        block = column_in[t]
        lanes = pl.ds(t * LANES, LANES)
        x = [block[b:b + 1] for b in range(3)]
        square = x[0] * x[0] + x[1] * x[1] + x[2] * x[2]
        feature = jnp.where(
            rows8 < 3, -2.0 * block,
            jnp.where(rows8 == 3, 1.0, jnp.where(rows8 == 4, square + soften, 0.0)),
        )
        t1, t2, t3 = split3(feature)
        tf[0:16, lanes] = jnp.concatenate([t1, t1], axis=0).astype(BF16)
        tf[16:32, lanes] = jnp.concatenate([t2, t1], axis=0).astype(BF16)
        tf[32:48, lanes] = jnp.concatenate([t3, t2], axis=0).astype(BF16)
        for a in range(3):
            value = jnp.zeros((16, LANES), F32)
            for b in range(3):
                value = jnp.where(rows16 == b, x[a] * x[b] + (square if a == b else 0.0), value)
                for c in range(3):
                    part = jnp.zeros((1, LANES), F32)
                    if c == a:
                        part = part - 2.0 * x[b]
                    if b == c:
                        part = part - x[a]
                    if b == a:
                        part = part - x[c]
                    value = jnp.where(rows16 == 3 + 3 * b + c, part, value)
            phi[a, :, lanes] = jnp.where(rows16 == 12 + a, 1.0, value)
        column_u[0, t] = block[4:8]

    source_rows(2, 8)

    image[...] = jnp.zeros_like(image)

    def factor_block(s, carry):
        rows = pl.ds(pl.multiple_of(s * CHUNK, CHUNK), CHUNK)
        left = psi[:, rows]
        for b in range(BLOCKS):
            square = lax.dot_general(
                sf[:, rows], tf[:, b * WIDE:(b + 1) * WIDE], (((0,), (0,)), ((), ())),
                preferred_element_type=F32,
            )
            root = lax.rsqrt(square)
            factor = root * root * root
            high = factor.astype(BF16)
            low = (factor - high.astype(F32)).astype(BF16)
            matrix[b, rows, 0:WIDE] = high
            matrix[b, rows, WIDE:2 * WIDE] = low
            image[:, b * WIDE:(b + 1) * WIDE] += jnp.dot(
                left, high, preferred_element_type=F32
            ) + jnp.dot(left, low, preferred_element_type=F32)
        return carry

    lax.fori_loop(0, sources // CHUNK, factor_block, 0)

    def to_parts(k, b, both):
        summed = both[0:16] + both[16:32] + both[32:48]
        for a in range(3):
            row = jnp.sum(phi[a, :, b * WIDE:(b + 1) * WIDE] * summed, axis=0, keepdims=True)
            for c in range(WIDE // LANES):
                part_out[k, b * (WIDE // LANES) + c, a:a + 1, :] = (
                    row[:, c * LANES:(c + 1) * LANES]
                )

    for b in range(BLOCKS):
        to_parts(0, b, image[:, b * WIDE:(b + 1) * WIDE])

    lane_row = lax.broadcasted_iota(jnp.int32, (1, LANES), 1)
    hes_rows, hes_lanes = row_iota(8), lax.broadcasted_iota(jnp.int32, (8, LANES), 1)

    def inner(left, right):
        return total_of(jnp.sum(left * right, axis=0)[0:3])

    def at_lane(lane, value):
        return jnp.where(lane_row == lane, value, 0.0)

    def grams(k):
        latest = column_u[k]
        row = at_lane(6, inner(latest, latest))
        for i in range(ITERS):
            value = inner(column_u[i], latest)
            row = row + at_lane(8 + i, value)
        return row

    def exchange(k, with_column):
        message = plane_w.at[k, my_p]
        if with_column:
            for _, device in plane_peers[:16]:
                send(message, message, device, 1, plane_sem.at[k])
            for device in column_peers:
                send(message, column_w.at[k, my_z], device, 0, column_sem.at[k])
            for _, device in plane_peers[16:]:
                send(message, message, device, 1, plane_sem.at[k])
        else:
            for _, device in plane_peers:
                send(message, message, device, 1, plane_sem.at[k])
        arrived(plane_w.at[k, pl.ds(0, PLANE - 1)], plane_sem.at[k])
        sums = jnp.sum(plane_w[k, :, 3, :], axis=0, keepdims=True)
        gram[pl.ds(k, 1), :] = sums
        norm = jnp.sqrt(sums[:, 6:7])
        scaled = 1.0 / norm
        inverse[pl.ds(k, 1), :] = jnp.broadcast_to(scaled, (1, LANES))
        table = jnp.where((hes_rows == k) & (hes_lanes == k - 1), norm, hes[0:8])
        factors = []
        for i in range(ITERS):
            present = inverse[i:i + 1, 0:1]
            value = sums[:, i:i + 1] * present * scaled
            table = jnp.where((hes_rows == i) & (hes_lanes == k), value, table)
            factors.append(value * present)
        hes[0:8] = table
        hes[8:9] = jnp.where(k == 0, jnp.broadcast_to(norm, (1, LANES)), hes[8:9])
        return scaled, factors

    sent(plane_in.at[pl.ds(0, DEPTH - 1)], 0)
    sent(plane_in.at[pl.ds(0, PLANE - 1)], 1)

    def one_step(k, carry):
        partial = part_out[k]
        row = jnp.zeros((1, LANES), F32)
        for i in range(ITERS):
            row = row + at_lane(i, inner(column_u[i], partial))
        for t in range(DEPTH):
            part_out[k, t, 3:4, :] = row
        for device in column_peers:
            send(part_out.at[k, device[0]], part_in.at[k, my_z], device, 2, part_sem.at[k])
        part_in[k, my_z] = part_out[k, my_z]
        row = grams(k)
        for i in range(ITERS):
            row = row + at_lane(i, row[:, 8 + i:9 + i])
        applied = column_u[k, my_z]
        arrived(part_in.at[k, pl.ds(0, DEPTH - 1)], part_sem.at[k])
        summed = part_in[k, 0]
        for z in range(1, DEPTH):
            summed = summed + part_in[k, z]
        applied = applied + summed
        plane_w[k, my_p] = jnp.concatenate([applied[0:3], summed[3:4] + row], axis=0)
        column_w[k, my_z] = plane_w[k, my_p]
        scaled, factors = exchange(k, True)
        for s in range(PLANE):
            lanes = slice(s * LANES, (s + 1) * LANES)
            fresh = plane_w[k, s] * scaled
            for i in range(ITERS):
                fresh = fresh - factors[i] * plane_u[i, s]
            plane_u[k + 1, s] = fresh
            value = (
                coef[0, :, lanes] * fresh[0:1]
                + coef[1, :, lanes] * fresh[1:2]
                + coef[2, :, lanes] * fresh[2:3]
            )
            for piece, part in enumerate(split3(value)):
                psi[16 * piece:16 * piece + 16, lanes] = part.astype(BF16)
        arrived(column_w.at[k, pl.ds(0, DEPTH - 1)], column_sem.at[k])
        fresh = column_w[k] * scaled
        for i in range(ITERS):
            fresh = fresh - factors[i] * column_u[i]
        column_u[k + 1] = fresh
        sent(plane_w.at[0, pl.ds(0, DEPTH - 1)], 2)
        sent(plane_w.at[0, pl.ds(0, DEPTH - 1)], 0)
        sent(plane_w.at[0, pl.ds(0, PLANE - 1)], 1)
        for b in range(BLOCKS):
            both = jnp.zeros((48, WIDE), F32)
            for q in range(0, sources, DEEP):
                product = jnp.dot(
                    psi[:, q:q + DEEP], matrix[b, q:q + DEEP], preferred_element_type=F32
                )
                both = both + (product[:, 0:WIDE] + product[:, WIDE:2 * WIDE])
            to_parts(k + 1, b, both)
        return carry

    lax.fori_loop(0, ITERS - 1, one_step, 0)

    k = ITERS - 1
    for device in column_peers:
        send(part_out.at[k], part_all.at[my_z], device, 2, part_sem.at[k])
    part_all[my_z] = part_out[k]
    row = grams(k)
    arrived(part_all.at[pl.ds(0, DEPTH - 1)], part_sem.at[k])
    applied = column_u[k]
    for z in range(DEPTH):
        applied = applied + part_all[z]
    row = row + at_lane(4, inner(applied, applied))
    for i in range(ITERS):
        row = row + at_lane(i, inner(column_u[i], applied))
    column_u[k + 1] = applied
    plane_w[k, my_p] = jnp.concatenate([applied[0, 0:3], row], axis=0)
    scaled, factors = exchange(k, False)
    fresh = column_u[k + 1, my_z] * scaled
    for i in range(ITERS):
        fresh = fresh - factors[i] * column_u[i, my_z]
    column_u[k + 1, my_z] = fresh

    present = [inverse[i:i + 1, 0:1] for i in range(ITERS)]
    tall = [hes[i:i + 1, ITERS - 1:ITERS] for i in range(ITERS)]
    whole = gram[ITERS - 1:ITERS, 4:5] * present[-1] * present[-1]
    square = whole
    for i in range(ITERS):
        square = square - tall[i] * tall[i]
        for j in range(i + 1, ITERS):
            square = square + 2.0 * (tall[i] * present[i]) * (tall[j] * present[j]) * (
                gram[j:j + 1, 8 + i:9 + i]
            )
    norm = jnp.sqrt(jnp.maximum(square, whole * 1e-14))
    inverse[ITERS:ITERS + 1, :] = jnp.broadcast_to(1.0 / norm, (1, LANES))
    table = jnp.where((hes_rows == ITERS) & (hes_lanes == ITERS - 1), norm, hes[0:8])
    packed_ref[8:16] = table
    entry = [[table[i:i + 1, k:k + 1] for k in range(ITERS)] for i in range(ITERS + 1)]
    beta = hes[8:9, 0:1]
    y = least_squares(
        [[entry[i][k] for i in range(k + 1)] for k in range(ITERS)],
        [entry[k + 1][k] for k in range(ITERS)],
        beta,
    )
    solved = jnp.zeros((4, LANES), F32)
    misfit = jnp.zeros((4, LANES), F32)
    for i in range(ITERS + 1):
        basis = column_u[i, my_z] * inverse[i:i + 1, :]
        if i < ITERS:
            solved = solved + y[i] * basis
        g = beta if i == 0 else jnp.zeros_like(beta)
        for k in range(max(i - 1, 0), ITERS):
            g = g - entry[i][k] * y[k]
        misfit = misfit + g * basis
    packed_ref[0:4] = solved
    packed_ref[4:8] = misfit
    sent(part_all.at[pl.ds(0, DEPTH - 1)], 2)
    sent(plane_w.at[0, pl.ds(0, PLANE - 1)], 1)


def unpack(packed_ref, sol_ref, res_ref, hes_ref):
    sol_ref[...] = packed_ref[0:3]
    res_ref[...] = packed_ref[4:7]
    hes_ref[...] = packed_ref[8:16].T[0:ITERS, 0:ITERS + 1]


def shards(positions, areas, right_side):
    vmem = pl.BlockSpec(memory_space=pltpu.VMEM)
    sources, targets = PLANE * LANES, DEPTH * LANES
    packed = pl.pallas_call(
        kernel,
        out_shape=jax.ShapeDtypeStruct((16, LANES), F32),
        in_specs=[pl.BlockSpec(memory_space=pl.ANY)] * 3,
        out_specs=vmem,
        scratch_shapes=[
            pltpu.VMEM((PLANE, 8, LANES), F32),
            pltpu.VMEM((DEPTH, 8, LANES), F32),
            pltpu.VMEM((BLOCKS, sources, 2 * WIDE), BF16),
            pltpu.VMEM((48, sources), BF16),
            pltpu.VMEM((48, targets), BF16),
            pltpu.VMEM((3, 16, sources), F32),
            pltpu.VMEM((3, 16, targets), F32),
            pltpu.VMEM((48, sources), BF16),
            pltpu.VMEM((48, targets), F32),
            pltpu.VMEM((ITERS, PLANE, 4, LANES), F32),
            pltpu.VMEM((ITERS, DEPTH, 4, LANES), F32),
            pltpu.VMEM((ITERS, DEPTH, 4, LANES), F32),
            pltpu.VMEM((ITERS, DEPTH, 4, LANES), F32),
            pltpu.VMEM((DEPTH, DEPTH, 4, LANES), F32),
            pltpu.VMEM((ITERS + 1, PLANE, 4, LANES), F32),
            pltpu.VMEM((ITERS + 1, DEPTH, 4, LANES), F32),
            pltpu.VMEM((8, LANES), F32),
            pltpu.VMEM((16, LANES), F32),
            pltpu.VMEM((8, LANES), F32),
            pltpu.SemaphoreType.DMA((3,)),
            pltpu.SemaphoreType.DMA((3,)),
            pltpu.SemaphoreType.DMA((ITERS + 4,)),
            pltpu.SemaphoreType.DMA((ITERS + 1,)),
            pltpu.SemaphoreType.DMA((ITERS,)),
        ],
        compiler_params=pltpu.CompilerParams(
            collective_id=0, has_side_effects=True, vmem_limit_bytes=56 * 1024 * 1024
        ),
        name="arnoldi",
    )(positions, areas.reshape(1, -1), right_side)
    solved, misfit, turned = pl.pallas_call(
        unpack,
        out_shape=(
            jax.ShapeDtypeStruct((3, LANES), F32),
            jax.ShapeDtypeStruct((3, LANES), F32),
            jax.ShapeDtypeStruct((ITERS, ITERS + 1), F32),
        ),
        in_specs=[vmem],
        out_specs=(vmem,) * 3,
        name="unpack",
    )(packed)
    return solved, misfit, turned.T


def solution(mesh):
    split = Mesh(mesh.devices.reshape(DEPTH, PLANE), ("z", "p"))
    return jax.shard_map(
        shards,
        mesh=split,
        in_specs=(P(None, ("z", "p")), P(("z", "p")), P(None, ("z", "p"))),
        out_specs=(P(None, ("z", "p")), P(None, ("z", "p")), P()),
        check_vma=False,
    )
```

```python
import functools

import jax
import jax.numpy as jnp
from jax import lax
from jax.experimental import pallas as pl
from jax.experimental.pallas import tpu as pltpu
from jax.sharding import Mesh
from jax.sharding import PartitionSpec as P

ITERS = 4
soften = 0.0025
LANES = 128
WIDE = 256
CHUNK = 4096
DEEP = 512
DEPTH = 8
PLANE = 32
BLOCKS = DEPTH * LANES // WIDE
MESH = pl.DeviceIdType.MESH
F32 = jnp.float32
BF16 = jnp.bfloat16


def split3(value):
    first = value.astype(BF16).astype(F32)
    rest = value - first
    second = rest.astype(BF16).astype(F32)
    return first, second, rest - second


def row_iota(rows):
    return lax.broadcasted_iota(jnp.int32, (rows, LANES), 0)


def total_of(value):
    return jnp.sum(jnp.sum(value, axis=0, keepdims=True), axis=1, keepdims=True)


def least_squares(columns, heights, beta):
    zero = jnp.zeros_like(beta)
    size = len(columns)
    table = [[zero] * size for _ in range(size + 1)]
    for k in range(size):
        for i in range(k + 1):
            table[i][k] = columns[k][i]
        table[k + 1][k] = heights[k]
    target = [beta] + [zero] * size
    for c in range(size):
        lead, second = table[c][c], table[c + 1][c]
        radius = jnp.sqrt(lead * lead + second * second)
        cosine, sine = lead / radius, second / radius
        top, low = table[c], table[c + 1]
        new_top = [cosine * t + sine * l for t, l in zip(top, low)]
        new_low = [cosine * l - sine * t for t, l in zip(top, low)]
        table[c], table[c + 1] = new_top, new_low
        a, b = target[c], target[c + 1]
        target[c], target[c + 1] = cosine * a + sine * b, cosine * b - sine * a
    y = [zero] * size
    for r in reversed(range(size)):
        partial = zero
        for c in range(r + 1, size):
            partial = partial + table[r][c] * y[c]
        y[r] = (target[r] - partial) / table[r][r]
    return y


def kernel(
    pos_ref, area_ref, rhs_ref, packed_ref,
    plane_in, column_in, matrix, sf, tf, coef, phi, psi, image,
    plane_w, column_w, part_out, part_in, part_all, plane_u, column_u, gram, hes, inverse,
    load_sem, send_sem, plane_sem, column_sem, part_sem,
):
    my_z = lax.axis_index("z")
    my_p = lax.axis_index("p")
    my_y, my_x = my_p // 8, (my_p % 2) * 2 + (my_p // 4) % 2
    my_c = (my_p // 2) % 2
    sources = PLANE * LANES

    ys = [((my_y + d) % 4) * 8 for d in range(4)]
    xs = [((my_x + d) % 4) for d in range(4)]
    xs = [(x % 2) * 4 + x // 2 for x in xs]
    cs = [((my_c + d) % 2) * 2 for d in range(2)]
    hops = (0, 1, 2, 1)
    steps = [(a, b, c) for a in range(4) for b in range(4) for c in range(2)][1:]
    steps.sort(key=lambda s: -(4 * (hops[s[0]] + hops[s[1]]) + s[2]))
    plane_peers = [(s[0], (my_z, ys[s[0]] + xs[s[1]] + cs[s[2]])) for s in steps]
    column_peers = [((my_z + d) % DEPTH, my_p) for d in (4, 3, 5, 2, 6, 1, 7)]

    barrier = pltpu.get_barrier_semaphore()
    for device in column_peers + [peer for _, peer in plane_peers]:
        pl.semaphore_signal(barrier, inc=1, device_id=device, device_id_type=MESH)
    own = plane_in.at[my_p]
    loads = [
        pltpu.make_async_copy(pos_ref, own.at[0:3], load_sem.at[0]),
        pltpu.make_async_copy(area_ref, own.at[3:4], load_sem.at[1]),
        pltpu.make_async_copy(rhs_ref, own.at[4:7], load_sem.at[2]),
    ]
    for load in loads:
        load.start()
    plane_in[my_p, 7:8, :] = jnp.zeros((1, LANES), F32)
    hes[...] = jnp.zeros_like(hes)
    inverse[...] = jnp.zeros_like(inverse)
    plane_u[...] = jnp.zeros_like(plane_u)
    column_u[...] = jnp.zeros_like(column_u)
    part_out[...] = jnp.zeros_like(part_out)
    for load in loads:
        load.wait()
    pl.semaphore_wait(barrier, PLANE - 1 + DEPTH - 1)

    def send(src, dst, device, slot, recv_sem):
        pltpu.make_async_remote_copy(
            src_ref=src, dst_ref=dst, send_sem=send_sem.at[slot], recv_sem=recv_sem,
            device_id=device, device_id_type=MESH,
        ).start()

    def arrived(part, recv_sem):
        pltpu.make_async_remote_copy(
            src_ref=part, dst_ref=part, send_sem=send_sem.at[0], recv_sem=recv_sem,
            device_id=(my_z, my_p), device_id_type=MESH,
        ).wait_recv()

    def sent(part, slot):
        pltpu.make_async_remote_copy(
            src_ref=part, dst_ref=part, send_sem=send_sem.at[slot], recv_sem=load_sem.at[0],
            device_id=(my_z, my_p), device_id_type=MESH,
        ).wait_send()

    for device in column_peers:
        send(own, column_in.at[my_z], device, 0, column_sem.at[ITERS])
    for turn, device in plane_peers:
        send(own, own, device, 1, plane_sem.at[ITERS + (4 - turn) % 4])
    column_in[my_z] = plane_in[my_p]

    rows8, rows16 = row_iota(8), row_iota(16)
    scale = float(PLANE * DEPTH * LANES) ** (-0.5)

    def one_source_block(s):
        block = plane_in[s]
        lanes = pl.ds(pl.multiple_of(s * LANES, LANES), LANES)
        y = [block[b:b + 1] for b in range(3)]
        weight = block[3:4] * scale
        square = y[0] * y[0] + y[1] * y[1] + y[2] * y[2]
        feature = jnp.where(
            rows8 < 3, block, jnp.where(rows8 == 3, square, jnp.where(rows8 == 4, 1.0, 0.0))
        )
        m1, m2, m3 = split3(feature)
        sf[0:16, lanes] = jnp.concatenate([m1, m2], axis=0).astype(BF16)
        sf[16:32, lanes] = jnp.concatenate([m1, m3], axis=0).astype(BF16)
        sf[32:48, lanes] = jnp.concatenate([m1, m2], axis=0).astype(BF16)
        chosen = jnp.zeros((16, LANES), F32)
        for b in range(3):
            mine = ((rows16 >= 3 + 3 * b) & (rows16 < 6 + 3 * b)) | (rows16 == 12 + b)
            chosen = jnp.where(mine, y[b], chosen)
        total = jnp.zeros((16, LANES), F32)
        for b in range(3):
            linear = (rows16 == 3 + b) | (rows16 == 6 + b) | (rows16 == 9 + b)
            last = (rows16 >= 12) & (rows16 < 15)
            value = jnp.where(
                rows16 == b, 1.0, jnp.where(linear, chosen, jnp.where(last, chosen * y[b], 0.0))
            )
            value = value + jnp.where(rows16 == 12 + b, square + 2.0 * soften, 0.0)
            value = value * weight
            coef[b, :, lanes] = value
            total = total + value * block[4 + b:5 + b]
        for piece, part in enumerate(split3(total)):
            psi[16 * piece:16 * piece + 16, lanes] = part.astype(BF16)
        plane_u[0, s] = block[4:8]

    def source_rows(turn, count):
        arrived(plane_in.at[pl.ds(0, count)], plane_sem.at[ITERS + turn])
        first = ((my_y + turn) % 4) * 8

        def body(s, carry):
            one_source_block(first + s)
            return carry

        lax.fori_loop(0, 8, body, 0)

    source_rows(0, 7)
    source_rows(1, 8)
    source_rows(3, 8)

    arrived(column_in.at[pl.ds(0, DEPTH - 1)], column_sem.at[ITERS])
    for t in range(DEPTH):
        block = column_in[t]
        lanes = pl.ds(t * LANES, LANES)
        x = [block[b:b + 1] for b in range(3)]
        square = x[0] * x[0] + x[1] * x[1] + x[2] * x[2]
        feature = jnp.where(
            rows8 < 3, -2.0 * block,
            jnp.where(rows8 == 3, 1.0, jnp.where(rows8 == 4, square + soften, 0.0)),
        )
        t1, t2, t3 = split3(feature)
        tf[0:16, lanes] = jnp.concatenate([t1, t1], axis=0).astype(BF16)
        tf[16:32, lanes] = jnp.concatenate([t2, t1], axis=0).astype(BF16)
        tf[32:48, lanes] = jnp.concatenate([t3, t2], axis=0).astype(BF16)
        for a in range(3):
            value = jnp.zeros((16, LANES), F32)
            for b in range(3):
                value = jnp.where(rows16 == b, x[a] * x[b] + (square if a == b else 0.0), value)
                for c in range(3):
                    part = jnp.zeros((1, LANES), F32)
                    if c == a:
                        part = part - 2.0 * x[b]
                    if b == c:
                        part = part - x[a]
                    if b == a:
                        part = part - x[c]
                    value = jnp.where(rows16 == 3 + 3 * b + c, part, value)
            phi[a, :, lanes] = jnp.where(rows16 == 12 + a, 1.0, value)
        column_u[0, t] = block[4:8]

    source_rows(2, 8)

    image[...] = jnp.zeros_like(image)

    def factor_block(s, carry):
        rows = pl.ds(pl.multiple_of(s * CHUNK, CHUNK), CHUNK)
        left = psi[:, rows]
        for b in range(BLOCKS):
            square = lax.dot_general(
                sf[:, rows], tf[:, b * WIDE:(b + 1) * WIDE], (((0,), (0,)), ((), ())),
                preferred_element_type=F32,
            )
            root = lax.rsqrt(square)
            factor = root * root * root
            high = factor.astype(BF16)
            low = (factor - high.astype(F32)).astype(BF16)
            matrix[b, rows, 0:WIDE] = high
            matrix[b, rows, WIDE:2 * WIDE] = low
            image[:, b * WIDE:(b + 1) * WIDE] += jnp.dot(
                left, high, preferred_element_type=F32
            ) + jnp.dot(left, low, preferred_element_type=F32)
        return carry

    lax.fori_loop(0, sources // CHUNK, factor_block, 0)

    lane_row = lax.broadcasted_iota(jnp.int32, (1, LANES), 1)
    hes_rows, hes_lanes = row_iota(8), lax.broadcasted_iota(jnp.int32, (8, LANES), 1)

    def at_lane(lane, value):
        return jnp.where(lane_row == lane, value, 0.0)

    def to_parts(k, b, both, dots):
        summed = both[0:16] + both[16:32] + both[32:48]
        dots = list(dots)
        for a in range(3):
            row = jnp.sum(phi[a, :, b * WIDE:(b + 1) * WIDE] * summed, axis=0, keepdims=True)
            for c in range(WIDE // LANES):
                t, piece = b * (WIDE // LANES) + c, row[:, c * LANES:(c + 1) * LANES]
                part_out[k, t, a:a + 1, :] = piece
                for i in range(ITERS):
                    dots[i] = dots[i] + column_u[i, t, a:a + 1, :] * piece
        return dots

    def with_dots(k, dots):
        row = jnp.zeros((1, LANES), F32)
        for i in range(ITERS):
            row = row + at_lane(i, jnp.sum(dots[i], axis=1, keepdims=True))
        for t in range(DEPTH):
            part_out[k, t, 3:4, :] = row

    dots = [jnp.zeros((1, LANES), F32)] * ITERS
    for b in range(BLOCKS):
        dots = to_parts(0, b, image[:, b * WIDE:(b + 1) * WIDE], dots)
    with_dots(0, dots)

    def inner(left, right):
        return total_of(jnp.sum(left * right, axis=0)[0:3])

    def grams(k):
        latest = column_u[k]
        row = at_lane(6, inner(latest, latest))
        for i in range(ITERS):
            value = inner(column_u[i], latest)
            row = row + at_lane(8 + i, value)
        return row

    def exchange(k, with_column):
        message = plane_w.at[k, my_p]
        if with_column:
            for _, device in plane_peers[:16]:
                send(message, message, device, 1, plane_sem.at[k])
            for device in column_peers:
                send(message, column_w.at[k, my_z], device, 0, column_sem.at[k])
            for _, device in plane_peers[16:]:
                send(message, message, device, 1, plane_sem.at[k])
        else:
            for _, device in plane_peers:
                send(message, message, device, 1, plane_sem.at[k])
        arrived(plane_w.at[k, pl.ds(0, PLANE - 1)], plane_sem.at[k])
        sums = jnp.sum(plane_w[k, :, 3, :], axis=0, keepdims=True)
        gram[pl.ds(k, 1), :] = sums
        norm = jnp.sqrt(sums[:, 6:7])
        scaled = 1.0 / norm
        inverse[pl.ds(k, 1), :] = jnp.broadcast_to(scaled, (1, LANES))
        table = jnp.where((hes_rows == k) & (hes_lanes == k - 1), norm, hes[0:8])
        factors = []
        for i in range(ITERS):
            present = inverse[i:i + 1, 0:1]
            value = sums[:, i:i + 1] * present * scaled
            table = jnp.where((hes_rows == i) & (hes_lanes == k), value, table)
            factors.append(value * present)
        hes[0:8] = table
        hes[8:9] = jnp.where(k == 0, jnp.broadcast_to(norm, (1, LANES)), hes[8:9])
        return scaled, factors

    sent(plane_in.at[pl.ds(0, DEPTH - 1)], 0)
    sent(plane_in.at[pl.ds(0, PLANE - 1)], 1)

    def one_step(k, carry):
        for device in column_peers:
            send(part_out.at[k, device[0]], part_in.at[k, my_z], device, 2, part_sem.at[k])
        part_in[k, my_z] = part_out[k, my_z]
        row = grams(k)
        for i in range(ITERS):
            row = row + at_lane(i, row[:, 8 + i:9 + i])
        applied = column_u[k, my_z]
        arrived(part_in.at[k, pl.ds(0, DEPTH - 1)], part_sem.at[k])
        summed = part_in[k, 0]
        for z in range(1, DEPTH):
            summed = summed + part_in[k, z]
        applied = applied + summed
        plane_w[k, my_p] = jnp.concatenate([applied[0:3], summed[3:4] + row], axis=0)
        column_w[k, my_z] = plane_w[k, my_p]
        scaled, factors = exchange(k, True)
        for s in range(PLANE):
            lanes = slice(s * LANES, (s + 1) * LANES)
            fresh = plane_w[k, s] * scaled
            for i in range(ITERS):
                fresh = fresh - factors[i] * plane_u[i, s]
            plane_u[k + 1, s] = fresh
            value = (
                coef[0, :, lanes] * fresh[0:1]
                + coef[1, :, lanes] * fresh[1:2]
                + coef[2, :, lanes] * fresh[2:3]
            )
            for piece, part in enumerate(split3(value)):
                psi[16 * piece:16 * piece + 16, lanes] = part.astype(BF16)
        arrived(column_w.at[k, pl.ds(0, DEPTH - 1)], column_sem.at[k])
        fresh = column_w[k] * scaled
        for i in range(ITERS):
            fresh = fresh - factors[i] * column_u[i]
        column_u[k + 1] = fresh
        sent(plane_w.at[0, pl.ds(0, DEPTH - 1)], 2)
        sent(plane_w.at[0, pl.ds(0, DEPTH - 1)], 0)
        sent(plane_w.at[0, pl.ds(0, PLANE - 1)], 1)
        dots = [jnp.zeros((1, LANES), F32)] * ITERS
        for b in range(BLOCKS):
            both = jnp.zeros((48, WIDE), F32)
            for q in range(0, sources, DEEP):
                product = jnp.dot(
                    psi[:, q:q + DEEP], matrix[b, q:q + DEEP], preferred_element_type=F32
                )
                both = both + (product[:, 0:WIDE] + product[:, WIDE:2 * WIDE])
            dots = to_parts(k + 1, b, both, dots)
        with_dots(k + 1, dots)
        return carry

    lax.fori_loop(0, ITERS - 1, one_step, 0)

    k = ITERS - 1
    for device in column_peers:
        send(part_out.at[k], part_all.at[my_z], device, 2, part_sem.at[k])
    part_all[my_z] = part_out[k]
    row = grams(k)
    arrived(part_all.at[pl.ds(0, DEPTH - 1)], part_sem.at[k])
    applied = column_u[k]
    for z in range(DEPTH):
        applied = applied + part_all[z]
    row = row + at_lane(4, inner(applied, applied))
    for i in range(ITERS):
        row = row + at_lane(i, inner(column_u[i], applied))
    column_u[k + 1] = applied
    plane_w[k, my_p] = jnp.concatenate([applied[0, 0:3], row], axis=0)
    scaled, factors = exchange(k, False)
    fresh = column_u[k + 1, my_z] * scaled
    for i in range(ITERS):
        fresh = fresh - factors[i] * column_u[i, my_z]
    column_u[k + 1, my_z] = fresh

    present = [inverse[i:i + 1, 0:1] for i in range(ITERS)]
    tall = [hes[i:i + 1, ITERS - 1:ITERS] for i in range(ITERS)]
    whole = gram[ITERS - 1:ITERS, 4:5] * present[-1] * present[-1]
    square = whole
    for i in range(ITERS):
        square = square - tall[i] * tall[i]
        for j in range(i + 1, ITERS):
            square = square + 2.0 * (tall[i] * present[i]) * (tall[j] * present[j]) * (
                gram[j:j + 1, 8 + i:9 + i]
            )
    norm = jnp.sqrt(jnp.maximum(square, whole * 1e-14))
    inverse[ITERS:ITERS + 1, :] = jnp.broadcast_to(1.0 / norm, (1, LANES))
    table = jnp.where((hes_rows == ITERS) & (hes_lanes == ITERS - 1), norm, hes[0:8])
    packed_ref[8:16] = table
    entry = [[table[i:i + 1, k:k + 1] for k in range(ITERS)] for i in range(ITERS + 1)]
    beta = hes[8:9, 0:1]
    y = least_squares(
        [[entry[i][k] for i in range(k + 1)] for k in range(ITERS)],
        [entry[k + 1][k] for k in range(ITERS)],
        beta,
    )
    solved = jnp.zeros((4, LANES), F32)
    misfit = jnp.zeros((4, LANES), F32)
    for i in range(ITERS + 1):
        basis = column_u[i, my_z] * inverse[i:i + 1, :]
        if i < ITERS:
            solved = solved + y[i] * basis
        g = beta if i == 0 else jnp.zeros_like(beta)
        for k in range(max(i - 1, 0), ITERS):
            g = g - entry[i][k] * y[k]
        misfit = misfit + g * basis
    packed_ref[0:4] = solved
    packed_ref[4:8] = misfit
    sent(part_all.at[pl.ds(0, DEPTH - 1)], 2)
    sent(plane_w.at[0, pl.ds(0, PLANE - 1)], 1)


def unpack(packed_ref, sol_ref, res_ref, hes_ref):
    sol_ref[...] = packed_ref[0:3]
    res_ref[...] = packed_ref[4:7]
    hes_ref[...] = packed_ref[8:16].T[0:ITERS, 0:ITERS + 1]


def shards(positions, areas, right_side):
    vmem = pl.BlockSpec(memory_space=pltpu.VMEM)
    sources, targets = PLANE * LANES, DEPTH * LANES
    packed = pl.pallas_call(
        kernel,
        out_shape=pltpu.VMEM((16, LANES), F32),
        in_specs=[pl.BlockSpec(memory_space=pl.ANY)] * 3,
        out_specs=vmem,
        scratch_shapes=[
            pltpu.VMEM((PLANE, 8, LANES), F32),
            pltpu.VMEM((DEPTH, 8, LANES), F32),
            pltpu.VMEM((BLOCKS, sources, 2 * WIDE), BF16),
            pltpu.VMEM((48, sources), BF16),
            pltpu.VMEM((48, targets), BF16),
            pltpu.VMEM((3, 16, sources), F32),
            pltpu.VMEM((3, 16, targets), F32),
            pltpu.VMEM((48, sources), BF16),
            pltpu.VMEM((48, targets), F32),
            pltpu.VMEM((ITERS, PLANE, 4, LANES), F32),
            pltpu.VMEM((ITERS, DEPTH, 4, LANES), F32),
            pltpu.VMEM((ITERS, DEPTH, 4, LANES), F32),
            pltpu.VMEM((ITERS, DEPTH, 4, LANES), F32),
            pltpu.VMEM((DEPTH, DEPTH, 4, LANES), F32),
            pltpu.VMEM((ITERS + 1, PLANE, 4, LANES), F32),
            pltpu.VMEM((ITERS + 1, DEPTH, 4, LANES), F32),
            pltpu.VMEM((8, LANES), F32),
            pltpu.VMEM((16, LANES), F32),
            pltpu.VMEM((8, LANES), F32),
            pltpu.SemaphoreType.DMA((3,)),
            pltpu.SemaphoreType.DMA((3,)),
            pltpu.SemaphoreType.DMA((ITERS + 4,)),
            pltpu.SemaphoreType.DMA((ITERS + 1,)),
            pltpu.SemaphoreType.DMA((ITERS,)),
        ],
        compiler_params=pltpu.CompilerParams(
            collective_id=0, has_side_effects=True, vmem_limit_bytes=56 * 1024 * 1024
        ),
        name="arnoldi",
    )(positions, areas.reshape(1, -1), right_side)
    solved, misfit, turned = pl.pallas_call(
        unpack,
        out_shape=(
            jax.ShapeDtypeStruct((3, LANES), F32),
            jax.ShapeDtypeStruct((3, LANES), F32),
            jax.ShapeDtypeStruct((ITERS, ITERS + 1), F32),
        ),
        in_specs=[vmem],
        out_specs=(vmem,) * 3,
        name="unpack",
    )(pltpu.with_memory_space_constraint(packed, pltpu.VMEM))
    return solved, misfit, turned.T


def solution(mesh):
    split = Mesh(mesh.devices.reshape(DEPTH, PLANE), ("z", "p"))
    return jax.shard_map(
        shards,
        mesh=split,
        in_specs=(P(None, ("z", "p")), P(("z", "p")), P(None, ("z", "p"))),
        out_specs=(P(None, ("z", "p")), P(None, ("z", "p")), P()),
        check_vma=False,
    )
```

```python
import functools

import jax
import jax.numpy as jnp
from jax import lax
from jax.experimental import pallas as pl
from jax.experimental.pallas import tpu as pltpu
from jax.sharding import Mesh
from jax.sharding import PartitionSpec as P

ITERS = 4
soften = 0.0025
LANES = 128
WIDE = 256
CHUNK = 4096
DEEP = 512
DEPTH = 8
PLANE = 32
BLOCKS = DEPTH * LANES // WIDE
MESH = pl.DeviceIdType.MESH
F32 = jnp.float32
BF16 = jnp.bfloat16


def split3(value):
    first = value.astype(BF16).astype(F32)
    rest = value - first
    second = rest.astype(BF16).astype(F32)
    return first, second, rest - second


def row_iota(rows):
    return lax.broadcasted_iota(jnp.int32, (rows, LANES), 0)


def total_of(value):
    return jnp.sum(jnp.sum(value, axis=0, keepdims=True), axis=1, keepdims=True)


def least_squares(columns, heights, beta):
    zero = jnp.zeros_like(beta)
    size = len(columns)
    table = [[zero] * size for _ in range(size + 1)]
    for k in range(size):
        for i in range(k + 1):
            table[i][k] = columns[k][i]
        table[k + 1][k] = heights[k]
    target = [beta] + [zero] * size
    for c in range(size):
        lead, second = table[c][c], table[c + 1][c]
        radius = jnp.sqrt(lead * lead + second * second)
        cosine, sine = lead / radius, second / radius
        top, low = table[c], table[c + 1]
        new_top = [cosine * t + sine * l for t, l in zip(top, low)]
        new_low = [cosine * l - sine * t for t, l in zip(top, low)]
        table[c], table[c + 1] = new_top, new_low
        a, b = target[c], target[c + 1]
        target[c], target[c + 1] = cosine * a + sine * b, cosine * b - sine * a
    y = [zero] * size
    for r in reversed(range(size)):
        partial = zero
        for c in range(r + 1, size):
            partial = partial + table[r][c] * y[c]
        y[r] = (target[r] - partial) / table[r][r]
    return y


def kernel(
    pos_ref, area_ref, rhs_ref, packed_ref,
    plane_in, column_in, matrix, sf, tf, coef, phi, psi, image,
    plane_w, column_w, part_out, part_in, part_all, plane_u, column_u, gram, hes, inverse,
    load_sem, send_sem, plane_sem, column_sem, part_sem,
):
    my_z = lax.axis_index("z")
    my_p = lax.axis_index("p")
    my_y, my_x = my_p // 8, (my_p % 2) * 2 + (my_p // 4) % 2
    my_c = (my_p // 2) % 2
    sources = PLANE * LANES

    ys = [((my_y + d) % 4) * 8 for d in range(4)]
    xs = [((my_x + d) % 4) for d in range(4)]
    xs = [(x % 2) * 4 + x // 2 for x in xs]
    cs = [((my_c + d) % 2) * 2 for d in range(2)]
    hops = (0, 1, 2, 1)
    steps = [(a, b, c) for a in range(4) for b in range(4) for c in range(2)][1:]
    steps.sort(key=lambda s: -(4 * (hops[s[0]] + hops[s[1]]) + s[2]))
    plane_peers = [(s[0], (my_z, ys[s[0]] + xs[s[1]] + cs[s[2]])) for s in steps]
    column_peers = [((my_z + d) % DEPTH, my_p) for d in (4, 3, 5, 2, 6, 1, 7)]

    barrier = pltpu.get_barrier_semaphore()
    for device in column_peers + [peer for _, peer in plane_peers]:
        pl.semaphore_signal(barrier, inc=1, device_id=device, device_id_type=MESH)
    own = plane_in.at[my_p]
    loads = [
        pltpu.make_async_copy(pos_ref, own.at[0:3], load_sem.at[0]),
        pltpu.make_async_copy(area_ref, own.at[3:4], load_sem.at[1]),
        pltpu.make_async_copy(rhs_ref, own.at[4:7], load_sem.at[2]),
    ]
    for load in loads:
        load.start()
    plane_in[my_p, 7:8, :] = jnp.zeros((1, LANES), F32)
    hes[...] = jnp.zeros_like(hes)
    inverse[...] = jnp.zeros_like(inverse)
    plane_u[...] = jnp.zeros_like(plane_u)
    column_u[...] = jnp.zeros_like(column_u)
    part_out[...] = jnp.zeros_like(part_out)
    for load in loads:
        load.wait()
    pl.semaphore_wait(barrier, PLANE - 1 + DEPTH - 1)

    def send(src, dst, device, slot, recv_sem):
        pltpu.make_async_remote_copy(
            src_ref=src, dst_ref=dst, send_sem=send_sem.at[slot], recv_sem=recv_sem,
            device_id=device, device_id_type=MESH,
        ).start()

    def arrived(part, recv_sem):
        pltpu.make_async_remote_copy(
            src_ref=part, dst_ref=part, send_sem=send_sem.at[0], recv_sem=recv_sem,
            device_id=(my_z, my_p), device_id_type=MESH,
        ).wait_recv()

    def sent(part, slot):
        pltpu.make_async_remote_copy(
            src_ref=part, dst_ref=part, send_sem=send_sem.at[slot], recv_sem=load_sem.at[0],
            device_id=(my_z, my_p), device_id_type=MESH,
        ).wait_send()

    for device in column_peers:
        send(own, column_in.at[my_z], device, 0, column_sem.at[ITERS])
    for turn, device in plane_peers:
        send(own, own, device, 1, plane_sem.at[ITERS + (4 - turn) % 4])
    column_in[my_z] = plane_in[my_p]

    rows8, rows16 = row_iota(8), row_iota(16)
    scale = float(PLANE * DEPTH * LANES) ** (-0.5)

    def one_source_block(s):
        block = plane_in[s]
        lanes = pl.ds(pl.multiple_of(s * LANES, LANES), LANES)
        y = [block[b:b + 1] for b in range(3)]
        weight = block[3:4] * scale
        square = y[0] * y[0] + y[1] * y[1] + y[2] * y[2]
        feature = jnp.where(
            rows8 < 3, block, jnp.where(rows8 == 3, square, jnp.where(rows8 == 4, 1.0, 0.0))
        )
        m1, m2, m3 = split3(feature)
        sf[0:16, lanes] = jnp.concatenate([m1, m2], axis=0).astype(BF16)
        sf[16:32, lanes] = jnp.concatenate([m1, m3], axis=0).astype(BF16)
        sf[32:48, lanes] = jnp.concatenate([m1, m2], axis=0).astype(BF16)
        chosen = jnp.zeros((16, LANES), F32)
        for b in range(3):
            mine = ((rows16 >= 3 + 3 * b) & (rows16 < 6 + 3 * b)) | (rows16 == 12 + b)
            chosen = jnp.where(mine, y[b], chosen)
        total = jnp.zeros((16, LANES), F32)
        for b in range(3):
            linear = (rows16 == 3 + b) | (rows16 == 6 + b) | (rows16 == 9 + b)
            last = (rows16 >= 12) & (rows16 < 15)
            value = jnp.where(
                rows16 == b, 1.0, jnp.where(linear, chosen, jnp.where(last, chosen * y[b], 0.0))
            )
            value = value + jnp.where(rows16 == 12 + b, square + 2.0 * soften, 0.0)
            value = value * weight
            coef[b, :, lanes] = value
            total = total + value * block[4 + b:5 + b]
        for piece, part in enumerate(split3(total)):
            psi[16 * piece:16 * piece + 16, lanes] = part.astype(BF16)
        plane_u[0, s] = block[4:8]

    def source_rows(turn, count):
        arrived(plane_in.at[pl.ds(0, count)], plane_sem.at[ITERS + turn])
        first = ((my_y + turn) % 4) * 8

        def body(s, carry):
            one_source_block(first + s)
            return carry

        lax.fori_loop(0, 8, body, 0)

    source_rows(0, 7)
    source_rows(1, 8)
    source_rows(3, 8)

    arrived(column_in.at[pl.ds(0, DEPTH - 1)], column_sem.at[ITERS])
    for t in range(DEPTH):
        block = column_in[t]
        lanes = pl.ds(t * LANES, LANES)
        x = [block[b:b + 1] for b in range(3)]
        square = x[0] * x[0] + x[1] * x[1] + x[2] * x[2]
        feature = jnp.where(
            rows8 < 3, -2.0 * block,
            jnp.where(rows8 == 3, 1.0, jnp.where(rows8 == 4, square + soften, 0.0)),
        )
        t1, t2, t3 = split3(feature)
        tf[0:16, lanes] = jnp.concatenate([t1, t1], axis=0).astype(BF16)
        tf[16:32, lanes] = jnp.concatenate([t2, t1], axis=0).astype(BF16)
        tf[32:48, lanes] = jnp.concatenate([t3, t2], axis=0).astype(BF16)
        for a in range(3):
            value = jnp.zeros((16, LANES), F32)
            for b in range(3):
                value = jnp.where(rows16 == b, x[a] * x[b] + (square if a == b else 0.0), value)
                for c in range(3):
                    part = jnp.zeros((1, LANES), F32)
                    if c == a:
                        part = part - 2.0 * x[b]
                    if b == c:
                        part = part - x[a]
                    if b == a:
                        part = part - x[c]
                    value = jnp.where(rows16 == 3 + 3 * b + c, part, value)
            phi[a, :, lanes] = jnp.where(rows16 == 12 + a, 1.0, value)
        column_u[0, t] = block[4:8]

    source_rows(2, 8)

    image[...] = jnp.zeros_like(image)

    def factor_block(s, carry):
        rows = pl.ds(pl.multiple_of(s * CHUNK, CHUNK), CHUNK)
        left = psi[:, rows]
        for b in range(BLOCKS):
            square = lax.dot_general(
                sf[:, rows], tf[:, b * WIDE:(b + 1) * WIDE], (((0,), (0,)), ((), ())),
                preferred_element_type=F32,
            )
            root = lax.rsqrt(square)
            factor = root * root * root
            high = factor.astype(BF16)
            low = (factor - high.astype(F32)).astype(BF16)
            matrix[b, rows, 0:WIDE] = high
            matrix[b, rows, WIDE:2 * WIDE] = low
            image[:, b * WIDE:(b + 1) * WIDE] += jnp.dot(
                left, high, preferred_element_type=F32
            ) + jnp.dot(left, low, preferred_element_type=F32)
        return carry

    lax.fori_loop(0, sources // CHUNK, factor_block, 0)

    lane_row = lax.broadcasted_iota(jnp.int32, (1, LANES), 1)
    hes_rows, hes_lanes = row_iota(8), lax.broadcasted_iota(jnp.int32, (8, LANES), 1)

    def at_lane(lane, value):
        return jnp.where(lane_row == lane, value, 0.0)

    def to_parts(k, b, both, dots):
        summed = both[0:16] + both[16:32] + both[32:48]
        dots = list(dots)
        for a in range(3):
            row = jnp.sum(phi[a, :, b * WIDE:(b + 1) * WIDE] * summed, axis=0, keepdims=True)
            for c in range(WIDE // LANES):
                t, piece = b * (WIDE // LANES) + c, row[:, c * LANES:(c + 1) * LANES]
                part_out[k, t, a:a + 1, :] = piece
                for i in range(len(dots)):
                    dots[i] = dots[i] + column_u[i, t, a:a + 1, :] * piece
        return dots

    def with_dots(k, dots):
        row = jnp.zeros((1, LANES), F32)
        for i in range(len(dots)):
            row = row + at_lane(i, jnp.sum(dots[i], axis=1, keepdims=True))
        for t in range(DEPTH):
            part_out[k, t, 3:4, :] = row

    dots = [jnp.zeros((1, LANES), F32)]
    for b in range(BLOCKS):
        dots = to_parts(0, b, image[:, b * WIDE:(b + 1) * WIDE], dots)
    with_dots(0, dots)

    def inner(left, right):
        return total_of(jnp.sum(left * right, axis=0)[0:3])

    def grams(k):
        latest = column_u[k]
        values = [inner(column_u[i], latest) for i in range(k + 1)]
        row = at_lane(6, values[k])
        for i in range(k + 1):
            row = row + at_lane(8 + i, values[i])
        return row, values

    def exchange(k, with_column):
        message = plane_w.at[k, my_p]
        if with_column:
            for _, device in plane_peers[:16]:
                send(message, message, device, 1, plane_sem.at[k])
            for device in column_peers:
                send(message, column_w.at[k, my_z], device, 0, column_sem.at[k])
            for _, device in plane_peers[16:]:
                send(message, message, device, 1, plane_sem.at[k])
        else:
            for _, device in plane_peers:
                send(message, message, device, 1, plane_sem.at[k])
        arrived(plane_w.at[k, pl.ds(0, PLANE - 1)], plane_sem.at[k])
        sums = jnp.sum(plane_w[k, :, 3, :], axis=0, keepdims=True)
        gram[k:k + 1, :] = sums
        norm = jnp.sqrt(sums[:, 6:7])
        scaled = 1.0 / norm
        inverse[k:k + 1, :] = jnp.broadcast_to(scaled, (1, LANES))
        table = hes[0:8]
        if k > 0:
            table = jnp.where((hes_rows == k) & (hes_lanes == k - 1), norm, table)
        factors = []
        for i in range(k + 1):
            present = scaled if i == k else inverse[i:i + 1, 0:1]
            value = sums[:, i:i + 1] * present * scaled
            table = jnp.where((hes_rows == i) & (hes_lanes == k), value, table)
            factors.append(value * present)
        hes[0:8] = table
        if k == 0:
            hes[8:9] = jnp.broadcast_to(norm, (1, LANES))
        return scaled, factors

    sent(plane_in.at[pl.ds(0, DEPTH - 1)], 0)
    sent(plane_in.at[pl.ds(0, PLANE - 1)], 1)

    def last_parts(first, slot):
        half = pl.ds(first, DEPTH // 2)
        for device in column_peers:
            send(
                part_out.at[ITERS - 1, half, 0:3], part_all.at[my_z, half, 0:3], device, 2 + slot,
                part_sem.at[ITERS - 1 + slot],
            )

    for k in range(ITERS - 1):
        for device in column_peers:
            send(part_out.at[k, device[0]], part_in.at[k, my_z], device, 2, part_sem.at[k])
        part_in[k, my_z] = part_out[k, my_z]
        row, values = grams(k)
        for i in range(k + 1):
            row = row + at_lane(i, values[i])
        applied = column_u[k, my_z]
        arrived(part_in.at[k, pl.ds(0, DEPTH - 1)], part_sem.at[k])
        summed = part_in[k, 0]
        for z in range(1, DEPTH):
            summed = summed + part_in[k, z]
        applied = applied + summed
        plane_w[k, my_p] = jnp.concatenate([applied[0:3], summed[3:4] + row], axis=0)
        column_w[k, my_z] = plane_w[k, my_p]
        scaled, factors = exchange(k, True)
        for s in range(PLANE):
            lanes = slice(s * LANES, (s + 1) * LANES)
            fresh = plane_w[k, s] * scaled
            for i in range(k + 1):
                fresh = fresh - factors[i] * plane_u[i, s]
            plane_u[k + 1, s] = fresh
            value = (
                coef[0, :, lanes] * fresh[0:1]
                + coef[1, :, lanes] * fresh[1:2]
                + coef[2, :, lanes] * fresh[2:3]
            )
            for piece, part in enumerate(split3(value)):
                psi[16 * piece:16 * piece + 16, lanes] = part.astype(BF16)
        arrived(column_w.at[k, pl.ds(0, DEPTH - 1)], column_sem.at[k])
        fresh = column_w[k] * scaled
        for i in range(k + 1):
            fresh = fresh - factors[i] * column_u[i]
        column_u[k + 1] = fresh
        sent(plane_w.at[0, pl.ds(0, DEPTH - 1)], 2)
        sent(plane_w.at[0, pl.ds(0, DEPTH - 1)], 0)
        sent(plane_w.at[0, pl.ds(0, PLANE - 1)], 1)
        final = k + 1 == ITERS - 1
        dots = [jnp.zeros((1, LANES), F32)] * (0 if final else k + 2)
        for b in range(BLOCKS):
            both = jnp.zeros((48, WIDE), F32)
            for q in range(0, sources, DEEP):
                product = jnp.dot(
                    psi[:, q:q + DEEP], matrix[b, q:q + DEEP], preferred_element_type=F32
                )
                both = both + (product[:, 0:WIDE] + product[:, WIDE:2 * WIDE])
            dots = to_parts(k + 1, b, both, dots)
            if final and b == BLOCKS // 2 - 1:
                last_parts(0, 0)
        if final:
            last_parts(DEPTH // 2, 1)
        else:
            with_dots(k + 1, dots)

    k = ITERS - 1
    part_all[my_z] = part_out[k]
    row, _ = grams(k)
    for slot in range(2):
        arrived(part_all.at[pl.ds(0, DEPTH - 1), pl.ds(0, DEPTH // 2), 0:3], part_sem.at[k + slot])
    applied = column_u[k]
    for z in range(DEPTH):
        applied = applied + part_all[z]
    row = row + at_lane(4, inner(applied, applied))
    for i in range(ITERS):
        row = row + at_lane(i, inner(column_u[i], applied))
    column_u[k + 1] = applied
    plane_w[k, my_p] = jnp.concatenate([applied[0, 0:3], row], axis=0)
    scaled, factors = exchange(k, False)
    fresh = column_u[k + 1, my_z] * scaled
    for i in range(ITERS):
        fresh = fresh - factors[i] * column_u[i, my_z]
    column_u[k + 1, my_z] = fresh

    present = [inverse[i:i + 1, 0:1] for i in range(ITERS)]
    tall = [hes[i:i + 1, ITERS - 1:ITERS] for i in range(ITERS)]
    whole = gram[ITERS - 1:ITERS, 4:5] * present[-1] * present[-1]
    square = whole
    for i in range(ITERS):
        square = square - tall[i] * tall[i]
        for j in range(i + 1, ITERS):
            square = square + 2.0 * (tall[i] * present[i]) * (tall[j] * present[j]) * (
                gram[j:j + 1, 8 + i:9 + i]
            )
    norm = jnp.sqrt(jnp.maximum(square, whole * 1e-14))
    inverse[ITERS:ITERS + 1, :] = jnp.broadcast_to(1.0 / norm, (1, LANES))
    table = jnp.where((hes_rows == ITERS) & (hes_lanes == ITERS - 1), norm, hes[0:8])
    packed_ref[8:16] = table
    entry = [[table[i:i + 1, k:k + 1] for k in range(ITERS)] for i in range(ITERS + 1)]
    beta = hes[8:9, 0:1]
    y = least_squares(
        [[entry[i][k] for i in range(k + 1)] for k in range(ITERS)],
        [entry[k + 1][k] for k in range(ITERS)],
        beta,
    )
    solved = jnp.zeros((4, LANES), F32)
    misfit = jnp.zeros((4, LANES), F32)
    for i in range(ITERS + 1):
        basis = column_u[i, my_z] * inverse[i:i + 1, :]
        if i < ITERS:
            solved = solved + y[i] * basis
        g = beta if i == 0 else jnp.zeros_like(beta)
        for k in range(max(i - 1, 0), ITERS):
            g = g - entry[i][k] * y[k]
        misfit = misfit + g * basis
    packed_ref[0:4] = solved
    packed_ref[4:8] = misfit
    for slot in range(2):
        sent(part_all.at[pl.ds(0, DEPTH - 1), pl.ds(0, DEPTH // 2), 0:3], 2 + slot)
    sent(plane_w.at[0, pl.ds(0, PLANE - 1)], 1)


def unpack(packed_ref, sol_ref, res_ref, hes_ref):
    sol_ref[...] = packed_ref[0:3]
    res_ref[...] = packed_ref[4:7]
    hes_ref[...] = packed_ref[8:16].T[0:ITERS, 0:ITERS + 1]


def shards(positions, areas, right_side):
    vmem = pl.BlockSpec(memory_space=pltpu.VMEM)
    sources, targets = PLANE * LANES, DEPTH * LANES
    packed = pl.pallas_call(
        kernel,
        out_shape=pltpu.VMEM((16, LANES), F32),
        in_specs=[pl.BlockSpec(memory_space=pl.ANY)] * 3,
        out_specs=vmem,
        scratch_shapes=[
            pltpu.VMEM((PLANE, 8, LANES), F32),
            pltpu.VMEM((DEPTH, 8, LANES), F32),
            pltpu.VMEM((BLOCKS, sources, 2 * WIDE), BF16),
            pltpu.VMEM((48, sources), BF16),
            pltpu.VMEM((48, targets), BF16),
            pltpu.VMEM((3, 16, sources), F32),
            pltpu.VMEM((3, 16, targets), F32),
            pltpu.VMEM((48, sources), BF16),
            pltpu.VMEM((48, targets), F32),
            pltpu.VMEM((ITERS, PLANE, 4, LANES), F32),
            pltpu.VMEM((ITERS, DEPTH, 4, LANES), F32),
            pltpu.VMEM((ITERS, DEPTH, 4, LANES), F32),
            pltpu.VMEM((ITERS, DEPTH, 4, LANES), F32),
            pltpu.VMEM((DEPTH, DEPTH, 4, LANES), F32),
            pltpu.VMEM((ITERS + 1, PLANE, 4, LANES), F32),
            pltpu.VMEM((ITERS + 1, DEPTH, 4, LANES), F32),
            pltpu.VMEM((8, LANES), F32),
            pltpu.VMEM((16, LANES), F32),
            pltpu.VMEM((8, LANES), F32),
            pltpu.SemaphoreType.DMA((3,)),
            pltpu.SemaphoreType.DMA((4,)),
            pltpu.SemaphoreType.DMA((ITERS + 4,)),
            pltpu.SemaphoreType.DMA((ITERS + 1,)),
            pltpu.SemaphoreType.DMA((ITERS + 1,)),
        ],
        compiler_params=pltpu.CompilerParams(
            collective_id=0, has_side_effects=True, vmem_limit_bytes=56 * 1024 * 1024
        ),
        name="arnoldi",
    )(positions, areas.reshape(1, -1), right_side)
    solved, misfit, turned = pl.pallas_call(
        unpack,
        out_shape=(
            jax.ShapeDtypeStruct((3, LANES), F32),
            jax.ShapeDtypeStruct((3, LANES), F32),
            jax.ShapeDtypeStruct((ITERS, ITERS + 1), F32),
        ),
        in_specs=[vmem],
        out_specs=(vmem,) * 3,
        name="unpack",
    )(pltpu.with_memory_space_constraint(packed, pltpu.VMEM))
    return solved, misfit, turned.T


def solution(mesh):
    split = Mesh(mesh.devices.reshape(DEPTH, PLANE), ("z", "p"))
    return jax.shard_map(
        shards,
        mesh=split,
        in_specs=(P(None, ("z", "p")), P(("z", "p")), P(None, ("z", "p"))),
        out_specs=(P(None, ("z", "p")), P(None, ("z", "p")), P()),
        check_vma=False,
    )
```

```python
import functools

import jax
import jax.numpy as jnp
from jax import lax
from jax.experimental import pallas as pl
from jax.experimental.pallas import tpu as pltpu
from jax.sharding import Mesh
from jax.sharding import PartitionSpec as P

ITERS = 4
soften = 0.0025
LANES = 128
WIDE = 256
CHUNK = 512
DEEP = 512
DEPTH = 8
PLANE = 32
BLOCKS = DEPTH * LANES // WIDE
MESH = pl.DeviceIdType.MESH
F32 = jnp.float32
BF16 = jnp.bfloat16


def split3(value):
    first = value.astype(BF16).astype(F32)
    rest = value - first
    second = rest.astype(BF16).astype(F32)
    return first, second, rest - second


def row_iota(rows):
    return lax.broadcasted_iota(jnp.int32, (rows, LANES), 0)


def total_of(value):
    return jnp.sum(jnp.sum(value, axis=0, keepdims=True), axis=1, keepdims=True)


def least_squares(columns, heights, beta):
    zero = jnp.zeros_like(beta)
    size = len(columns)
    table = [[zero] * size for _ in range(size + 1)]
    for k in range(size):
        for i in range(k + 1):
            table[i][k] = columns[k][i]
        table[k + 1][k] = heights[k]
    target = [beta] + [zero] * size
    for c in range(size):
        lead, second = table[c][c], table[c + 1][c]
        radius = jnp.sqrt(lead * lead + second * second)
        cosine, sine = lead / radius, second / radius
        top, low = table[c], table[c + 1]
        new_top = [cosine * t + sine * l for t, l in zip(top, low)]
        new_low = [cosine * l - sine * t for t, l in zip(top, low)]
        table[c], table[c + 1] = new_top, new_low
        a, b = target[c], target[c + 1]
        target[c], target[c + 1] = cosine * a + sine * b, cosine * b - sine * a
    y = [zero] * size
    for r in reversed(range(size)):
        partial = zero
        for c in range(r + 1, size):
            partial = partial + table[r][c] * y[c]
        y[r] = (target[r] - partial) / table[r][r]
    return y


def kernel(
    pos_ref, area_ref, rhs_ref, packed_ref,
    plane_in, column_in, matrix, sf, tf, coef, phi, psi,
    plane_w, column_w, part_out, part_in, part_all, plane_u, column_u, gram, hes, inverse,
    load_sem, send_sem, plane_sem, column_sem, part_sem,
):
    my_z = lax.axis_index("z")
    my_p = lax.axis_index("p")
    my_y, my_x = my_p // 8, (my_p % 2) * 2 + (my_p // 4) % 2
    my_c = (my_p // 2) % 2
    sources = PLANE * LANES

    ys = [((my_y + d) % 4) * 8 for d in range(4)]
    xs = [((my_x + d) % 4) for d in range(4)]
    xs = [(x % 2) * 4 + x // 2 for x in xs]
    cs = [((my_c + d) % 2) * 2 for d in range(2)]
    hops = (0, 1, 2, 1)
    steps = [(a, b, c) for a in range(4) for b in range(4) for c in range(2)][1:]
    steps.sort(key=lambda s: -(4 * (hops[s[0]] + hops[s[1]]) + s[2]))
    plane_peers = [(s[0], (my_z, ys[s[0]] + xs[s[1]] + cs[s[2]])) for s in steps]
    column_peers = [((my_z + d) % DEPTH, my_p) for d in (4, 3, 5, 2, 6, 1, 7)]

    barrier = pltpu.get_barrier_semaphore()
    for device in column_peers + [peer for _, peer in plane_peers]:
        pl.semaphore_signal(barrier, inc=1, device_id=device, device_id_type=MESH)
    own = plane_in.at[my_p]
    loads = [
        pltpu.make_async_copy(pos_ref, own.at[0:3], load_sem.at[0]),
        pltpu.make_async_copy(area_ref, own.at[3:4], load_sem.at[1]),
        pltpu.make_async_copy(rhs_ref, own.at[4:7], load_sem.at[2]),
    ]
    for load in loads:
        load.start()
    plane_in[my_p, 7:8, :] = jnp.zeros((1, LANES), F32)
    hes[...] = jnp.zeros_like(hes)
    inverse[...] = jnp.zeros_like(inverse)
    plane_u[...] = jnp.zeros_like(plane_u)
    column_u[...] = jnp.zeros_like(column_u)
    part_out[...] = jnp.zeros_like(part_out)
    for load in loads:
        load.wait()
    pl.semaphore_wait(barrier, PLANE - 1 + DEPTH - 1)

    def send(src, dst, device, slot, recv_sem):
        pltpu.make_async_remote_copy(
            src_ref=src, dst_ref=dst, send_sem=send_sem.at[slot], recv_sem=recv_sem,
            device_id=device, device_id_type=MESH,
        ).start()

    def arrived(part, recv_sem):
        pltpu.make_async_remote_copy(
            src_ref=part, dst_ref=part, send_sem=send_sem.at[0], recv_sem=recv_sem,
            device_id=(my_z, my_p), device_id_type=MESH,
        ).wait_recv()

    def sent(part, slot):
        pltpu.make_async_remote_copy(
            src_ref=part, dst_ref=part, send_sem=send_sem.at[slot], recv_sem=load_sem.at[0],
            device_id=(my_z, my_p), device_id_type=MESH,
        ).wait_send()

    for device in column_peers:
        send(own, column_in.at[my_z], device, 0, column_sem.at[ITERS])
    for turn, device in plane_peers:
        send(own, own, device, 1, plane_sem.at[ITERS + (4 - turn) % 4])
    column_in[my_z] = plane_in[my_p]

    rows8, rows16 = row_iota(8), row_iota(16)
    scale = float(PLANE * DEPTH * LANES) ** (-0.5)

    def one_source_block(s):
        block = plane_in[s]
        lanes = pl.ds(pl.multiple_of(s * LANES, LANES), LANES)
        y = [block[b:b + 1] for b in range(3)]
        weight = block[3:4] * scale
        square = y[0] * y[0] + y[1] * y[1] + y[2] * y[2]
        feature = jnp.where(
            rows8 < 3, block, jnp.where(rows8 == 3, square, jnp.where(rows8 == 4, 1.0, 0.0))
        )
        m1, m2, m3 = split3(feature)
        sf[0:16, lanes] = jnp.concatenate([m1, m2], axis=0).astype(BF16)
        sf[16:32, lanes] = jnp.concatenate([m1, m3], axis=0).astype(BF16)
        sf[32:48, lanes] = jnp.concatenate([m1, m2], axis=0).astype(BF16)
        chosen = jnp.zeros((16, LANES), F32)
        for b in range(3):
            mine = ((rows16 >= 3 + 3 * b) & (rows16 < 6 + 3 * b)) | (rows16 == 12 + b)
            chosen = jnp.where(mine, y[b], chosen)
        total = jnp.zeros((16, LANES), F32)
        for b in range(3):
            linear = (rows16 == 3 + b) | (rows16 == 6 + b) | (rows16 == 9 + b)
            last = (rows16 >= 12) & (rows16 < 15)
            value = jnp.where(
                rows16 == b, 1.0, jnp.where(linear, chosen, jnp.where(last, chosen * y[b], 0.0))
            )
            value = value + jnp.where(rows16 == 12 + b, square + 2.0 * soften, 0.0)
            value = value * weight
            coef[b, :, lanes] = value
            total = total + value * block[4 + b:5 + b]
        for piece, part in enumerate(split3(total)):
            psi[16 * piece:16 * piece + 16, lanes] = part.astype(BF16)
        plane_u[0, s] = block[4:8]

    def source_rows(turn, count):
        arrived(plane_in.at[pl.ds(0, count)], plane_sem.at[ITERS + turn])
        first = ((my_y + turn) % 4) * 8

        def body(s, carry):
            one_source_block(first + s)
            return carry

        lax.fori_loop(0, 8, body, 0, unroll=turn == 2)

    source_rows(0, 7)
    source_rows(1, 8)
    source_rows(3, 8)

    arrived(column_in.at[pl.ds(0, DEPTH - 1)], column_sem.at[ITERS])
    for t in range(DEPTH):
        block = column_in[t]
        lanes = pl.ds(t * LANES, LANES)
        x = [block[b:b + 1] for b in range(3)]
        square = x[0] * x[0] + x[1] * x[1] + x[2] * x[2]
        feature = jnp.where(
            rows8 < 3, -2.0 * block,
            jnp.where(rows8 == 3, 1.0, jnp.where(rows8 == 4, square + soften, 0.0)),
        )
        t1, t2, t3 = split3(feature)
        tf[0:16, lanes] = jnp.concatenate([t1, t1], axis=0).astype(BF16)
        tf[16:32, lanes] = jnp.concatenate([t2, t1], axis=0).astype(BF16)
        tf[32:48, lanes] = jnp.concatenate([t3, t2], axis=0).astype(BF16)
        for a in range(3):
            value = jnp.zeros((16, LANES), F32)
            for b in range(3):
                value = jnp.where(rows16 == b, x[a] * x[b] + (square if a == b else 0.0), value)
                for c in range(3):
                    part = jnp.zeros((1, LANES), F32)
                    if c == a:
                        part = part - 2.0 * x[b]
                    if b == c:
                        part = part - x[a]
                    if b == a:
                        part = part - x[c]
                    value = jnp.where(rows16 == 3 + 3 * b + c, part, value)
            phi[a, :, lanes] = jnp.where(rows16 == 12 + a, 1.0, value)
        column_u[0, t] = block[4:8]

    source_rows(2, 8)

    lane_row = lax.broadcasted_iota(jnp.int32, (1, LANES), 1)
    hes_rows, hes_lanes = row_iota(8), lax.broadcasted_iota(jnp.int32, (8, LANES), 1)

    def at_lane(lane, value):
        return jnp.where(lane_row == lane, value, 0.0)

    def to_parts(k, b, both, dots):
        summed = both[0:16] + both[16:32] + both[32:48]
        dots = list(dots)
        for a in range(3):
            row = jnp.sum(phi[a, :, b * WIDE:(b + 1) * WIDE] * summed, axis=0, keepdims=True)
            for c in range(WIDE // LANES):
                t, piece = b * (WIDE // LANES) + c, row[:, c * LANES:(c + 1) * LANES]
                part_out[k, t, a:a + 1, :] = piece
                for i in range(len(dots)):
                    dots[i] = dots[i] + column_u[i, t, a:a + 1, :] * piece
        return dots

    def with_dots(k, dots):
        row = jnp.zeros((1, LANES), F32)
        for i in range(len(dots)):
            row = row + at_lane(i, jnp.sum(dots[i], axis=1, keepdims=True))
        for t in range(DEPTH):
            part_out[k, t, 3:4, :] = row

    dots = [jnp.zeros((1, LANES), F32)]
    for b in range(BLOCKS):
        both = jnp.zeros((48, WIDE), F32)
        for q in range(0, sources, CHUNK):
            square = lax.dot_general(
                sf[:, q:q + CHUNK], tf[:, b * WIDE:(b + 1) * WIDE], (((0,), (0,)), ((), ())),
                preferred_element_type=F32,
            )
            root = lax.rsqrt(square)
            factor = root * root * root
            high = factor.astype(BF16)
            low = (factor - high.astype(F32)).astype(BF16)
            matrix[b, q:q + CHUNK, 0:WIDE] = high
            matrix[b, q:q + CHUNK, WIDE:2 * WIDE] = low
            left = psi[:, q:q + CHUNK]
            both = both + (
                jnp.dot(left, high, preferred_element_type=F32)
                + jnp.dot(left, low, preferred_element_type=F32)
            )
        dots = to_parts(0, b, both, dots)
    with_dots(0, dots)

    def inner(left, right):
        return total_of(jnp.sum(left * right, axis=0)[0:3])

    def grams(k):
        latest = column_u[k]
        values = [inner(column_u[i], latest) for i in range(k + 1)]
        row = at_lane(6, values[k])
        for i in range(k + 1):
            row = row + at_lane(8 + i, values[i])
        return row, values

    def exchange(k, with_column):
        whole = slice(0, 4) if with_column else slice(3, 4)
        message = plane_w.at[k, my_p, whole]
        if with_column:
            for _, device in plane_peers[:16]:
                send(message, message, device, 1, plane_sem.at[k])
            for device in column_peers:
                send(message, column_w.at[k, my_z], device, 0, column_sem.at[k])
            for _, device in plane_peers[16:]:
                send(message, message, device, 1, plane_sem.at[k])
        else:
            for _, device in plane_peers:
                send(message, message, device, 1, plane_sem.at[k])
        arrived(plane_w.at[k, pl.ds(0, PLANE - 1), whole], plane_sem.at[k])
        sums = jnp.sum(plane_w[k, :, 3, :], axis=0, keepdims=True)
        gram[k:k + 1, :] = sums
        norm = jnp.sqrt(sums[:, 6:7])
        scaled = 1.0 / norm
        inverse[k:k + 1, :] = jnp.broadcast_to(scaled, (1, LANES))
        table = hes[0:8]
        if k > 0:
            table = jnp.where((hes_rows == k) & (hes_lanes == k - 1), norm, table)
        factors = []
        for i in range(k + 1):
            present = scaled if i == k else inverse[i:i + 1, 0:1]
            value = sums[:, i:i + 1] * present * scaled
            table = jnp.where((hes_rows == i) & (hes_lanes == k), value, table)
            factors.append(value * present)
        hes[0:8] = table
        if k == 0:
            hes[8:9] = jnp.broadcast_to(norm, (1, LANES))
        return scaled, factors

    sent(plane_in.at[pl.ds(0, DEPTH - 1)], 0)
    sent(plane_in.at[pl.ds(0, PLANE - 1)], 1)

    def last_parts(first, slot):
        half = pl.ds(first, DEPTH // 2)
        for device in column_peers:
            send(
                part_out.at[ITERS - 1, half, 0:3], part_all.at[my_z, half, 0:3], device, 2 + slot,
                part_sem.at[ITERS - 1 + slot],
            )

    for k in range(ITERS - 1):
        for device in column_peers:
            send(part_out.at[k, device[0]], part_in.at[k, my_z], device, 2, part_sem.at[k])
        part_in[k, my_z] = part_out[k, my_z]
        row, values = grams(k)
        for i in range(k + 1):
            row = row + at_lane(i, values[i])
        applied = column_u[k, my_z]
        arrived(part_in.at[k, pl.ds(0, DEPTH - 1)], part_sem.at[k])
        summed = part_in[k, 0]
        for z in range(1, DEPTH):
            summed = summed + part_in[k, z]
        applied = applied + summed
        plane_w[k, my_p] = jnp.concatenate([applied[0:3], summed[3:4] + row], axis=0)
        column_w[k, my_z] = plane_w[k, my_p]
        scaled, factors = exchange(k, True)
        for s in range(PLANE):
            lanes = slice(s * LANES, (s + 1) * LANES)
            fresh = plane_w[k, s] * scaled
            for i in range(k + 1):
                fresh = fresh - factors[i] * plane_u[i, s]
            plane_u[k + 1, s] = fresh
            value = (
                coef[0, :, lanes] * fresh[0:1]
                + coef[1, :, lanes] * fresh[1:2]
                + coef[2, :, lanes] * fresh[2:3]
            )
            for piece, part in enumerate(split3(value)):
                psi[16 * piece:16 * piece + 16, lanes] = part.astype(BF16)
        arrived(column_w.at[k, pl.ds(0, DEPTH - 1)], column_sem.at[k])
        fresh = column_w[k] * scaled
        for i in range(k + 1):
            fresh = fresh - factors[i] * column_u[i]
        column_u[k + 1] = fresh
        sent(plane_w.at[0, pl.ds(0, DEPTH - 1)], 2)
        sent(plane_w.at[0, pl.ds(0, DEPTH - 1)], 0)
        sent(plane_w.at[0, pl.ds(0, PLANE - 1)], 1)
        final = k + 1 == ITERS - 1
        dots = [jnp.zeros((1, LANES), F32)] * (0 if final else k + 2)
        for b in range(BLOCKS):
            both = jnp.zeros((48, WIDE), F32)
            for q in range(0, sources, DEEP):
                product = jnp.dot(
                    psi[:, q:q + DEEP], matrix[b, q:q + DEEP], preferred_element_type=F32
                )
                both = both + (product[:, 0:WIDE] + product[:, WIDE:2 * WIDE])
            dots = to_parts(k + 1, b, both, dots)
            if final and b == BLOCKS // 2 - 1:
                last_parts(0, 0)
        if final:
            last_parts(DEPTH // 2, 1)
        else:
            with_dots(k + 1, dots)

    k = ITERS - 1
    part_all[my_z] = part_out[k]
    row, _ = grams(k)
    for slot in range(2):
        arrived(part_all.at[pl.ds(0, DEPTH - 1), pl.ds(0, DEPTH // 2), 0:3], part_sem.at[k + slot])
    applied = column_u[k]
    for z in range(DEPTH):
        applied = applied + part_all[z]
    row = row + at_lane(4, inner(applied, applied))
    for i in range(ITERS):
        row = row + at_lane(i, inner(column_u[i], applied))
    column_u[k + 1] = applied
    plane_w[k, my_p] = jnp.concatenate([applied[0, 0:3], row], axis=0)
    scaled, factors = exchange(k, False)
    fresh = column_u[k + 1, my_z] * scaled
    for i in range(ITERS):
        fresh = fresh - factors[i] * column_u[i, my_z]
    column_u[k + 1, my_z] = fresh

    present = [inverse[i:i + 1, 0:1] for i in range(ITERS)]
    tall = [hes[i:i + 1, ITERS - 1:ITERS] for i in range(ITERS)]
    whole = gram[ITERS - 1:ITERS, 4:5] * present[-1] * present[-1]
    square = whole
    for i in range(ITERS):
        square = square - tall[i] * tall[i]
        for j in range(i + 1, ITERS):
            square = square + 2.0 * (tall[i] * present[i]) * (tall[j] * present[j]) * (
                gram[j:j + 1, 8 + i:9 + i]
            )
    norm = jnp.sqrt(jnp.maximum(square, whole * 1e-14))
    inverse[ITERS:ITERS + 1, :] = jnp.broadcast_to(1.0 / norm, (1, LANES))
    table = jnp.where((hes_rows == ITERS) & (hes_lanes == ITERS - 1), norm, hes[0:8])
    packed_ref[8:16] = table
    entry = [[table[i:i + 1, k:k + 1] for k in range(ITERS)] for i in range(ITERS + 1)]
    beta = hes[8:9, 0:1]
    y = least_squares(
        [[entry[i][k] for i in range(k + 1)] for k in range(ITERS)],
        [entry[k + 1][k] for k in range(ITERS)],
        beta,
    )
    solved = jnp.zeros((4, LANES), F32)
    misfit = jnp.zeros((4, LANES), F32)
    for i in range(ITERS + 1):
        basis = column_u[i, my_z] * inverse[i:i + 1, :]
        if i < ITERS:
            solved = solved + y[i] * basis
        g = beta if i == 0 else jnp.zeros_like(beta)
        for k in range(max(i - 1, 0), ITERS):
            g = g - entry[i][k] * y[k]
        misfit = misfit + g * basis
    packed_ref[0:4] = solved
    packed_ref[4:8] = misfit
    for slot in range(2):
        sent(part_all.at[pl.ds(0, DEPTH - 1), pl.ds(0, DEPTH // 2), 0:3], 2 + slot)
    sent(plane_w.at[0, pl.ds(0, PLANE - 1), 3:4], 1)


def unpack(packed_ref, sol_ref, res_ref, hes_ref):
    sol_ref[...] = packed_ref[0:3]
    res_ref[...] = packed_ref[4:7]
    hes_ref[...] = packed_ref[8:16].T[0:ITERS, 0:ITERS + 1]


def shards(positions, areas, right_side):
    vmem = pl.BlockSpec(memory_space=pltpu.VMEM)
    sources, targets = PLANE * LANES, DEPTH * LANES
    packed = pl.pallas_call(
        kernel,
        out_shape=pltpu.VMEM((16, LANES), F32),
        in_specs=[pl.BlockSpec(memory_space=pl.ANY)] * 3,
        out_specs=vmem,
        scratch_shapes=[
            pltpu.VMEM((PLANE, 8, LANES), F32),
            pltpu.VMEM((DEPTH, 8, LANES), F32),
            pltpu.VMEM((BLOCKS, sources, 2 * WIDE), BF16),
            pltpu.VMEM((48, sources), BF16),
            pltpu.VMEM((48, targets), BF16),
            pltpu.VMEM((3, 16, sources), F32),
            pltpu.VMEM((3, 16, targets), F32),
            pltpu.VMEM((48, sources), BF16),
            pltpu.VMEM((ITERS, PLANE, 4, LANES), F32),
            pltpu.VMEM((ITERS, DEPTH, 4, LANES), F32),
            pltpu.VMEM((ITERS, DEPTH, 4, LANES), F32),
            pltpu.VMEM((ITERS, DEPTH, 4, LANES), F32),
            pltpu.VMEM((DEPTH, DEPTH, 4, LANES), F32),
            pltpu.VMEM((ITERS + 1, PLANE, 4, LANES), F32),
            pltpu.VMEM((ITERS + 1, DEPTH, 4, LANES), F32),
            pltpu.VMEM((8, LANES), F32),
            pltpu.VMEM((16, LANES), F32),
            pltpu.VMEM((8, LANES), F32),
            pltpu.SemaphoreType.DMA((3,)),
            pltpu.SemaphoreType.DMA((4,)),
            pltpu.SemaphoreType.DMA((ITERS + 4,)),
            pltpu.SemaphoreType.DMA((ITERS + 1,)),
            pltpu.SemaphoreType.DMA((ITERS + 1,)),
        ],
        compiler_params=pltpu.CompilerParams(
            collective_id=0, has_side_effects=True, vmem_limit_bytes=56 * 1024 * 1024
        ),
        name="arnoldi",
    )(positions, areas.reshape(1, -1), right_side)
    solved, misfit, turned = pl.pallas_call(
        unpack,
        out_shape=(
            jax.ShapeDtypeStruct((3, LANES), F32),
            jax.ShapeDtypeStruct((3, LANES), F32),
            jax.ShapeDtypeStruct((ITERS, ITERS + 1), F32),
        ),
        in_specs=[vmem],
        out_specs=(vmem,) * 3,
        name="unpack",
    )(pltpu.with_memory_space_constraint(packed, pltpu.VMEM))
    return solved, misfit, turned.T


def solution(mesh):
    split = Mesh(mesh.devices.reshape(DEPTH, PLANE), ("z", "p"))
    return jax.shard_map(
        shards,
        mesh=split,
        in_specs=(P(None, ("z", "p")), P(("z", "p")), P(None, ("z", "p"))),
        out_specs=(P(None, ("z", "p")), P(None, ("z", "p")), P()),
        check_vma=False,
    )
```

```python
import functools

import jax
import jax.numpy as jnp
from jax import lax
from jax.experimental import pallas as pl
from jax.experimental.pallas import tpu as pltpu
from jax.sharding import Mesh
from jax.sharding import PartitionSpec as P

ITERS = 4
soften = 0.0025
LANES = 128
WIDE = 256
CHUNK = 512
DEEP = 512
DEPTH = 8
PLANE = 32
BLOCKS = DEPTH * LANES // WIDE
MESH = pl.DeviceIdType.MESH
F32 = jnp.float32
BF16 = jnp.bfloat16


def split3(value):
    first = value.astype(BF16).astype(F32)
    rest = value - first
    second = rest.astype(BF16).astype(F32)
    return first, second, rest - second


def row_iota(rows):
    return lax.broadcasted_iota(jnp.int32, (rows, LANES), 0)


def total_of(value):
    return jnp.sum(jnp.sum(value, axis=0, keepdims=True), axis=1, keepdims=True)


def least_squares(columns, heights, beta):
    zero = jnp.zeros_like(beta)
    size = len(columns)
    table = [[zero] * size for _ in range(size + 1)]
    for k in range(size):
        for i in range(k + 1):
            table[i][k] = columns[k][i]
        table[k + 1][k] = heights[k]
    target = [beta] + [zero] * size
    for c in range(size):
        lead, second = table[c][c], table[c + 1][c]
        radius = jnp.sqrt(lead * lead + second * second)
        cosine, sine = lead / radius, second / radius
        top, low = table[c], table[c + 1]
        new_top = [cosine * t + sine * l for t, l in zip(top, low)]
        new_low = [cosine * l - sine * t for t, l in zip(top, low)]
        table[c], table[c + 1] = new_top, new_low
        a, b = target[c], target[c + 1]
        target[c], target[c + 1] = cosine * a + sine * b, cosine * b - sine * a
    y = [zero] * size
    for r in reversed(range(size)):
        partial = zero
        for c in range(r + 1, size):
            partial = partial + table[r][c] * y[c]
        y[r] = (target[r] - partial) / table[r][r]
    return y


def kernel(
    pos_ref, area_ref, rhs_ref, packed_ref,
    plane_in, column_in, matrix, sf, tf, coef, phi, psi,
    plane_w, column_w, part_out, part_in, part_all, plane_u, column_u, gram, hes, inverse,
    load_sem, send_sem, plane_sem, column_sem, part_sem,
):
    my_z = lax.axis_index("z")
    my_p = lax.axis_index("p")
    my_y, my_x = my_p // 8, (my_p % 2) * 2 + (my_p // 4) % 2
    my_c = (my_p // 2) % 2
    sources = PLANE * LANES

    ys = [((my_y + d) % 4) * 8 for d in range(4)]
    xs = [((my_x + d) % 4) for d in range(4)]
    xs = [(x % 2) * 4 + x // 2 for x in xs]
    cs = [((my_c + d) % 2) * 2 for d in range(2)]
    hops = (0, 1, 2, 1)
    steps = [(a, b, c) for a in range(4) for b in range(4) for c in range(2)][1:]
    steps.sort(key=lambda s: -(4 * (hops[s[0]] + hops[s[1]]) + s[2]))
    plane_peers = [(s[0], (my_z, ys[s[0]] + xs[s[1]] + cs[s[2]])) for s in steps]
    column_peers = [((my_z + d) % DEPTH, my_p) for d in (4, 3, 5, 2, 6, 1, 7)]

    barrier = pltpu.get_barrier_semaphore()
    for device in column_peers + [peer for _, peer in plane_peers]:
        pl.semaphore_signal(barrier, inc=1, device_id=device, device_id_type=MESH)
    own = plane_in.at[my_p]
    loads = [
        pltpu.make_async_copy(pos_ref, own.at[0:3], load_sem.at[0]),
        pltpu.make_async_copy(area_ref, own.at[3:4], load_sem.at[1]),
        pltpu.make_async_copy(rhs_ref, own.at[4:7], load_sem.at[2]),
    ]
    for load in loads:
        load.start()
    plane_in[:, 7:8, :] = jnp.zeros((PLANE, 1, LANES), F32)
    column_in[:, 7:8, :] = jnp.zeros((DEPTH, 1, LANES), F32)
    hes[...] = jnp.zeros_like(hes)
    inverse[...] = jnp.zeros_like(inverse)
    plane_u[...] = jnp.zeros_like(plane_u)
    column_u[...] = jnp.zeros_like(column_u)
    part_out[...] = jnp.zeros_like(part_out)
    for load in loads:
        load.wait()
    pl.semaphore_wait(barrier, PLANE - 1 + DEPTH - 1)

    def send(src, dst, device, slot, recv_sem):
        pltpu.make_async_remote_copy(
            src_ref=src, dst_ref=dst, send_sem=send_sem.at[slot], recv_sem=recv_sem,
            device_id=device, device_id_type=MESH,
        ).start()

    def arrived(part, recv_sem):
        pltpu.make_async_remote_copy(
            src_ref=part, dst_ref=part, send_sem=send_sem.at[0], recv_sem=recv_sem,
            device_id=(my_z, my_p), device_id_type=MESH,
        ).wait_recv()

    def sent(part, slot):
        pltpu.make_async_remote_copy(
            src_ref=part, dst_ref=part, send_sem=send_sem.at[slot], recv_sem=load_sem.at[0],
            device_id=(my_z, my_p), device_id_type=MESH,
        ).wait_send()

    used = own.at[0:7]
    for turn, device in plane_peers[:8]:
        send(used, used, device, 1, plane_sem.at[ITERS + (4 - turn) % 4])
    for device in column_peers:
        send(used, column_in.at[my_z, 0:7], device, 0, column_sem.at[ITERS])
    for turn, device in plane_peers[8:]:
        send(used, used, device, 1, plane_sem.at[ITERS + (4 - turn) % 4])
    column_in[my_z] = plane_in[my_p]

    rows8, rows16 = row_iota(8), row_iota(16)
    scale = float(PLANE * DEPTH * LANES) ** (-0.5)

    def one_source_block(s):
        block = plane_in[s]
        lanes = pl.ds(pl.multiple_of(s * LANES, LANES), LANES)
        y = [block[b:b + 1] for b in range(3)]
        weight = block[3:4] * scale
        square = y[0] * y[0] + y[1] * y[1] + y[2] * y[2]
        feature = jnp.where(
            rows8 < 3, block, jnp.where(rows8 == 3, square, jnp.where(rows8 == 4, 1.0, 0.0))
        )
        m1, m2, m3 = split3(feature)
        sf[0:16, lanes] = jnp.concatenate([m1, m2], axis=0).astype(BF16)
        sf[16:32, lanes] = jnp.concatenate([m1, m3], axis=0).astype(BF16)
        sf[32:48, lanes] = jnp.concatenate([m1, m2], axis=0).astype(BF16)
        sf[48:64, lanes] = jnp.concatenate([m2, m3], axis=0).astype(BF16)
        chosen = jnp.zeros((16, LANES), F32)
        for b in range(3):
            mine = ((rows16 >= 3 + 3 * b) & (rows16 < 6 + 3 * b)) | (rows16 == 12 + b)
            chosen = jnp.where(mine, y[b], chosen)
        total = jnp.zeros((16, LANES), F32)
        for b in range(3):
            linear = (rows16 == 3 + b) | (rows16 == 6 + b) | (rows16 == 9 + b)
            last = (rows16 >= 12) & (rows16 < 15)
            value = jnp.where(
                rows16 == b, 1.0, jnp.where(linear, chosen, jnp.where(last, chosen * y[b], 0.0))
            )
            value = value + jnp.where(rows16 == 12 + b, square + 2.0 * soften, 0.0)
            value = value * weight
            coef[b, :, lanes] = value
            total = total + value * block[4 + b:5 + b]
        for piece, part in enumerate(split3(total)):
            psi[16 * piece:16 * piece + 16, lanes] = part.astype(BF16)
        plane_u[0, s] = block[4:8]

    def source_rows(turn, count):
        arrived(plane_in.at[pl.ds(0, count), 0:7], plane_sem.at[ITERS + turn])
        first = ((my_y + turn) % 4) * 8

        def body(s, carry):
            one_source_block(first + s)
            return carry

        lax.fori_loop(0, 8, body, 0, unroll=turn == 2)

    source_rows(0, 7)
    source_rows(1, 8)
    source_rows(3, 8)

    arrived(column_in.at[pl.ds(0, DEPTH - 1), 0:7], column_sem.at[ITERS])
    for t in range(DEPTH):
        block = column_in[t]
        lanes = pl.ds(t * LANES, LANES)
        x = [block[b:b + 1] for b in range(3)]
        square = x[0] * x[0] + x[1] * x[1] + x[2] * x[2]
        feature = jnp.where(
            rows8 < 3, -2.0 * block,
            jnp.where(rows8 == 3, 1.0, jnp.where(rows8 == 4, square + soften, 0.0)),
        )
        t1, t2, t3 = split3(feature)
        tf[0:16, lanes] = jnp.concatenate([t1, t1], axis=0).astype(BF16)
        tf[16:32, lanes] = jnp.concatenate([t2, t1], axis=0).astype(BF16)
        tf[32:48, lanes] = jnp.concatenate([t3, t2], axis=0).astype(BF16)
        tf[48:64, lanes] = jnp.concatenate([t3, t2], axis=0).astype(BF16)
        for a in range(3):
            value = jnp.zeros((16, LANES), F32)
            for b in range(3):
                value = jnp.where(rows16 == b, x[a] * x[b] + (square if a == b else 0.0), value)
                for c in range(3):
                    part = jnp.zeros((1, LANES), F32)
                    if c == a:
                        part = part - 2.0 * x[b]
                    if b == c:
                        part = part - x[a]
                    if b == a:
                        part = part - x[c]
                    value = jnp.where(rows16 == 3 + 3 * b + c, part, value)
            phi[a, :, lanes] = jnp.where(rows16 == 12 + a, 1.0, value)
        column_u[0, t] = block[4:8]

    source_rows(2, 8)

    lane_row = lax.broadcasted_iota(jnp.int32, (1, LANES), 1)
    hes_rows, hes_lanes = row_iota(8), lax.broadcasted_iota(jnp.int32, (8, LANES), 1)

    def at_lane(lane, value):
        return jnp.where(lane_row == lane, value, 0.0)

    def to_parts(k, b, both, dots):
        summed = both[0:16] + both[16:32] + both[32:48]
        dots = list(dots)
        for a in range(3):
            row = jnp.sum(phi[a, :, b * WIDE:(b + 1) * WIDE] * summed, axis=0, keepdims=True)
            for c in range(WIDE // LANES):
                t, piece = b * (WIDE // LANES) + c, row[:, c * LANES:(c + 1) * LANES]
                part_out[k, t, a:a + 1, :] = piece
                for i in range(len(dots)):
                    dots[i] = dots[i] + column_u[i, t, a:a + 1, :] * piece
        return dots

    def with_dots(k, dots):
        row = jnp.zeros((1, LANES), F32)
        for i in range(len(dots)):
            row = row + at_lane(i, jnp.sum(dots[i], axis=1, keepdims=True))
        for t in range(DEPTH):
            part_out[k, t, 3:4, :] = row

    dots = [jnp.zeros((1, LANES), F32)]
    for b in range(BLOCKS):
        both = jnp.zeros((48, WIDE), F32)
        for q in range(0, sources, CHUNK):
            square = lax.dot_general(
                sf[:, q:q + CHUNK], tf[:, b * WIDE:(b + 1) * WIDE], (((0,), (0,)), ((), ())),
                preferred_element_type=F32,
            )
            root = lax.rsqrt(square)
            factor = root * root * root
            high = factor.astype(BF16)
            low = (factor - high.astype(F32)).astype(BF16)
            matrix[b, q:q + CHUNK, 0:WIDE] = high
            matrix[b, q:q + CHUNK, WIDE:2 * WIDE] = low
            left = psi[:, q:q + CHUNK]
            both = both + (
                jnp.dot(left, high, preferred_element_type=F32)
                + jnp.dot(left, low, preferred_element_type=F32)
            )
        dots = to_parts(0, b, both, dots)
    with_dots(0, dots)

    def inner(left, right):
        return total_of(jnp.sum(left * right, axis=0)[0:3])

    def grams(k):
        latest = column_u[k]
        values = [inner(column_u[i], latest) for i in range(k + 1)]
        row = at_lane(6, values[k])
        for i in range(k + 1):
            row = row + at_lane(8 + i, values[i])
        return row, values

    def exchange(k, with_column):
        whole = slice(0, 4) if with_column else slice(3, 4)
        message = plane_w.at[k, my_p, whole]
        if with_column:
            for _, device in plane_peers[:16]:
                send(message, message, device, 1, plane_sem.at[k])
            for device in column_peers:
                send(message, column_w.at[k, my_z], device, 0, column_sem.at[k])
            for _, device in plane_peers[16:]:
                send(message, message, device, 1, plane_sem.at[k])
        else:
            for _, device in plane_peers:
                send(message, message, device, 1, plane_sem.at[k])
        arrived(plane_w.at[k, pl.ds(0, PLANE - 1), whole], plane_sem.at[k])
        sums = jnp.sum(plane_w[k, :, 3, :], axis=0, keepdims=True)
        gram[k:k + 1, :] = sums
        norm = jnp.sqrt(sums[:, 6:7])
        scaled = 1.0 / norm
        inverse[k:k + 1, :] = jnp.broadcast_to(scaled, (1, LANES))
        table = hes[0:8]
        if k > 0:
            table = jnp.where((hes_rows == k) & (hes_lanes == k - 1), norm, table)
        factors = []
        for i in range(k + 1):
            present = scaled if i == k else inverse[i:i + 1, 0:1]
            value = sums[:, i:i + 1] * present * scaled
            table = jnp.where((hes_rows == i) & (hes_lanes == k), value, table)
            factors.append(value * present)
        hes[0:8] = table
        if k == 0:
            hes[8:9] = jnp.broadcast_to(norm, (1, LANES))
        return scaled, factors

    sent(plane_in.at[pl.ds(0, DEPTH - 1), 0:7], 0)
    sent(plane_in.at[pl.ds(0, PLANE - 1), 0:7], 1)

    def last_parts(first, slot):
        half = pl.ds(first, DEPTH // 2)
        for device in column_peers:
            send(
                part_out.at[ITERS - 1, half, 0:3], part_all.at[my_z, half, 0:3], device, 2 + slot,
                part_sem.at[ITERS - 1 + slot],
            )

    for k in range(ITERS - 1):
        for device in column_peers:
            send(part_out.at[k, device[0]], part_in.at[k, my_z], device, 2, part_sem.at[k])
        part_in[k, my_z] = part_out[k, my_z]
        row, values = grams(k)
        for i in range(k + 1):
            row = row + at_lane(i, values[i])
        applied = column_u[k, my_z]
        arrived(part_in.at[k, pl.ds(0, DEPTH - 1)], part_sem.at[k])
        summed = part_in[k, 0]
        for z in range(1, DEPTH):
            summed = summed + part_in[k, z]
        applied = applied + summed
        plane_w[k, my_p] = jnp.concatenate([applied[0:3], summed[3:4] + row], axis=0)
        column_w[k, my_z] = plane_w[k, my_p]
        scaled, factors = exchange(k, True)
        for s in range(PLANE):
            lanes = slice(s * LANES, (s + 1) * LANES)
            fresh = plane_w[k, s] * scaled
            for i in range(k + 1):
                fresh = fresh - factors[i] * plane_u[i, s]
            plane_u[k + 1, s] = fresh
            value = (
                coef[0, :, lanes] * fresh[0:1]
                + coef[1, :, lanes] * fresh[1:2]
                + coef[2, :, lanes] * fresh[2:3]
            )
            for piece, part in enumerate(split3(value)):
                psi[16 * piece:16 * piece + 16, lanes] = part.astype(BF16)
        arrived(column_w.at[k, pl.ds(0, DEPTH - 1)], column_sem.at[k])
        fresh = column_w[k] * scaled
        for i in range(k + 1):
            fresh = fresh - factors[i] * column_u[i]
        column_u[k + 1] = fresh
        sent(plane_w.at[0, pl.ds(0, DEPTH - 1)], 2)
        sent(plane_w.at[0, pl.ds(0, DEPTH - 1)], 0)
        sent(plane_w.at[0, pl.ds(0, PLANE - 1)], 1)
        final = k + 1 == ITERS - 1
        dots = [jnp.zeros((1, LANES), F32)] * (0 if final else k + 2)
        for b in range(BLOCKS):
            both = jnp.zeros((48, WIDE), F32)
            for q in range(0, sources, DEEP):
                product = jnp.dot(
                    psi[:, q:q + DEEP], matrix[b, q:q + DEEP], preferred_element_type=F32
                )
                both = both + (product[:, 0:WIDE] + product[:, WIDE:2 * WIDE])
            dots = to_parts(k + 1, b, both, dots)
            if final and b == BLOCKS // 2 - 1:
                last_parts(0, 0)
        if final:
            last_parts(DEPTH // 2, 1)
        else:
            with_dots(k + 1, dots)

    k = ITERS - 1
    part_all[my_z] = part_out[k]
    row, _ = grams(k)
    for slot in range(2):
        arrived(part_all.at[pl.ds(0, DEPTH - 1), pl.ds(0, DEPTH // 2), 0:3], part_sem.at[k + slot])
    applied = column_u[k]
    for z in range(DEPTH):
        applied = applied + part_all[z]
    row = row + at_lane(4, inner(applied, applied))
    for i in range(ITERS):
        row = row + at_lane(i, inner(column_u[i], applied))
    column_u[k + 1] = applied
    plane_w[k, my_p] = jnp.concatenate([applied[0, 0:3], row], axis=0)
    scaled, factors = exchange(k, False)
    fresh = column_u[k + 1, my_z] * scaled
    for i in range(ITERS):
        fresh = fresh - factors[i] * column_u[i, my_z]
    column_u[k + 1, my_z] = fresh

    present = [inverse[i:i + 1, 0:1] for i in range(ITERS)]
    tall = [hes[i:i + 1, ITERS - 1:ITERS] for i in range(ITERS)]
    whole = gram[ITERS - 1:ITERS, 4:5] * present[-1] * present[-1]
    square = whole
    for i in range(ITERS):
        square = square - tall[i] * tall[i]
        for j in range(i + 1, ITERS):
            square = square + 2.0 * (tall[i] * present[i]) * (tall[j] * present[j]) * (
                gram[j:j + 1, 8 + i:9 + i]
            )
    norm = jnp.sqrt(jnp.maximum(square, whole * 1e-14))
    inverse[ITERS:ITERS + 1, :] = jnp.broadcast_to(1.0 / norm, (1, LANES))
    table = jnp.where((hes_rows == ITERS) & (hes_lanes == ITERS - 1), norm, hes[0:8])
    packed_ref[8:16] = table
    entry = [[table[i:i + 1, k:k + 1] for k in range(ITERS)] for i in range(ITERS + 1)]
    beta = hes[8:9, 0:1]
    y = least_squares(
        [[entry[i][k] for i in range(k + 1)] for k in range(ITERS)],
        [entry[k + 1][k] for k in range(ITERS)],
        beta,
    )
    solved = jnp.zeros((4, LANES), F32)
    misfit = jnp.zeros((4, LANES), F32)
    for i in range(ITERS + 1):
        basis = column_u[i, my_z] * inverse[i:i + 1, :]
        if i < ITERS:
            solved = solved + y[i] * basis
        g = beta if i == 0 else jnp.zeros_like(beta)
        for k in range(max(i - 1, 0), ITERS):
            g = g - entry[i][k] * y[k]
        misfit = misfit + g * basis
    packed_ref[0:4] = solved
    packed_ref[4:8] = misfit
    for slot in range(2):
        sent(part_all.at[pl.ds(0, DEPTH - 1), pl.ds(0, DEPTH // 2), 0:3], 2 + slot)
    sent(plane_w.at[0, pl.ds(0, PLANE - 1), 3:4], 1)


def unpack(packed_ref, sol_ref, res_ref, hes_ref):
    sol_ref[...] = packed_ref[0:3]
    res_ref[...] = packed_ref[4:7]
    hes_ref[...] = packed_ref[8:16].T[0:ITERS, 0:ITERS + 1]


def shards(positions, areas, right_side):
    vmem = pl.BlockSpec(memory_space=pltpu.VMEM)
    sources, targets = PLANE * LANES, DEPTH * LANES
    packed = pl.pallas_call(
        kernel,
        out_shape=pltpu.VMEM((16, LANES), F32),
        in_specs=[pl.BlockSpec(memory_space=pl.ANY)] * 3,
        out_specs=vmem,
        scratch_shapes=[
            pltpu.VMEM((PLANE, 8, LANES), F32),
            pltpu.VMEM((DEPTH, 8, LANES), F32),
            pltpu.VMEM((BLOCKS, sources, 2 * WIDE), BF16),
            pltpu.VMEM((64, sources), BF16),
            pltpu.VMEM((64, targets), BF16),
            pltpu.VMEM((3, 16, sources), F32),
            pltpu.VMEM((3, 16, targets), F32),
            pltpu.VMEM((48, sources), BF16),
            pltpu.VMEM((ITERS, PLANE, 4, LANES), F32),
            pltpu.VMEM((ITERS, DEPTH, 4, LANES), F32),
            pltpu.VMEM((ITERS, DEPTH, 4, LANES), F32),
            pltpu.VMEM((ITERS, DEPTH, 4, LANES), F32),
            pltpu.VMEM((DEPTH, DEPTH, 4, LANES), F32),
            pltpu.VMEM((ITERS + 1, PLANE, 4, LANES), F32),
            pltpu.VMEM((ITERS + 1, DEPTH, 4, LANES), F32),
            pltpu.VMEM((8, LANES), F32),
            pltpu.VMEM((16, LANES), F32),
            pltpu.VMEM((8, LANES), F32),
            pltpu.SemaphoreType.DMA((3,)),
            pltpu.SemaphoreType.DMA((4,)),
            pltpu.SemaphoreType.DMA((ITERS + 4,)),
            pltpu.SemaphoreType.DMA((ITERS + 1,)),
            pltpu.SemaphoreType.DMA((ITERS + 1,)),
        ],
        compiler_params=pltpu.CompilerParams(
            collective_id=0, has_side_effects=True, vmem_limit_bytes=56 * 1024 * 1024
        ),
        name="arnoldi",
    )(positions, areas.reshape(1, -1), right_side)
    solved, misfit, turned = pl.pallas_call(
        unpack,
        out_shape=(
            jax.ShapeDtypeStruct((3, LANES), F32),
            jax.ShapeDtypeStruct((3, LANES), F32),
            jax.ShapeDtypeStruct((ITERS, ITERS + 1), F32),
        ),
        in_specs=[vmem],
        out_specs=(vmem,) * 3,
        name="unpack",
    )(pltpu.with_memory_space_constraint(packed, pltpu.VMEM))
    return solved, misfit, turned.T


def solution(mesh):
    split = Mesh(mesh.devices.reshape(DEPTH, PLANE), ("z", "p"))
    return jax.shard_map(
        shards,
        mesh=split,
        in_specs=(P(None, ("z", "p")), P(("z", "p")), P(None, ("z", "p"))),
        out_specs=(P(None, ("z", "p")), P(None, ("z", "p")), P()),
        check_vma=False,
    )
```

```python
import functools

import jax
import jax.numpy as jnp
from jax import lax
from jax.experimental import pallas as pl
from jax.experimental.pallas import tpu as pltpu
from jax.sharding import Mesh
from jax.sharding import PartitionSpec as P

ITERS = 4
soften = 0.0025
LANES = 128
WIDE = 256
CHUNK = 512
DEEP = 512
DEPTH = 8
PLANE = 32
BLOCKS = DEPTH * LANES // WIDE
MESH = pl.DeviceIdType.MESH
F32 = jnp.float32
BF16 = jnp.bfloat16


def split3(value):
    first = value.astype(BF16).astype(F32)
    rest = value - first
    second = rest.astype(BF16).astype(F32)
    return first, second, rest - second


def row_iota(rows):
    return lax.broadcasted_iota(jnp.int32, (rows, LANES), 0)


def total_of(value):
    return jnp.sum(jnp.sum(value, axis=0, keepdims=True), axis=1, keepdims=True)


def least_squares(columns, heights, beta):
    zero = jnp.zeros_like(beta)
    size = len(columns)
    table = [[zero] * size for _ in range(size + 1)]
    for k in range(size):
        for i in range(k + 1):
            table[i][k] = columns[k][i]
        table[k + 1][k] = heights[k]
    target = [beta] + [zero] * size
    for c in range(size):
        lead, second = table[c][c], table[c + 1][c]
        radius = jnp.sqrt(lead * lead + second * second)
        cosine, sine = lead / radius, second / radius
        top, low = table[c], table[c + 1]
        new_top = [cosine * t + sine * l for t, l in zip(top, low)]
        new_low = [cosine * l - sine * t for t, l in zip(top, low)]
        table[c], table[c + 1] = new_top, new_low
        a, b = target[c], target[c + 1]
        target[c], target[c + 1] = cosine * a + sine * b, cosine * b - sine * a
    y = [zero] * size
    for r in reversed(range(size)):
        partial = zero
        for c in range(r + 1, size):
            partial = partial + table[r][c] * y[c]
        y[r] = (target[r] - partial) / table[r][r]
    return y


def kernel(
    pos_ref, area_ref, rhs_ref, packed_ref,
    plane_in, column_in, matrix, sf, tf, coef, phi, psi,
    plane_w, column_w, part_out, part_in, part_all, plane_u, column_u, gram, hes, inverse,
    load_sem, send_sem, plane_sem, column_sem, part_sem,
):
    my_z = lax.axis_index("z")
    my_p = lax.axis_index("p")
    my_y, my_x = my_p // 8, (my_p % 2) * 2 + (my_p // 4) % 2
    my_c = (my_p // 2) % 2
    sources = PLANE * LANES

    ys = [((my_y + d) % 4) * 8 for d in range(4)]
    xs = [((my_x + d) % 4) for d in range(4)]
    xs = [(x % 2) * 4 + x // 2 for x in xs]
    cs = [((my_c + d) % 2) * 2 for d in range(2)]
    hops = (0, 1, 2, 1)
    steps = [(a, b, c) for a in range(4) for b in range(4) for c in range(2)][1:]
    steps.sort(key=lambda s: -(4 * (hops[s[0]] + hops[s[1]]) + s[2]))
    plane_peers = [(s[0], (my_z, ys[s[0]] + xs[s[1]] + cs[s[2]])) for s in steps]
    column_peers = [((my_z + d) % DEPTH, my_p) for d in (4, 3, 5, 2, 6, 1, 7)]

    barrier = pltpu.get_barrier_semaphore()
    own = plane_in.at[my_p]
    loads = [
        pltpu.make_async_copy(pos_ref, own.at[0:3], load_sem.at[0]),
        pltpu.make_async_copy(area_ref, own.at[3:4], load_sem.at[1]),
        pltpu.make_async_copy(rhs_ref, own.at[4:7], load_sem.at[2]),
    ]
    for load in loads:
        load.start()
    for device in column_peers + [peer for _, peer in plane_peers]:
        pl.semaphore_signal(barrier, inc=1, device_id=device, device_id_type=MESH)
    for load in loads:
        load.wait()
    pl.semaphore_wait(barrier, PLANE - 1 + DEPTH - 1)

    def send(src, dst, device, slot, recv_sem):
        pltpu.make_async_remote_copy(
            src_ref=src, dst_ref=dst, send_sem=send_sem.at[slot], recv_sem=recv_sem,
            device_id=device, device_id_type=MESH,
        ).start()

    def arrived(part, recv_sem):
        pltpu.make_async_remote_copy(
            src_ref=part, dst_ref=part, send_sem=send_sem.at[0], recv_sem=recv_sem,
            device_id=(my_z, my_p), device_id_type=MESH,
        ).wait_recv()

    def sent(part, slot):
        pltpu.make_async_remote_copy(
            src_ref=part, dst_ref=part, send_sem=send_sem.at[slot], recv_sem=load_sem.at[0],
            device_id=(my_z, my_p), device_id_type=MESH,
        ).wait_send()

    used = own.at[0:7]
    for turn, device in plane_peers[:8]:
        send(used, used, device, 1, plane_sem.at[ITERS + (4 - turn) % 4])
    for device in column_peers:
        send(used, column_in.at[my_z, 0:7], device, 0, column_sem.at[ITERS])
    for turn, device in plane_peers[8:]:
        send(used, used, device, 1, plane_sem.at[ITERS + (4 - turn) % 4])
    plane_in[:, 7:8, :] = jnp.zeros((PLANE, 1, LANES), F32)
    column_in[:, 7:8, :] = jnp.zeros((DEPTH, 1, LANES), F32)
    column_in[my_z] = plane_in[my_p]
    hes[...] = jnp.zeros_like(hes)
    part_out[ITERS - 1] = jnp.zeros((DEPTH, 4, LANES), F32)

    rows8, rows16 = row_iota(8), row_iota(16)
    scale = float(PLANE * DEPTH * LANES) ** (-0.5)

    def one_source_block(s):
        block = plane_in[s]
        lanes = pl.ds(pl.multiple_of(s * LANES, LANES), LANES)
        y = [block[b:b + 1] for b in range(3)]
        weight = block[3:4] * scale
        square = y[0] * y[0] + y[1] * y[1] + y[2] * y[2]
        feature = jnp.where(
            rows8 < 3, block, jnp.where(rows8 == 3, square, jnp.where(rows8 == 4, 1.0, 0.0))
        )
        m1, m2, m3 = split3(feature)
        sf[0:16, lanes] = jnp.concatenate([m1, m2], axis=0).astype(BF16)
        sf[16:32, lanes] = jnp.concatenate([m1, m3], axis=0).astype(BF16)
        sf[32:48, lanes] = jnp.concatenate([m1, m2], axis=0).astype(BF16)
        sf[48:64, lanes] = jnp.concatenate([m2, m3], axis=0).astype(BF16)
        chosen = jnp.zeros((16, LANES), F32)
        for b in range(3):
            mine = ((rows16 >= 3 + 3 * b) & (rows16 < 6 + 3 * b)) | (rows16 == 12 + b)
            chosen = jnp.where(mine, y[b], chosen)
        total = jnp.zeros((16, LANES), F32)
        for b in range(3):
            linear = (rows16 == 3 + b) | (rows16 == 6 + b) | (rows16 == 9 + b)
            last = (rows16 >= 12) & (rows16 < 15)
            value = jnp.where(
                rows16 == b, 1.0, jnp.where(linear, chosen, jnp.where(last, chosen * y[b], 0.0))
            )
            value = value + jnp.where(rows16 == 12 + b, square + 2.0 * soften, 0.0)
            value = value * weight
            coef[b, :, lanes] = value
            total = total + value * block[4 + b:5 + b]
        for piece, part in enumerate(split3(total)):
            psi[16 * piece:16 * piece + 16, lanes] = part.astype(BF16)
        plane_u[0, s] = block[4:8]

    def source_rows(turn, count):
        arrived(plane_in.at[pl.ds(0, count), 0:7], plane_sem.at[ITERS + turn])
        first = ((my_y + turn) % 4) * 8

        def body(s, carry):
            one_source_block(first + s)
            return carry

        lax.fori_loop(0, 8, body, 0, unroll=turn == 2)

    source_rows(0, 7)
    source_rows(1, 8)
    source_rows(3, 8)

    arrived(column_in.at[pl.ds(0, DEPTH - 1), 0:7], column_sem.at[ITERS])
    for t in range(DEPTH):
        block = column_in[t]
        lanes = pl.ds(t * LANES, LANES)
        x = [block[b:b + 1] for b in range(3)]
        square = x[0] * x[0] + x[1] * x[1] + x[2] * x[2]
        feature = jnp.where(
            rows8 < 3, -2.0 * block,
            jnp.where(rows8 == 3, 1.0, jnp.where(rows8 == 4, square + soften, 0.0)),
        )
        t1, t2, t3 = split3(feature)
        tf[0:16, lanes] = jnp.concatenate([t1, t1], axis=0).astype(BF16)
        tf[16:32, lanes] = jnp.concatenate([t2, t1], axis=0).astype(BF16)
        tf[32:48, lanes] = jnp.concatenate([t3, t2], axis=0).astype(BF16)
        tf[48:64, lanes] = jnp.concatenate([t3, t2], axis=0).astype(BF16)
        for a in range(3):
            value = jnp.zeros((16, LANES), F32)
            for b in range(3):
                value = jnp.where(rows16 == b, x[a] * x[b] + (square if a == b else 0.0), value)
                for c in range(3):
                    part = jnp.zeros((1, LANES), F32)
                    if c == a:
                        part = part - 2.0 * x[b]
                    if b == c:
                        part = part - x[a]
                    if b == a:
                        part = part - x[c]
                    value = jnp.where(rows16 == 3 + 3 * b + c, part, value)
            phi[a, :, lanes] = jnp.where(rows16 == 12 + a, 1.0, value)
        column_u[0, t] = block[4:8]

    source_rows(2, 8)

    lane_row = lax.broadcasted_iota(jnp.int32, (1, LANES), 1)
    hes_rows, hes_lanes = row_iota(8), lax.broadcasted_iota(jnp.int32, (8, LANES), 1)

    def at_lane(lane, value):
        return jnp.where(lane_row == lane, value, 0.0)

    def to_parts(k, b, both, dots):
        summed = both[0:16] + both[16:32] + both[32:48]
        dots = list(dots)
        for a in range(3):
            row = jnp.sum(phi[a, :, b * WIDE:(b + 1) * WIDE] * summed, axis=0, keepdims=True)
            for c in range(WIDE // LANES):
                t, piece = b * (WIDE // LANES) + c, row[:, c * LANES:(c + 1) * LANES]
                part_out[k, t, a:a + 1, :] = piece
                for i in range(len(dots)):
                    dots[i] = dots[i] + column_u[i, t, a:a + 1, :] * piece
        return dots

    def with_dots(k, dots):
        row = jnp.zeros((1, LANES), F32)
        for i in range(len(dots)):
            row = row + at_lane(i, jnp.sum(dots[i], axis=1, keepdims=True))
        for t in range(DEPTH):
            part_out[k, t, 3:4, :] = row

    dots = [jnp.zeros((1, LANES), F32)]
    for b in range(BLOCKS):
        both = jnp.zeros((48, WIDE), F32)
        for q in range(0, sources, CHUNK):
            square = lax.dot_general(
                sf[:, q:q + CHUNK], tf[:, b * WIDE:(b + 1) * WIDE], (((0,), (0,)), ((), ())),
                preferred_element_type=F32,
            )
            root = lax.rsqrt(square)
            factor = root * root * root
            high = factor.astype(BF16)
            low = (factor - high.astype(F32)).astype(BF16)
            matrix[b, q:q + CHUNK, 0:WIDE] = high
            matrix[b, q:q + CHUNK, WIDE:2 * WIDE] = low
            left = psi[:, q:q + CHUNK]
            both = both + (
                jnp.dot(left, high, preferred_element_type=F32)
                + jnp.dot(left, low, preferred_element_type=F32)
            )
        dots = to_parts(0, b, both, dots)
    with_dots(0, dots)

    def inner(left, right):
        return total_of(jnp.sum(left * right, axis=0)[0:3])

    def grams(k):
        latest = column_u[k]
        values = [inner(column_u[i], latest) for i in range(k + 1)]
        row = at_lane(6, values[k])
        for i in range(k + 1):
            row = row + at_lane(8 + i, values[i])
        return row, values

    def exchange(k, with_column):
        whole = slice(0, 4) if with_column else slice(3, 4)
        message = plane_w.at[k, my_p, whole]
        if with_column:
            for _, device in plane_peers[:16]:
                send(message, message, device, 1, plane_sem.at[k])
            for device in column_peers:
                send(message, column_w.at[k, my_z], device, 0, column_sem.at[k])
            for _, device in plane_peers[16:]:
                send(message, message, device, 1, plane_sem.at[k])
        else:
            for _, device in plane_peers:
                send(message, message, device, 1, plane_sem.at[k])
        arrived(plane_w.at[k, pl.ds(0, PLANE - 1), whole], plane_sem.at[k])
        sums = jnp.sum(plane_w[k, :, 3, :], axis=0, keepdims=True)
        gram[k:k + 1, :] = sums
        norm = jnp.sqrt(sums[:, 6:7])
        scaled = 1.0 / norm
        inverse[k:k + 1, :] = jnp.broadcast_to(scaled, (1, LANES))
        table = hes[0:8]
        if k > 0:
            table = jnp.where((hes_rows == k) & (hes_lanes == k - 1), norm, table)
        factors = []
        for i in range(k + 1):
            present = scaled if i == k else inverse[i:i + 1, 0:1]
            value = sums[:, i:i + 1] * present * scaled
            table = jnp.where((hes_rows == i) & (hes_lanes == k), value, table)
            factors.append(value * present)
        hes[0:8] = table
        if k == 0:
            hes[8:9] = jnp.broadcast_to(norm, (1, LANES))
        return scaled, factors

    sent(plane_in.at[pl.ds(0, DEPTH - 1), 0:7], 0)
    sent(plane_in.at[pl.ds(0, PLANE - 1), 0:7], 1)

    def last_parts(first, slot):
        half = pl.ds(first, DEPTH // 2)
        for device in column_peers:
            send(
                part_out.at[ITERS - 1, half, 0:3], part_all.at[my_z, half, 0:3], device, 2 + slot,
                part_sem.at[ITERS - 1 + slot],
            )

    for k in range(ITERS - 1):
        for device in column_peers:
            send(part_out.at[k, device[0]], part_in.at[k, my_z], device, 2, part_sem.at[k])
        part_in[k, my_z] = part_out[k, my_z]
        row, values = grams(k)
        for i in range(k + 1):
            row = row + at_lane(i, values[i])
        applied = column_u[k, my_z]
        arrived(part_in.at[k, pl.ds(0, DEPTH - 1)], part_sem.at[k])
        summed = part_in[k, 0]
        for z in range(1, DEPTH):
            summed = summed + part_in[k, z]
        applied = applied + summed
        plane_w[k, my_p] = jnp.concatenate([applied[0:3], summed[3:4] + row], axis=0)
        column_w[k, my_z] = plane_w[k, my_p]
        scaled, factors = exchange(k, True)
        for s in range(PLANE):
            lanes = slice(s * LANES, (s + 1) * LANES)
            fresh = plane_w[k, s] * scaled
            for i in range(k + 1):
                fresh = fresh - factors[i] * plane_u[i, s]
            plane_u[k + 1, s] = fresh
            value = (
                coef[0, :, lanes] * fresh[0:1]
                + coef[1, :, lanes] * fresh[1:2]
                + coef[2, :, lanes] * fresh[2:3]
            )
            for piece, part in enumerate(split3(value)):
                psi[16 * piece:16 * piece + 16, lanes] = part.astype(BF16)
        arrived(column_w.at[k, pl.ds(0, DEPTH - 1)], column_sem.at[k])
        fresh = column_w[k] * scaled
        for i in range(k + 1):
            fresh = fresh - factors[i] * column_u[i]
        column_u[k + 1] = fresh
        sent(plane_w.at[0, pl.ds(0, DEPTH - 1)], 2)
        sent(plane_w.at[0, pl.ds(0, DEPTH - 1)], 0)
        sent(plane_w.at[0, pl.ds(0, PLANE - 1)], 1)
        final = k + 1 == ITERS - 1
        dots = [jnp.zeros((1, LANES), F32)] * (0 if final else k + 2)
        for b in range(BLOCKS):
            both = jnp.zeros((48, WIDE), F32)
            for q in range(0, sources, DEEP):
                product = jnp.dot(
                    psi[:, q:q + DEEP], matrix[b, q:q + DEEP], preferred_element_type=F32
                )
                both = both + (product[:, 0:WIDE] + product[:, WIDE:2 * WIDE])
            dots = to_parts(k + 1, b, both, dots)
            if final and b == BLOCKS // 2 - 1:
                last_parts(0, 0)
        if final:
            last_parts(DEPTH // 2, 1)
        else:
            with_dots(k + 1, dots)

    k = ITERS - 1
    part_all[my_z] = part_out[k]
    row, _ = grams(k)
    for slot in range(2):
        arrived(part_all.at[pl.ds(0, DEPTH - 1), pl.ds(0, DEPTH // 2), 0:3], part_sem.at[k + slot])
    applied = column_u[k]
    for z in range(DEPTH):
        applied = applied + part_all[z]
    row = row + at_lane(4, inner(applied, applied))
    for i in range(ITERS):
        row = row + at_lane(i, inner(column_u[i], applied))
    column_u[k + 1] = applied
    plane_w[k, my_p] = jnp.concatenate([applied[0, 0:3], row], axis=0)
    scaled, factors = exchange(k, False)
    fresh = column_u[k + 1, my_z] * scaled
    for i in range(ITERS):
        fresh = fresh - factors[i] * column_u[i, my_z]
    column_u[k + 1, my_z] = fresh

    present = [inverse[i:i + 1, 0:1] for i in range(ITERS)]
    tall = [hes[i:i + 1, ITERS - 1:ITERS] for i in range(ITERS)]
    whole = gram[ITERS - 1:ITERS, 4:5] * present[-1] * present[-1]
    square = whole
    for i in range(ITERS):
        square = square - tall[i] * tall[i]
        for j in range(i + 1, ITERS):
            square = square + 2.0 * (tall[i] * present[i]) * (tall[j] * present[j]) * (
                gram[j:j + 1, 8 + i:9 + i]
            )
    norm = jnp.sqrt(jnp.maximum(square, whole * 1e-14))
    inverse[ITERS:ITERS + 1, :] = jnp.broadcast_to(1.0 / norm, (1, LANES))
    table = jnp.where((hes_rows == ITERS) & (hes_lanes == ITERS - 1), norm, hes[0:8])
    packed_ref[8:16] = table
    entry = [[table[i:i + 1, k:k + 1] for k in range(ITERS)] for i in range(ITERS + 1)]
    beta = hes[8:9, 0:1]
    y = least_squares(
        [[entry[i][k] for i in range(k + 1)] for k in range(ITERS)],
        [entry[k + 1][k] for k in range(ITERS)],
        beta,
    )
    solved = jnp.zeros((4, LANES), F32)
    misfit = jnp.zeros((4, LANES), F32)
    for i in range(ITERS + 1):
        basis = column_u[i, my_z] * inverse[i:i + 1, :]
        if i < ITERS:
            solved = solved + y[i] * basis
        g = beta if i == 0 else jnp.zeros_like(beta)
        for k in range(max(i - 1, 0), ITERS):
            g = g - entry[i][k] * y[k]
        misfit = misfit + g * basis
    packed_ref[0:4] = solved
    packed_ref[4:8] = misfit
    for slot in range(2):
        sent(part_all.at[pl.ds(0, DEPTH - 1), pl.ds(0, DEPTH // 2), 0:3], 2 + slot)
    sent(plane_w.at[0, pl.ds(0, PLANE - 1), 3:4], 1)


def unpack(packed_ref, sol_ref, res_ref, hes_ref):
    sol_ref[...] = packed_ref[0:3]
    res_ref[...] = packed_ref[4:7]
    hes_ref[...] = packed_ref[8:16].T[0:ITERS, 0:ITERS + 1]


def shards(positions, areas, right_side):
    vmem = pl.BlockSpec(memory_space=pltpu.VMEM)
    sources, targets = PLANE * LANES, DEPTH * LANES
    packed = pl.pallas_call(
        kernel,
        out_shape=pltpu.VMEM((16, LANES), F32),
        in_specs=[pl.BlockSpec(memory_space=pl.ANY)] * 3,
        out_specs=vmem,
        scratch_shapes=[
            pltpu.VMEM((PLANE, 8, LANES), F32),
            pltpu.VMEM((DEPTH, 8, LANES), F32),
            pltpu.VMEM((BLOCKS, sources, 2 * WIDE), BF16),
            pltpu.VMEM((64, sources), BF16),
            pltpu.VMEM((64, targets), BF16),
            pltpu.VMEM((3, 16, sources), F32),
            pltpu.VMEM((3, 16, targets), F32),
            pltpu.VMEM((48, sources), BF16),
            pltpu.VMEM((ITERS, PLANE, 4, LANES), F32),
            pltpu.VMEM((ITERS, DEPTH, 4, LANES), F32),
            pltpu.VMEM((ITERS, DEPTH, 4, LANES), F32),
            pltpu.VMEM((ITERS, DEPTH, 4, LANES), F32),
            pltpu.VMEM((DEPTH, DEPTH, 4, LANES), F32),
            pltpu.VMEM((ITERS + 1, PLANE, 4, LANES), F32),
            pltpu.VMEM((ITERS + 1, DEPTH, 4, LANES), F32),
            pltpu.VMEM((8, LANES), F32),
            pltpu.VMEM((16, LANES), F32),
            pltpu.VMEM((8, LANES), F32),
            pltpu.SemaphoreType.DMA((3,)),
            pltpu.SemaphoreType.DMA((4,)),
            pltpu.SemaphoreType.DMA((ITERS + 4,)),
            pltpu.SemaphoreType.DMA((ITERS + 1,)),
            pltpu.SemaphoreType.DMA((ITERS + 1,)),
        ],
        compiler_params=pltpu.CompilerParams(
            collective_id=0, has_side_effects=True, vmem_limit_bytes=56 * 1024 * 1024
        ),
        name="arnoldi",
    )(positions, areas.reshape(1, -1), right_side)
    solved, misfit, turned = pl.pallas_call(
        unpack,
        out_shape=(
            jax.ShapeDtypeStruct((3, LANES), F32),
            jax.ShapeDtypeStruct((3, LANES), F32),
            jax.ShapeDtypeStruct((ITERS, ITERS + 1), F32),
        ),
        in_specs=[vmem],
        out_specs=(vmem,) * 3,
        name="unpack",
    )(pltpu.with_memory_space_constraint(packed, pltpu.VMEM))
    return solved, misfit, turned.T


def solution(mesh):
    split = Mesh(mesh.devices.reshape(DEPTH, PLANE), ("z", "p"))
    return jax.shard_map(
        shards,
        mesh=split,
        in_specs=(P(None, ("z", "p")), P(("z", "p")), P(None, ("z", "p"))),
        out_specs=(P(None, ("z", "p")), P(None, ("z", "p")), P()),
        check_vma=False,
    )
```

```python
import functools

import jax
import jax.numpy as jnp
from jax import lax
from jax.experimental import pallas as pl
from jax.experimental.pallas import tpu as pltpu
from jax.sharding import Mesh
from jax.sharding import PartitionSpec as P

ITERS = 4
soften = 0.0025
LANES = 128
WIDE = 256
CHUNK = 512
DEEP = 512
DEPTH = 8
PLANE = 32
BLOCKS = DEPTH * LANES // WIDE
MESH = pl.DeviceIdType.MESH
F32 = jnp.float32
BF16 = jnp.bfloat16


def split3(value):
    first = value.astype(BF16).astype(F32)
    rest = value - first
    second = rest.astype(BF16).astype(F32)
    return first, second, rest - second


def row_iota(rows):
    return lax.broadcasted_iota(jnp.int32, (rows, LANES), 0)


def total_of(value):
    return jnp.sum(jnp.sum(value, axis=0, keepdims=True), axis=1, keepdims=True)


def least_squares(columns, heights, beta):
    zero = jnp.zeros_like(beta)
    size = len(columns)
    table = [[zero] * size for _ in range(size + 1)]
    for k in range(size):
        for i in range(k + 1):
            table[i][k] = columns[k][i]
        table[k + 1][k] = heights[k]
    target = [beta] + [zero] * size
    for c in range(size):
        lead, second = table[c][c], table[c + 1][c]
        radius = jnp.sqrt(lead * lead + second * second)
        cosine, sine = lead / radius, second / radius
        top, low = table[c], table[c + 1]
        new_top = [cosine * t + sine * l for t, l in zip(top, low)]
        new_low = [cosine * l - sine * t for t, l in zip(top, low)]
        table[c], table[c + 1] = new_top, new_low
        a, b = target[c], target[c + 1]
        target[c], target[c + 1] = cosine * a + sine * b, cosine * b - sine * a
    y = [zero] * size
    for r in reversed(range(size)):
        partial = zero
        for c in range(r + 1, size):
            partial = partial + table[r][c] * y[c]
        y[r] = (target[r] - partial) / table[r][r]
    return y


def kernel(
    pos_ref, area_ref, rhs_ref, packed_ref,
    plane_in, column_in, matrix, sf, tf, coef, phi, psi,
    plane_w, column_w, part_out, part_in, part_all, plane_u, column_u, gram, hes, inverse,
    load_sem, send_sem, plane_sem, column_sem, part_sem,
):
    my_z = lax.axis_index("z")
    my_p = lax.axis_index("p")
    my_y, my_x = my_p // 8, (my_p % 2) * 2 + (my_p // 4) % 2
    my_c = (my_p // 2) % 2
    sources = PLANE * LANES

    ys = [((my_y + d) % 4) * 8 for d in range(4)]
    xs = [((my_x + d) % 4) for d in range(4)]
    xs = [(x % 2) * 4 + x // 2 for x in xs]
    cs = [((my_c + d) % 2) * 2 for d in range(2)]
    hops = (0, 1, 2, 1)
    steps = [(a, b, c) for a in range(4) for b in range(4) for c in range(2)][1:]
    steps.sort(key=lambda s: -(4 * (hops[s[0]] + hops[s[1]]) + s[2]))
    plane_peers = [(s[0], (my_z, ys[s[0]] + xs[s[1]] + cs[s[2]])) for s in steps]
    column_peers = [((my_z + d) % DEPTH, my_p) for d in (4, 3, 5, 2, 6, 1, 7)]

    barrier = pltpu.get_barrier_semaphore()
    own = plane_in.at[my_p]
    loads = [
        pltpu.make_async_copy(pos_ref, own.at[0:3], load_sem.at[0]),
        pltpu.make_async_copy(area_ref, own.at[3:4], load_sem.at[1]),
        pltpu.make_async_copy(rhs_ref, own.at[4:7], load_sem.at[2]),
    ]
    for load in loads:
        load.start()
    for device in column_peers + [peer for _, peer in plane_peers]:
        pl.semaphore_signal(barrier, inc=1, device_id=device, device_id_type=MESH)
    for load in loads:
        load.wait()
    pl.semaphore_wait(barrier, PLANE - 1 + DEPTH - 1)

    def send(src, dst, device, slot, recv_sem):
        pltpu.make_async_remote_copy(
            src_ref=src, dst_ref=dst, send_sem=send_sem.at[slot], recv_sem=recv_sem,
            device_id=device, device_id_type=MESH,
        ).start()

    def arrived(part, recv_sem):
        pltpu.make_async_remote_copy(
            src_ref=part, dst_ref=part, send_sem=send_sem.at[0], recv_sem=recv_sem,
            device_id=(my_z, my_p), device_id_type=MESH,
        ).wait_recv()

    def sent(part, slot):
        pltpu.make_async_remote_copy(
            src_ref=part, dst_ref=part, send_sem=send_sem.at[slot], recv_sem=load_sem.at[0],
            device_id=(my_z, my_p), device_id_type=MESH,
        ).wait_send()

    used = own.at[0:7]
    for turn, device in plane_peers[:8]:
        send(used, used, device, 1, plane_sem.at[ITERS + (4 - turn) % 4])
    for device in column_peers:
        send(used, column_in.at[my_z, 0:7], device, 0, column_sem.at[ITERS])
    for turn, device in plane_peers[8:]:
        send(used, used, device, 1, plane_sem.at[ITERS + (4 - turn) % 4])
    plane_in[:, 7:8, :] = jnp.zeros((PLANE, 1, LANES), F32)
    column_in[:, 7:8, :] = jnp.zeros((DEPTH, 1, LANES), F32)
    column_in[my_z] = plane_in[my_p]
    hes[...] = jnp.zeros_like(hes)
    part_out[ITERS - 1] = jnp.zeros((DEPTH, 4, LANES), F32)

    rows8, rows16 = row_iota(8), row_iota(16)
    scale = float(PLANE * DEPTH * LANES) ** (-0.5)

    def one_source_block(s):
        block = plane_in[s]
        lanes = pl.ds(pl.multiple_of(s * LANES, LANES), LANES)
        y = [block[b:b + 1] for b in range(3)]
        weight = block[3:4] * scale
        square = y[0] * y[0] + y[1] * y[1] + y[2] * y[2]
        feature = jnp.where(
            rows8 < 3, block, jnp.where(rows8 == 3, square, jnp.where(rows8 == 4, 1.0, 0.0))
        )
        m1, m2, m3 = split3(feature)
        sf[0:16, lanes] = jnp.concatenate([m1, m2], axis=0).astype(BF16)
        sf[16:32, lanes] = jnp.concatenate([m1, m3], axis=0).astype(BF16)
        sf[32:48, lanes] = jnp.concatenate([m1, m2], axis=0).astype(BF16)
        sf[48:64, lanes] = jnp.concatenate([m2, m3], axis=0).astype(BF16)
        chosen = jnp.zeros((16, LANES), F32)
        for b in range(3):
            mine = ((rows16 >= 3 + 3 * b) & (rows16 < 6 + 3 * b)) | (rows16 == 12 + b)
            chosen = jnp.where(mine, y[b], chosen)
        total = jnp.zeros((16, LANES), F32)
        for b in range(3):
            linear = (rows16 == 3 + b) | (rows16 == 6 + b) | (rows16 == 9 + b)
            last = (rows16 >= 12) & (rows16 < 15)
            value = jnp.where(
                rows16 == b, 1.0, jnp.where(linear, chosen, jnp.where(last, chosen * y[b], 0.0))
            )
            value = value + jnp.where(rows16 == 12 + b, square + 2.0 * soften, 0.0)
            value = value * weight
            coef[b, :, lanes] = value
            total = total + value * block[4 + b:5 + b]
        for piece, part in enumerate(split3(total)):
            psi[16 * piece:16 * piece + 16, lanes] = part.astype(BF16)
        plane_u[0, s] = block[4:8]

    def source_rows(turn, count):
        arrived(plane_in.at[pl.ds(0, count), 0:7], plane_sem.at[ITERS + turn])
        first = ((my_y + turn) % 4) * 8

        def body(s, carry):
            one_source_block(first + s)
            return carry

        lax.fori_loop(0, 8, body, 0, unroll=turn == 2)

    source_rows(0, 7)
    source_rows(1, 8)
    source_rows(3, 8)

    arrived(column_in.at[pl.ds(0, DEPTH - 1), 0:7], column_sem.at[ITERS])
    for t in range(DEPTH):
        block = column_in[t]
        lanes = pl.ds(t * LANES, LANES)
        x = [block[b:b + 1] for b in range(3)]
        square = x[0] * x[0] + x[1] * x[1] + x[2] * x[2]
        feature = jnp.where(
            rows8 < 3, -2.0 * block,
            jnp.where(rows8 == 3, 1.0, jnp.where(rows8 == 4, square + soften, 0.0)),
        )
        t1, t2, t3 = split3(feature)
        tf[0:16, lanes] = jnp.concatenate([t1, t1], axis=0).astype(BF16)
        tf[16:32, lanes] = jnp.concatenate([t2, t1], axis=0).astype(BF16)
        tf[32:48, lanes] = jnp.concatenate([t3, t2], axis=0).astype(BF16)
        tf[48:64, lanes] = jnp.concatenate([t3, t2], axis=0).astype(BF16)
        for a in range(3):
            value = jnp.zeros((16, LANES), F32)
            for b in range(3):
                value = jnp.where(rows16 == b, x[a] * x[b] + (square if a == b else 0.0), value)
                for c in range(3):
                    part = jnp.zeros((1, LANES), F32)
                    if c == a:
                        part = part - 2.0 * x[b]
                    if b == c:
                        part = part - x[a]
                    if b == a:
                        part = part - x[c]
                    value = jnp.where(rows16 == 3 + 3 * b + c, part, value)
            phi[a, :, lanes] = jnp.where(rows16 == 12 + a, 1.0, value)
        column_u[0, t] = block[4:8]

    source_rows(2, 8)

    lane_row = lax.broadcasted_iota(jnp.int32, (1, LANES), 1)
    hes_rows, hes_lanes = row_iota(8), lax.broadcasted_iota(jnp.int32, (8, LANES), 1)

    def at_lane(lane, value):
        return jnp.where(lane_row == lane, value, 0.0)

    def to_parts(k, b, both, dots):
        summed = both[0:16] + both[16:32] + both[32:48]
        dots = list(dots)
        for a in range(3):
            row = jnp.sum(phi[a, :, b * WIDE:(b + 1) * WIDE] * summed, axis=0, keepdims=True)
            for c in range(WIDE // LANES):
                t, piece = b * (WIDE // LANES) + c, row[:, c * LANES:(c + 1) * LANES]
                part_out[k, t, a:a + 1, :] = piece
                for i in range(len(dots)):
                    dots[i] = dots[i] + column_u[i, t, a:a + 1, :] * piece
        return dots

    def with_dots(k, dots):
        row = jnp.zeros((1, LANES), F32)
        for i in range(len(dots)):
            row = row + at_lane(i, jnp.sum(dots[i], axis=1, keepdims=True))
        for t in range(DEPTH):
            part_out[k, t, 3:4, :] = row

    dots = [jnp.zeros((1, LANES), F32)]
    boths = [jnp.zeros((48, WIDE), F32)] * BLOCKS
    for q in range(0, sources, CHUNK):
        left = psi[:, q:q + CHUNK]
        right = sf[:, q:q + CHUNK].T
        for b in range(BLOCKS):
            square = jnp.dot(
                right, tf[:, b * WIDE:(b + 1) * WIDE], preferred_element_type=F32
            )
            root = lax.rsqrt(square)
            factor = root * root * root
            high = factor.astype(BF16)
            low = (factor - high.astype(F32)).astype(BF16)
            matrix[b, q:q + CHUNK, 0:WIDE] = high
            matrix[b, q:q + CHUNK, WIDE:2 * WIDE] = low
            boths[b] = boths[b] + (
                jnp.dot(left, high, preferred_element_type=F32)
                + jnp.dot(left, low, preferred_element_type=F32)
            )
    for b in range(BLOCKS):
        dots = to_parts(0, b, boths[b], dots)
    with_dots(0, dots)

    def inner(left, right):
        return total_of(jnp.sum(left * right, axis=0)[0:3])

    def grams(k):
        latest = column_u[k]
        values = [inner(column_u[i], latest) for i in range(k + 1)]
        row = at_lane(6, values[k])
        for i in range(k + 1):
            row = row + at_lane(8 + i, values[i])
        return row, values

    def exchange(k, with_column):
        whole = slice(0, 4) if with_column else slice(3, 4)
        message = plane_w.at[k, my_p, whole]
        if with_column:
            for _, device in plane_peers[:16]:
                send(message, message, device, 1, plane_sem.at[k])
            for device in column_peers:
                send(message, column_w.at[k, my_z], device, 0, column_sem.at[k])
            for _, device in plane_peers[16:]:
                send(message, message, device, 1, plane_sem.at[k])
        else:
            for _, device in plane_peers:
                send(message, message, device, 1, plane_sem.at[k])
        arrived(plane_w.at[k, pl.ds(0, PLANE - 1), whole], plane_sem.at[k])
        sums = jnp.sum(plane_w[k, :, 3, :], axis=0, keepdims=True)
        gram[k:k + 1, :] = sums
        norm = jnp.sqrt(sums[:, 6:7])
        scaled = 1.0 / norm
        inverse[k:k + 1, :] = jnp.broadcast_to(scaled, (1, LANES))
        table = hes[0:8]
        if k > 0:
            table = jnp.where((hes_rows == k) & (hes_lanes == k - 1), norm, table)
        factors = []
        for i in range(k + 1):
            present = scaled if i == k else inverse[i:i + 1, 0:1]
            value = sums[:, i:i + 1] * present * scaled
            table = jnp.where((hes_rows == i) & (hes_lanes == k), value, table)
            factors.append(value * present)
        hes[0:8] = table
        if k == 0:
            hes[8:9] = jnp.broadcast_to(norm, (1, LANES))
        return scaled, factors

    sent(plane_in.at[pl.ds(0, DEPTH - 1), 0:7], 0)
    sent(plane_in.at[pl.ds(0, PLANE - 1), 0:7], 1)

    def last_parts(first, slot):
        half = pl.ds(first, DEPTH // 2)
        for device in column_peers:
            send(
                part_out.at[ITERS - 1, half, 0:3], part_all.at[my_z, half, 0:3], device, 2 + slot,
                part_sem.at[ITERS - 1 + slot],
            )

    for k in range(ITERS - 1):
        for device in column_peers:
            send(part_out.at[k, device[0]], part_in.at[k, my_z], device, 2, part_sem.at[k])
        part_in[k, my_z] = part_out[k, my_z]
        row, values = grams(k)
        for i in range(k + 1):
            row = row + at_lane(i, values[i])
        applied = column_u[k, my_z]
        arrived(part_in.at[k, pl.ds(0, DEPTH - 1)], part_sem.at[k])
        summed = part_in[k, 0]
        for z in range(1, DEPTH):
            summed = summed + part_in[k, z]
        applied = applied + summed
        plane_w[k, my_p] = jnp.concatenate([applied[0:3], summed[3:4] + row], axis=0)
        column_w[k, my_z] = plane_w[k, my_p]
        scaled, factors = exchange(k, True)
        for s in range(PLANE):
            lanes = slice(s * LANES, (s + 1) * LANES)
            fresh = plane_w[k, s] * scaled
            for i in range(k + 1):
                fresh = fresh - factors[i] * plane_u[i, s]
            plane_u[k + 1, s] = fresh
            value = (
                coef[0, :, lanes] * fresh[0:1]
                + coef[1, :, lanes] * fresh[1:2]
                + coef[2, :, lanes] * fresh[2:3]
            )
            for piece, part in enumerate(split3(value)):
                psi[16 * piece:16 * piece + 16, lanes] = part.astype(BF16)
        arrived(column_w.at[k, pl.ds(0, DEPTH - 1)], column_sem.at[k])
        fresh = column_w[k] * scaled
        for i in range(k + 1):
            fresh = fresh - factors[i] * column_u[i]
        column_u[k + 1] = fresh
        sent(plane_w.at[0, pl.ds(0, DEPTH - 1)], 2)
        sent(plane_w.at[0, pl.ds(0, DEPTH - 1)], 0)
        sent(plane_w.at[0, pl.ds(0, PLANE - 1)], 1)
        final = k + 1 == ITERS - 1
        dots = [jnp.zeros((1, LANES), F32)] * (0 if final else k + 2)
        for b in range(BLOCKS):
            both = jnp.zeros((48, WIDE), F32)
            for q in range(0, sources, DEEP):
                product = jnp.dot(
                    psi[:, q:q + DEEP], matrix[b, q:q + DEEP], preferred_element_type=F32
                )
                both = both + (product[:, 0:WIDE] + product[:, WIDE:2 * WIDE])
            dots = to_parts(k + 1, b, both, dots)
            if final and b == BLOCKS // 2 - 1:
                last_parts(0, 0)
        if final:
            last_parts(DEPTH // 2, 1)
        else:
            with_dots(k + 1, dots)

    k = ITERS - 1
    part_all[my_z] = part_out[k]
    row, _ = grams(k)
    for slot in range(2):
        arrived(part_all.at[pl.ds(0, DEPTH - 1), pl.ds(0, DEPTH // 2), 0:3], part_sem.at[k + slot])
    applied = column_u[k]
    for z in range(DEPTH):
        applied = applied + part_all[z]
    row = row + at_lane(4, inner(applied, applied))
    for i in range(ITERS):
        row = row + at_lane(i, inner(column_u[i], applied))
    column_u[k + 1] = applied
    plane_w[k, my_p] = jnp.concatenate([applied[0, 0:3], row], axis=0)
    scaled, factors = exchange(k, False)
    fresh = column_u[k + 1, my_z] * scaled
    for i in range(ITERS):
        fresh = fresh - factors[i] * column_u[i, my_z]
    column_u[k + 1, my_z] = fresh

    present = [inverse[i:i + 1, 0:1] for i in range(ITERS)]
    tall = [hes[i:i + 1, ITERS - 1:ITERS] for i in range(ITERS)]
    whole = gram[ITERS - 1:ITERS, 4:5] * present[-1] * present[-1]
    square = whole
    for i in range(ITERS):
        square = square - tall[i] * tall[i]
        for j in range(i + 1, ITERS):
            square = square + 2.0 * (tall[i] * present[i]) * (tall[j] * present[j]) * (
                gram[j:j + 1, 8 + i:9 + i]
            )
    norm = jnp.sqrt(jnp.maximum(square, whole * 1e-14))
    inverse[ITERS:ITERS + 1, :] = jnp.broadcast_to(1.0 / norm, (1, LANES))
    table = jnp.where((hes_rows == ITERS) & (hes_lanes == ITERS - 1), norm, hes[0:8])
    packed_ref[8:16] = table
    entry = [[table[i:i + 1, k:k + 1] for k in range(ITERS)] for i in range(ITERS + 1)]
    beta = hes[8:9, 0:1]
    y = least_squares(
        [[entry[i][k] for i in range(k + 1)] for k in range(ITERS)],
        [entry[k + 1][k] for k in range(ITERS)],
        beta,
    )
    solved = jnp.zeros((4, LANES), F32)
    misfit = jnp.zeros((4, LANES), F32)
    for i in range(ITERS + 1):
        basis = column_u[i, my_z] * inverse[i:i + 1, :]
        if i < ITERS:
            solved = solved + y[i] * basis
        g = beta if i == 0 else jnp.zeros_like(beta)
        for k in range(max(i - 1, 0), ITERS):
            g = g - entry[i][k] * y[k]
        misfit = misfit + g * basis
    packed_ref[0:4] = solved
    packed_ref[4:8] = misfit
    for slot in range(2):
        sent(part_all.at[pl.ds(0, DEPTH - 1), pl.ds(0, DEPTH // 2), 0:3], 2 + slot)
    sent(plane_w.at[0, pl.ds(0, PLANE - 1), 3:4], 1)


def unpack(packed_ref, sol_ref, res_ref, hes_ref):
    sol_ref[...] = packed_ref[0:3]
    res_ref[...] = packed_ref[4:7]
    hes_ref[...] = packed_ref[8:16].T[0:ITERS, 0:ITERS + 1]


def shards(positions, areas, right_side):
    vmem = pl.BlockSpec(memory_space=pltpu.VMEM)
    sources, targets = PLANE * LANES, DEPTH * LANES
    packed = pl.pallas_call(
        kernel,
        out_shape=pltpu.VMEM((16, LANES), F32),
        in_specs=[pl.BlockSpec(memory_space=pl.ANY)] * 3,
        out_specs=vmem,
        scratch_shapes=[
            pltpu.VMEM((PLANE, 8, LANES), F32),
            pltpu.VMEM((DEPTH, 8, LANES), F32),
            pltpu.VMEM((BLOCKS, sources, 2 * WIDE), BF16),
            pltpu.VMEM((64, sources), BF16),
            pltpu.VMEM((64, targets), BF16),
            pltpu.VMEM((3, 16, sources), F32),
            pltpu.VMEM((3, 16, targets), F32),
            pltpu.VMEM((48, sources), BF16),
            pltpu.VMEM((ITERS, PLANE, 4, LANES), F32),
            pltpu.VMEM((ITERS, DEPTH, 4, LANES), F32),
            pltpu.VMEM((ITERS, DEPTH, 4, LANES), F32),
            pltpu.VMEM((ITERS, DEPTH, 4, LANES), F32),
            pltpu.VMEM((DEPTH, DEPTH, 4, LANES), F32),
            pltpu.VMEM((ITERS + 1, PLANE, 4, LANES), F32),
            pltpu.VMEM((ITERS + 1, DEPTH, 4, LANES), F32),
            pltpu.VMEM((8, LANES), F32),
            pltpu.VMEM((16, LANES), F32),
            pltpu.VMEM((8, LANES), F32),
            pltpu.SemaphoreType.DMA((3,)),
            pltpu.SemaphoreType.DMA((4,)),
            pltpu.SemaphoreType.DMA((ITERS + 4,)),
            pltpu.SemaphoreType.DMA((ITERS + 1,)),
            pltpu.SemaphoreType.DMA((ITERS + 1,)),
        ],
        compiler_params=pltpu.CompilerParams(
            collective_id=0, has_side_effects=True, vmem_limit_bytes=56 * 1024 * 1024
        ),
        name="arnoldi",
    )(positions, areas.reshape(1, -1), right_side)
    solved, misfit, turned = pl.pallas_call(
        unpack,
        out_shape=(
            jax.ShapeDtypeStruct((3, LANES), F32),
            jax.ShapeDtypeStruct((3, LANES), F32),
            jax.ShapeDtypeStruct((ITERS, ITERS + 1), F32),
        ),
        in_specs=[vmem],
        out_specs=(vmem,) * 3,
        name="unpack",
    )(pltpu.with_memory_space_constraint(packed, pltpu.VMEM))
    return solved, misfit, turned.T


def solution(mesh):
    split = Mesh(mesh.devices.reshape(DEPTH, PLANE), ("z", "p"))
    return jax.shard_map(
        shards,
        mesh=split,
        in_specs=(P(None, ("z", "p")), P(("z", "p")), P(None, ("z", "p"))),
        out_specs=(P(None, ("z", "p")), P(None, ("z", "p")), P()),
        check_vma=False,
    )
```

```python
import functools

import jax
import jax.numpy as jnp
from jax import lax
from jax.experimental import pallas as pl
from jax.experimental.pallas import tpu as pltpu
from jax.sharding import Mesh
from jax.sharding import PartitionSpec as P

ITERS = 4
soften = 0.0025
LANES = 128
WIDE = 256
CHUNK = 512
DEEP = 512
DEPTH = 8
PLANE = 32
BLOCKS = DEPTH * LANES // WIDE
MESH = pl.DeviceIdType.MESH
F32 = jnp.float32
BF16 = jnp.bfloat16


def split3(value):
    first = value.astype(BF16).astype(F32)
    rest = value - first
    second = rest.astype(BF16).astype(F32)
    return first, second, rest - second


def row_iota(rows):
    return lax.broadcasted_iota(jnp.int32, (rows, LANES), 0)


def total_of(value):
    return jnp.sum(jnp.sum(value, axis=0, keepdims=True), axis=1, keepdims=True)


def least_squares(columns, heights, beta):
    zero = jnp.zeros_like(beta)
    size = len(columns)
    table = [[zero] * size for _ in range(size + 1)]
    for k in range(size):
        for i in range(k + 1):
            table[i][k] = columns[k][i]
        table[k + 1][k] = heights[k]
    target = [beta] + [zero] * size
    for c in range(size):
        lead, second = table[c][c], table[c + 1][c]
        radius = jnp.sqrt(lead * lead + second * second)
        cosine, sine = lead / radius, second / radius
        top, low = table[c], table[c + 1]
        new_top = [cosine * t + sine * l for t, l in zip(top, low)]
        new_low = [cosine * l - sine * t for t, l in zip(top, low)]
        table[c], table[c + 1] = new_top, new_low
        a, b = target[c], target[c + 1]
        target[c], target[c + 1] = cosine * a + sine * b, cosine * b - sine * a
    y = [zero] * size
    for r in reversed(range(size)):
        partial = zero
        for c in range(r + 1, size):
            partial = partial + table[r][c] * y[c]
        y[r] = (target[r] - partial) / table[r][r]
    return y


def kernel(
    pos_ref, area_ref, rhs_ref, packed_ref,
    plane_in, column_in, matrix, sf, tf, coef, phi, psi,
    plane_w, column_w, part_out, part_in, part_all, plane_u, column_u, gram, hes, inverse,
    load_sem, send_sem, plane_sem, column_sem, part_sem,
):
    my_z = lax.axis_index("z")
    my_p = lax.axis_index("p")
    my_y, my_x = my_p // 8, (my_p % 2) * 2 + (my_p // 4) % 2
    my_c = (my_p // 2) % 2
    sources = PLANE * LANES

    ys = [((my_y + d) % 4) * 8 for d in range(4)]
    xs = [((my_x + d) % 4) for d in range(4)]
    xs = [(x % 2) * 4 + x // 2 for x in xs]
    cs = [((my_c + d) % 2) * 2 for d in range(2)]
    hops = (0, 1, 2, 1)
    steps = [(a, b, c) for a in range(4) for b in range(4) for c in range(2)][1:]
    steps.sort(key=lambda s: -(4 * (hops[s[0]] + hops[s[1]]) + s[2]))
    plane_peers = [(s[0], (my_z, ys[s[0]] + xs[s[1]] + cs[s[2]])) for s in steps]
    column_peers = [((my_z + d) % DEPTH, my_p) for d in (4, 3, 5, 2, 6, 1, 7)]

    barrier = pltpu.get_barrier_semaphore()
    own = plane_in.at[my_p]
    loads = [
        pltpu.make_async_copy(pos_ref, own.at[0:3], load_sem.at[0]),
        pltpu.make_async_copy(area_ref, own.at[3:4], load_sem.at[1]),
        pltpu.make_async_copy(rhs_ref, own.at[4:7], load_sem.at[2]),
    ]
    for load in loads:
        load.start()
    for device in column_peers + [peer for _, peer in plane_peers]:
        pl.semaphore_signal(barrier, inc=1, device_id=device, device_id_type=MESH)
    for load in loads:
        load.wait()
    pl.semaphore_wait(barrier, PLANE - 1 + DEPTH - 1)

    def send(src, dst, device, slot, recv_sem):
        pltpu.make_async_remote_copy(
            src_ref=src, dst_ref=dst, send_sem=send_sem.at[slot], recv_sem=recv_sem,
            device_id=device, device_id_type=MESH,
        ).start()

    def arrived(part, recv_sem):
        pltpu.make_async_remote_copy(
            src_ref=part, dst_ref=part, send_sem=send_sem.at[0], recv_sem=recv_sem,
            device_id=(my_z, my_p), device_id_type=MESH,
        ).wait_recv()

    def sent(part, slot):
        pltpu.make_async_remote_copy(
            src_ref=part, dst_ref=part, send_sem=send_sem.at[slot], recv_sem=load_sem.at[0],
            device_id=(my_z, my_p), device_id_type=MESH,
        ).wait_send()

    used = own.at[0:7]
    for turn, device in plane_peers[:8]:
        send(used, used, device, 1, plane_sem.at[ITERS + (4 - turn) % 4])
    for device in column_peers:
        send(used, column_in.at[my_z, 0:7], device, 0, column_sem.at[ITERS])
    for turn, device in plane_peers[8:]:
        send(used, used, device, 1, plane_sem.at[ITERS + (4 - turn) % 4])
    plane_in[:, 7:8, :] = jnp.zeros((PLANE, 1, LANES), F32)
    column_in[:, 7:8, :] = jnp.zeros((DEPTH, 1, LANES), F32)
    column_in[my_z] = plane_in[my_p]
    hes[...] = jnp.zeros_like(hes)
    part_out[ITERS - 1] = jnp.zeros((DEPTH, 4, LANES), F32)

    rows8, rows16 = row_iota(8), row_iota(16)
    scale = float(PLANE * DEPTH * LANES) ** (-0.5)

    def one_source_block(s):
        block = plane_in[s]
        lanes = pl.ds(pl.multiple_of(s * LANES, LANES), LANES)
        y = [block[b:b + 1] for b in range(3)]
        weight = block[3:4] * scale
        square = y[0] * y[0] + y[1] * y[1] + y[2] * y[2]
        feature = jnp.where(
            rows8 < 3, block, jnp.where(rows8 == 3, square, jnp.where(rows8 == 4, 1.0, 0.0))
        )
        m1, m2, m3 = split3(feature)
        sf[0:16, lanes] = jnp.concatenate([m1, m2], axis=0).astype(BF16)
        sf[16:32, lanes] = jnp.concatenate([m1, m3], axis=0).astype(BF16)
        sf[32:48, lanes] = jnp.concatenate([m1, m2], axis=0).astype(BF16)
        sf[48:64, lanes] = jnp.concatenate([m2, m3], axis=0).astype(BF16)
        chosen = jnp.zeros((16, LANES), F32)
        for b in range(3):
            mine = ((rows16 >= 3 + 3 * b) & (rows16 < 6 + 3 * b)) | (rows16 == 12 + b)
            chosen = jnp.where(mine, y[b], chosen)
        total = jnp.zeros((16, LANES), F32)
        for b in range(3):
            linear = (rows16 == 3 + b) | (rows16 == 6 + b) | (rows16 == 9 + b)
            last = (rows16 >= 12) & (rows16 < 15)
            value = jnp.where(
                rows16 == b, 1.0, jnp.where(linear, chosen, jnp.where(last, chosen * y[b], 0.0))
            )
            value = value + jnp.where(rows16 == 12 + b, square + 2.0 * soften, 0.0)
            value = value * weight
            coef[b, :, lanes] = value
            total = total + value * block[4 + b:5 + b]
        for piece, part in enumerate(split3(total)):
            psi[16 * piece:16 * piece + 16, lanes] = part.astype(BF16)
        plane_u[0, s] = block[4:8]

    def source_rows(turn, count):
        arrived(plane_in.at[pl.ds(0, count), 0:7], plane_sem.at[ITERS + turn])
        first = ((my_y + turn) % 4) * 8

        def body(s, carry):
            one_source_block(first + s)
            return carry

        lax.fori_loop(0, 8, body, 0, unroll=turn == 2)

    source_rows(0, 7)
    source_rows(1, 8)
    source_rows(3, 8)

    arrived(column_in.at[pl.ds(0, DEPTH - 1), 0:7], column_sem.at[ITERS])
    for t in range(DEPTH):
        block = column_in[t]
        lanes = pl.ds(t * LANES, LANES)
        x = [block[b:b + 1] for b in range(3)]
        square = x[0] * x[0] + x[1] * x[1] + x[2] * x[2]
        feature = jnp.where(
            rows8 < 3, -2.0 * block,
            jnp.where(rows8 == 3, 1.0, jnp.where(rows8 == 4, square + soften, 0.0)),
        )
        t1, t2, t3 = split3(feature)
        tf[0:16, lanes] = jnp.concatenate([t1, t1], axis=0).astype(BF16)
        tf[16:32, lanes] = jnp.concatenate([t2, t1], axis=0).astype(BF16)
        tf[32:48, lanes] = jnp.concatenate([t3, t2], axis=0).astype(BF16)
        tf[48:64, lanes] = jnp.concatenate([t3, t2], axis=0).astype(BF16)
        for a in range(3):
            value = jnp.zeros((16, LANES), F32)
            for b in range(3):
                value = jnp.where(rows16 == b, x[a] * x[b] + (square if a == b else 0.0), value)
                for c in range(3):
                    part = jnp.zeros((1, LANES), F32)
                    if c == a:
                        part = part - 2.0 * x[b]
                    if b == c:
                        part = part - x[a]
                    if b == a:
                        part = part - x[c]
                    value = jnp.where(rows16 == 3 + 3 * b + c, part, value)
            phi[a, :, lanes] = jnp.where(rows16 == 12 + a, 1.0, value)
        column_u[0, t] = block[4:8]

    source_rows(2, 8)

    lane_row = lax.broadcasted_iota(jnp.int32, (1, LANES), 1)
    hes_rows, hes_lanes = row_iota(8), lax.broadcasted_iota(jnp.int32, (8, LANES), 1)

    def at_lane(lane, value):
        return jnp.where(lane_row == lane, value, 0.0)

    def to_parts(k, b, both, dots):
        summed = both[0:16] + both[16:32] + both[32:48]
        dots = list(dots)
        for a in range(3):
            row = jnp.sum(phi[a, :, b * WIDE:(b + 1) * WIDE] * summed, axis=0, keepdims=True)
            for c in range(WIDE // LANES):
                t, piece = b * (WIDE // LANES) + c, row[:, c * LANES:(c + 1) * LANES]
                part_out[k, t, a:a + 1, :] = piece
                for i in range(len(dots)):
                    dots[i] = dots[i] + column_u[i, t, a:a + 1, :] * piece
        return dots

    def with_dots(k, dots):
        row = jnp.zeros((1, LANES), F32)
        for i in range(len(dots)):
            row = row + at_lane(i, jnp.sum(dots[i], axis=1, keepdims=True))
        for t in range(DEPTH):
            part_out[k, t, 3:4, :] = row

    dots = [jnp.zeros((1, LANES), F32)]
    for b in range(BLOCKS):
        both = jnp.zeros((48, WIDE), F32)
        for q in range(0, sources, CHUNK):
            square = lax.dot_general(
                sf[:, q:q + CHUNK], tf[:, b * WIDE:(b + 1) * WIDE], (((0,), (0,)), ((), ())),
                preferred_element_type=F32,
            )
            root = lax.rsqrt(square)
            factor = root * root * root
            high = factor.astype(BF16)
            low = (factor - high.astype(F32)).astype(BF16)
            matrix[b, q:q + CHUNK, 0:WIDE] = high
            matrix[b, q:q + CHUNK, WIDE:2 * WIDE] = low
            left = psi[:, q:q + CHUNK]
            both = both + (
                jnp.dot(left, high, preferred_element_type=F32)
                + jnp.dot(left, low, preferred_element_type=F32)
            )
        dots = to_parts(0, b, both, dots)
    with_dots(0, dots)

    def inner(left, right):
        return total_of(jnp.sum(left * right, axis=0)[0:3])

    def grams(k):
        latest = column_u[k]
        values = [inner(column_u[i], latest) for i in range(k + 1)]
        row = at_lane(6, values[k])
        for i in range(k + 1):
            row = row + at_lane(8 + i, values[i])
        return row, values

    def exchange(k, with_column):
        whole = slice(0, 4) if with_column else slice(3, 4)
        message = plane_w.at[k, my_p, whole]
        if with_column:
            for _, device in plane_peers[:16]:
                send(message, message, device, 1, plane_sem.at[k])
            for device in column_peers:
                send(message, column_w.at[k, my_z], device, 0, column_sem.at[k])
            for _, device in plane_peers[16:]:
                send(message, message, device, 1, plane_sem.at[k])
        else:
            for _, device in plane_peers:
                send(message, message, device, 1, plane_sem.at[k])
        arrived(plane_w.at[k, pl.ds(0, PLANE - 1), whole], plane_sem.at[k])
        sums = jnp.sum(plane_w[k, :, 3, :], axis=0, keepdims=True)
        gram[k:k + 1, :] = sums
        norm = jnp.sqrt(sums[:, 6:7])
        scaled = 1.0 / norm
        inverse[k:k + 1, :] = jnp.broadcast_to(scaled, (1, LANES))
        table = hes[0:8]
        if k > 0:
            table = jnp.where((hes_rows == k) & (hes_lanes == k - 1), norm, table)
        factors = []
        for i in range(k + 1):
            present = scaled if i == k else inverse[i:i + 1, 0:1]
            value = sums[:, i:i + 1] * present * scaled
            table = jnp.where((hes_rows == i) & (hes_lanes == k), value, table)
            factors.append(value * present)
        hes[0:8] = table
        if k == 0:
            hes[8:9] = jnp.broadcast_to(norm, (1, LANES))
        return scaled, factors

    sent(plane_in.at[pl.ds(0, DEPTH - 1), 0:7], 0)
    sent(plane_in.at[pl.ds(0, PLANE - 1), 0:7], 1)

    def last_parts(first, slot):
        half = pl.ds(first, DEPTH // BLOCKS)
        for device in column_peers:
            send(
                part_out.at[ITERS - 1, half, 0:3], part_all.at[my_z, half, 0:3], device, 2 + slot,
                part_sem.at[ITERS - 1 + slot],
            )

    for k in range(ITERS - 1):
        for device in column_peers:
            send(part_out.at[k, device[0]], part_in.at[k, my_z], device, 2, part_sem.at[k])
        part_in[k, my_z] = part_out[k, my_z]
        row, values = grams(k)
        for i in range(k + 1):
            row = row + at_lane(i, values[i])
        applied = column_u[k, my_z]
        arrived(part_in.at[k, pl.ds(0, DEPTH - 1)], part_sem.at[k])
        summed = part_in[k, 0]
        for z in range(1, DEPTH):
            summed = summed + part_in[k, z]
        applied = applied + summed
        plane_w[k, my_p] = jnp.concatenate([applied[0:3], summed[3:4] + row], axis=0)
        column_w[k, my_z] = plane_w[k, my_p]
        scaled, factors = exchange(k, True)
        for s in range(PLANE):
            lanes = slice(s * LANES, (s + 1) * LANES)
            fresh = plane_w[k, s] * scaled
            for i in range(k + 1):
                fresh = fresh - factors[i] * plane_u[i, s]
            plane_u[k + 1, s] = fresh
            value = (
                coef[0, :, lanes] * fresh[0:1]
                + coef[1, :, lanes] * fresh[1:2]
                + coef[2, :, lanes] * fresh[2:3]
            )
            for piece, part in enumerate(split3(value)):
                psi[16 * piece:16 * piece + 16, lanes] = part.astype(BF16)
        arrived(column_w.at[k, pl.ds(0, DEPTH - 1)], column_sem.at[k])
        fresh = column_w[k] * scaled
        for i in range(k + 1):
            fresh = fresh - factors[i] * column_u[i]
        column_u[k + 1] = fresh
        sent(plane_w.at[0, pl.ds(0, DEPTH - 1)], 2)
        sent(plane_w.at[0, pl.ds(0, DEPTH - 1)], 0)
        sent(plane_w.at[0, pl.ds(0, PLANE - 1)], 1)
        final = k + 1 == ITERS - 1
        dots = [jnp.zeros((1, LANES), F32)] * (0 if final else k + 2)
        for b in range(BLOCKS):
            both = jnp.zeros((48, WIDE), F32)
            for q in range(0, sources, DEEP):
                product = jnp.dot(
                    psi[:, q:q + DEEP], matrix[b, q:q + DEEP], preferred_element_type=F32
                )
                both = both + (product[:, 0:WIDE] + product[:, WIDE:2 * WIDE])
            dots = to_parts(k + 1, b, both, dots)
            if final:
                last_parts(b * (DEPTH // BLOCKS), b)
        if not final:
            with_dots(k + 1, dots)

    k = ITERS - 1
    part_all[my_z] = part_out[k]
    row, _ = grams(k)
    for slot in range(BLOCKS):
        arrived(part_all.at[pl.ds(0, DEPTH - 1), pl.ds(0, DEPTH // BLOCKS), 0:3], part_sem.at[k + slot])
    applied = column_u[k]
    for z in range(DEPTH):
        applied = applied + part_all[z]
    row = row + at_lane(4, inner(applied, applied))
    for i in range(ITERS):
        row = row + at_lane(i, inner(column_u[i], applied))
    column_u[k + 1] = applied
    plane_w[k, my_p] = jnp.concatenate([applied[0, 0:3], row], axis=0)
    scaled, factors = exchange(k, False)
    fresh = column_u[k + 1, my_z] * scaled
    for i in range(ITERS):
        fresh = fresh - factors[i] * column_u[i, my_z]
    column_u[k + 1, my_z] = fresh

    present = [inverse[i:i + 1, 0:1] for i in range(ITERS)]
    tall = [hes[i:i + 1, ITERS - 1:ITERS] for i in range(ITERS)]
    whole = gram[ITERS - 1:ITERS, 4:5] * present[-1] * present[-1]
    square = whole
    for i in range(ITERS):
        square = square - tall[i] * tall[i]
        for j in range(i + 1, ITERS):
            square = square + 2.0 * (tall[i] * present[i]) * (tall[j] * present[j]) * (
                gram[j:j + 1, 8 + i:9 + i]
            )
    norm = jnp.sqrt(jnp.maximum(square, whole * 1e-14))
    inverse[ITERS:ITERS + 1, :] = jnp.broadcast_to(1.0 / norm, (1, LANES))
    table = jnp.where((hes_rows == ITERS) & (hes_lanes == ITERS - 1), norm, hes[0:8])
    packed_ref[8:16] = table
    entry = [[table[i:i + 1, k:k + 1] for k in range(ITERS)] for i in range(ITERS + 1)]
    beta = hes[8:9, 0:1]
    y = least_squares(
        [[entry[i][k] for i in range(k + 1)] for k in range(ITERS)],
        [entry[k + 1][k] for k in range(ITERS)],
        beta,
    )
    solved = jnp.zeros((4, LANES), F32)
    misfit = jnp.zeros((4, LANES), F32)
    for i in range(ITERS + 1):
        basis = column_u[i, my_z] * inverse[i:i + 1, :]
        if i < ITERS:
            solved = solved + y[i] * basis
        g = beta if i == 0 else jnp.zeros_like(beta)
        for k in range(max(i - 1, 0), ITERS):
            g = g - entry[i][k] * y[k]
        misfit = misfit + g * basis
    packed_ref[0:4] = solved
    packed_ref[4:8] = misfit
    for slot in range(BLOCKS):
        sent(part_all.at[pl.ds(0, DEPTH - 1), pl.ds(0, DEPTH // BLOCKS), 0:3], 2 + slot)
    sent(plane_w.at[0, pl.ds(0, PLANE - 1), 3:4], 1)


def unpack(packed_ref, sol_ref, res_ref, hes_ref):
    sol_ref[...] = packed_ref[0:3]
    res_ref[...] = packed_ref[4:7]
    hes_ref[...] = packed_ref[8:16].T[0:ITERS, 0:ITERS + 1]


def shards(positions, areas, right_side):
    vmem = pl.BlockSpec(memory_space=pltpu.VMEM)
    sources, targets = PLANE * LANES, DEPTH * LANES
    packed = pl.pallas_call(
        kernel,
        out_shape=pltpu.VMEM((16, LANES), F32),
        in_specs=[pl.BlockSpec(memory_space=pl.ANY)] * 3,
        out_specs=vmem,
        scratch_shapes=[
            pltpu.VMEM((PLANE, 8, LANES), F32),
            pltpu.VMEM((DEPTH, 8, LANES), F32),
            pltpu.VMEM((BLOCKS, sources, 2 * WIDE), BF16),
            pltpu.VMEM((64, sources), BF16),
            pltpu.VMEM((64, targets), BF16),
            pltpu.VMEM((3, 16, sources), F32),
            pltpu.VMEM((3, 16, targets), F32),
            pltpu.VMEM((48, sources), BF16),
            pltpu.VMEM((ITERS, PLANE, 4, LANES), F32),
            pltpu.VMEM((ITERS, DEPTH, 4, LANES), F32),
            pltpu.VMEM((ITERS, DEPTH, 4, LANES), F32),
            pltpu.VMEM((ITERS, DEPTH, 4, LANES), F32),
            pltpu.VMEM((DEPTH, DEPTH, 4, LANES), F32),
            pltpu.VMEM((ITERS + 1, PLANE, 4, LANES), F32),
            pltpu.VMEM((ITERS + 1, DEPTH, 4, LANES), F32),
            pltpu.VMEM((8, LANES), F32),
            pltpu.VMEM((16, LANES), F32),
            pltpu.VMEM((8, LANES), F32),
            pltpu.SemaphoreType.DMA((3,)),
            pltpu.SemaphoreType.DMA((2 + BLOCKS,)),
            pltpu.SemaphoreType.DMA((ITERS + 4,)),
            pltpu.SemaphoreType.DMA((ITERS + 1,)),
            pltpu.SemaphoreType.DMA((ITERS - 1 + BLOCKS,)),
        ],
        compiler_params=pltpu.CompilerParams(
            collective_id=0, has_side_effects=True, vmem_limit_bytes=56 * 1024 * 1024
        ),
        name="arnoldi",
    )(positions, areas.reshape(1, -1), right_side)
    solved, misfit, turned = pl.pallas_call(
        unpack,
        out_shape=(
            jax.ShapeDtypeStruct((3, LANES), F32),
            jax.ShapeDtypeStruct((3, LANES), F32),
            jax.ShapeDtypeStruct((ITERS, ITERS + 1), F32),
        ),
        in_specs=[vmem],
        out_specs=(vmem,) * 3,
        name="unpack",
    )(pltpu.with_memory_space_constraint(packed, pltpu.VMEM))
    return solved, misfit, turned.T


def solution(mesh):
    split = Mesh(mesh.devices.reshape(DEPTH, PLANE), ("z", "p"))
    return jax.shard_map(
        shards,
        mesh=split,
        in_specs=(P(None, ("z", "p")), P(("z", "p")), P(None, ("z", "p"))),
        out_specs=(P(None, ("z", "p")), P(None, ("z", "p")), P()),
        check_vma=False,
    )
```
